32 devices in a mesh: tm: 8 (over z, x), rows: 4 (over y, core).
Axes of the slice: x: 2, y: 2, z: 4, core: 2. Of those that a mesh axis runs over, the one named last changes fastest.
Arguments:
- initial_warmth: float32 [1024, 1024], P('rows'), may hold values from -6 to 6
- pattern_choice: int32 [16, 8, 8], P('tm'), may hold values from 0 to 7
- dissipation_tables: float32 [8, 128, 128], replicated, may hold values from -6 to 6
- material_label: int32 [8, 8], replicated, may hold values from 0 to 3
- intercept_kappa: float32 [4], replicated, may hold values from 4 to 8
- sensitivity_coef: float32 [4], replicated, may hold values from -0.5 to 0.5
Outputs:
- warmth_trajectory: float32 [16, 1024, 1024], P('tm', 'rows')
The draws below stay inside these ranges and needn't reach their ends.
All inputs are finite; a program needn't handle non-finite values.
Results may differ from the reference program's by a relative error of at most 0.0003.
Values sent between devices are 32-bit elements; how exact they have to be, the bound alone decides.
A program may use at most 128 MiB of HBM per device.

```python
import math
import jax
import jax.numpy as jnp
from jax import lax

TILES_PER_ROW = 1024
TILES_PER_COLUMN = 1024
TILE = 128
REGIONS = 4
PATTERNS = 8
ITERS = 2
HORIZON_COUNT = 16
TY = 8
TX = 8


def draw_pattern_choice(key, part):
    base_key = jax.random.fold_in(key, 101)
    fresh_key = jax.random.fold_in(key, 202)
    switch_key = jax.random.fold_in(key, 303)
    settled = jax.random.randint(base_key, (TY, TX), 0, PATTERNS)
    fresh = jax.random.randint(fresh_key, (HORIZON_COUNT, TY, TX), 0, PATTERNS)
    switch = jax.random.randint(switch_key, (HORIZON_COUNT, TY, TX), 0, 4)
    return jnp.where(switch == 0, fresh, settled[None]).astype(jnp.int32)


def draw_dissipation_tables(key, part):
    rough_key = jax.random.fold_in(key, 404)
    rough = jax.random.normal(rough_key, (PATTERNS, TILE, TILE), jnp.float32)
    return jnp.clip(rough, -6.0, 6.0).astype(jnp.float32)


def touch_ends(array, key, smallest, top_value):
    spot = [jax.random.randint(jax.random.fold_in(key, axis), (), 0, length) for axis, length in enumerate(array.shape)]
    widest = array.shape.index(max(array.shape))
    neighbour = spot[:widest] + [(spot[widest] + 1) % array.shape[widest]] + spot[widest + 1:]
    return array.at[tuple(spot)].set(smallest).at[tuple(neighbour)].set(top_value)


def level_of(stream_key, extent, cuts, least, largest):
    def one(position, shards_of):
        steps = jax.random.uniform(jax.random.fold_in(jax.random.fold_in(stream_key, 6), position), (shards_of,), jnp.float32, least / len(cuts), largest / len(cuts))
        return jnp.repeat(jnp.exp(steps), extent[position] // shards_of).reshape((-1,) + (1,) * (len(extent) - position - 1))

    factor_of = one(*cuts[0])
    for cut in cuts[1:]:
        factor_of = factor_of * one(*cut)
    return factor_of


def scatter_about(rng, shape, spread, most, cuts=(), kind=jnp.bfloat16):
    drawn = spread * jax.random.normal(rng, shape, jnp.float32)
    if cuts:
        drawn = drawn * level_of(rng, shape, cuts, -0.22, 0.18)
    return jnp.clip(drawn, -most, most).astype(kind)


def setup_inputs(seed: int = 0) -> dict:
    key_of = jax.random.split(jax.random.key(seed), 7)
    return {
        "initial_warmth": scatter_about(key_of[0], (TILES_PER_COLUMN, TILES_PER_ROW), 1.0, 6.0, ((0, 4),), jnp.float32),
        "pattern_choice": draw_pattern_choice(jax.random.fold_in(key_of[6], 71), 0),
        "dissipation_tables": draw_dissipation_tables(jax.random.fold_in(key_of[6], 71), 0),
        "material_label": touch_ends(jax.random.randint(key_of[3], (TY, TX), 0, REGIONS), jax.random.fold_in(key_of[3], 1), 0, REGIONS - 1).astype(jnp.int32),
        "intercept_kappa": jnp.clip(jnp.exp(jax.random.uniform(key_of[4], (REGIONS,), jnp.float32, math.log(4.0), math.log(8.0))), 4.0, 8.0),
        "sensitivity_coef": jnp.clip(jax.random.uniform(key_of[5], (REGIONS,), jnp.float32, -0.5, 0.5), -0.5, 0.5),
    }


TIMESTEP_SIZE = 2.0
ALPHA = 0.05
CROSS_WEIGHT = 1.0 / 64.0


def dct_last(values):
    count = values.shape[-1]
    mirrored = jnp.concatenate([values, jnp.flip(values, -1)], -1)
    spectrum = jnp.fft.fft(mirrored, axis=-1)[..., :count]
    angle = jnp.arange(count).astype(values.dtype) * (math.pi / (2 * count))
    return 0.5 * (jnp.real(spectrum) * jnp.cos(angle) + jnp.imag(spectrum) * jnp.sin(angle))


def idct_last(values):
    count = values.shape[-1]
    angle = jnp.arange(count).astype(values.dtype) * (math.pi / (2 * count))
    weights = jnp.where(jnp.arange(count) == 0, 1.0, 2.0).astype(values.dtype)
    scaled = values * weights
    filled = lax.complex(scaled * jnp.cos(angle), scaled * jnp.sin(angle))
    filled = jnp.concatenate([filled, jnp.zeros_like(filled)], -1)
    return 2.0 * jnp.real(jnp.fft.ifft(filled, axis=-1))[..., :count]


def both_forward(values):
    inner = dct_last(values)
    return jnp.swapaxes(dct_last(jnp.swapaxes(inner, 1, 2)), 1, 2)


def both_inverse(values):
    inner = jnp.swapaxes(idct_last(jnp.swapaxes(values, 1, 2)), 1, 2)
    return idct_last(inner)


def reference(initial_warmth, pattern_choice, dissipation_tables, material_label, intercept_kappa, sensitivity_coef):
    tiles = dissipation_tables[pattern_choice]
    forcing_term = jnp.transpose(tiles, (0, 1, 3, 2, 4)).reshape(HORIZON_COUNT, TILES_PER_COLUMN, TILES_PER_ROW)
    reference_level = jnp.repeat(jnp.repeat(intercept_kappa[material_label], TILE, 0), TILE, 1)
    kappa_derivative = jnp.repeat(jnp.repeat(sensitivity_coef[material_label], TILE, 0), TILE, 1)
    conduct = jnp.mean(intercept_kappa)
    amplification = jnp.exp(jnp.arange(HORIZON_COUNT).astype(jnp.float32) * (math.log(ALPHA) / HORIZON_COUNT))
    shrink = ALPHA ** (1.0 / HORIZON_COUNT)
    theta = jnp.arange(HORIZON_COUNT).astype(jnp.float32) * (2.0 * math.pi / HORIZON_COUNT)
    mu_rows = 2.0 - 2.0 * jnp.cos(jnp.arange(TILES_PER_COLUMN).astype(jnp.float32) * (math.pi / TILES_PER_COLUMN))
    mu_cols = 2.0 - 2.0 * jnp.cos(jnp.arange(TILES_PER_ROW).astype(jnp.float32) * (math.pi / TILES_PER_ROW))
    real_den = (1.0 - shrink * jnp.cos(theta))[:, None, None] / TIMESTEP_SIZE + conduct * (mu_rows[None, :, None] + CROSS_WEIGHT * mu_cols[None, None, :])
    imag_den = (shrink * jnp.sin(theta) / TIMESTEP_SIZE)[:, None, None]
    norm_den = real_den * real_den + imag_den * imag_den
    warmth_trajectory = jnp.broadcast_to(initial_warmth[None], (HORIZON_COUNT, TILES_PER_COLUMN, TILES_PER_ROW)).astype(jnp.float32)
    for sweep in range(ITERS):
        kappa_local = reference_level * (1.0 + kappa_derivative * jnp.tanh(warmth_trajectory))
        upward_current = 0.5 * (kappa_local[:, 1:] + kappa_local[:, :-1]) * (warmth_trajectory[:, 1:] - warmth_trajectory[:, :-1])
        lateral_current = CROSS_WEIGHT * (0.5 * (kappa_local[:, :, 1:] + kappa_local[:, :, :-1]) * (warmth_trajectory[:, :, 1:] - warmth_trajectory[:, :, :-1]))
        energy_ledger = jnp.pad(upward_current, ((0, 0), (0, 1), (0, 0))) - jnp.pad(upward_current, ((0, 0), (1, 0), (0, 0)))
        energy_ledger = energy_ledger + jnp.pad(lateral_current, ((0, 0), (0, 0), (0, 1))) - jnp.pad(lateral_current, ((0, 0), (0, 0), (1, 0)))
        former_warmth = jnp.concatenate([initial_warmth[None], warmth_trajectory[:-1]], 0)
        defect_vector = forcing_term - (warmth_trajectory - former_warmth) / TIMESTEP_SIZE + energy_ledger
        scaled = defect_vector * amplification[:, None, None]
        spectrum = jnp.fft.fft(scaled, axis=0)
        modes_re = both_forward(jnp.real(spectrum))
        modes_im = both_forward(jnp.imag(spectrum))
        solved_re = (modes_re * real_den + modes_im * imag_den) / norm_den
        solved_im = (modes_im * real_den - modes_re * imag_den) / norm_den
        field_re = both_inverse(solved_re)
        field_im = both_inverse(solved_im)
        correction_delta = jnp.real(jnp.fft.ifft(lax.complex(field_re, field_im), axis=0))
        warmth_trajectory = warmth_trajectory + correction_delta / amplification[:, None, None]
    return warmth_trajectory
```

```python
import math
from types import SimpleNamespace

import jax
import jax.numpy as jnp
import numpy as np
from jax import lax
from jax.experimental import pallas as pl
from jax.experimental.pallas import tpu as pltpu
from jax.sharding import PartitionSpec as P

TILE = 128
ITERS = 2
TIMESTEP_SIZE = 2.0
ALPHA = 0.05
CROSS_WEIGHT = 1.0 / 64.0
F32 = jnp.float32
BF16 = jnp.bfloat16


def extended(block, axis, dim):
    count = lax.axis_size(axis)
    forward = [(i, i + 1) for i in range(count - 1)]
    backward = [(target, source) for source, target in forward]
    low = lax.ppermute(
        lax.slice_in_dim(block, block.shape[dim] - 1, None, axis=dim), axis, forward
    )
    high = lax.ppermute(lax.slice_in_dim(block, 0, 1, axis=dim), axis, backward)
    return jnp.concatenate([low, block, high], axis=dim)


def cosine_table(length):
    modes = np.arange(length, dtype=np.int64)[:, None]
    cells = np.arange(length, dtype=np.int64)[None, :]
    phase = modes * (2 * cells + 1) % (4 * length)
    return np.cos(phase * (math.pi / (2 * length)))


def two_parts(table):
    high = np.asarray(table, dtype=np.float32).astype(BF16)
    low = (table - high.astype(np.float64)).astype(np.float32).astype(BF16)
    return jnp.asarray(high), jnp.asarray(low)


def split(values):
    high = values.astype(BF16)
    return high, (values - high.astype(F32)).astype(BF16)


def mul(left, right):
    return jnp.dot(left, right, preferred_element_type=F32)


def columns_kernel(x_ref, high_ref, low_ref, out_ref, x_high, x_low):
    @pl.when(pl.program_id(0) == 0)
    def _():
        x_high[...], x_low[...] = split(x_ref[...])

    high = high_ref[...]
    out_ref[...] = (
        mul(x_high[...], high) + mul(x_low[...], high) + mul(x_high[...], low_ref[...])
    )


def times_table(values, table):
    rows, depth = values.shape
    width = table[0].shape[1]
    block = min(256, width)
    return pl.pallas_call(
        columns_kernel,
        grid=(width // block,),
        out_shape=jax.ShapeDtypeStruct((rows, width), F32),
        in_specs=[
            pl.BlockSpec((rows, depth), lambda i: (0, 0)),
            pl.BlockSpec((depth, block), lambda i: (0, i)),
            pl.BlockSpec((depth, block), lambda i: (0, i)),
        ],
        out_specs=pl.BlockSpec((rows, block), lambda i: (0, i)),
        scratch_shapes=[pltpu.VMEM((rows, depth), BF16)] * 2,
    )(values, *table)


def rows_kernel(high_ref, low_ref, x_ref, out_ref, x_high, x_low):
    @pl.when(pl.program_id(0) == 0)
    def _():
        x_high[...], x_low[...] = split(x_ref[...])

    for n in range(x_ref.shape[0]):
        out_ref[n] = (
            mul(high_ref[...], x_high[n])
            + mul(high_ref[...], x_low[n])
            + mul(low_ref[...], x_high[n])
        )


def table_times(table, values):
    steps, depth, width = values.shape
    height = table[0].shape[0]
    block = min(256, height)
    return pl.pallas_call(
        rows_kernel,
        grid=(height // block,),
        out_shape=jax.ShapeDtypeStruct((steps, height, width), F32),
        in_specs=[
            pl.BlockSpec((block, depth), lambda i: (i, 0)),
            pl.BlockSpec((block, depth), lambda i: (i, 0)),
            pl.BlockSpec((steps, depth, width), lambda i: (0, 0, 0)),
        ],
        out_specs=pl.BlockSpec((steps, block, width), lambda i: (0, i, 0)),
        scratch_shapes=[pltpu.VMEM((steps, depth, width), BF16)] * 2,
    )(*table, values)


def power_kernel(choice_ref, table_ref, out_ref):
    steps, blocks, _, width = out_ref.shape
    across = width // TILE
    for n in range(steps):
        for b in range(blocks):
            for x in range(across):
                picked = choice_ref[n, b * across + x]
                out_ref[n, b, :, x * TILE : (x + 1) * TILE] = table_ref[picked]


def power_of(pattern_choice, tables, first_row, strip, width):
    steps = pattern_choice.shape[0]
    part = min(TILE, strip)
    blocks = strip // part
    offset = first_row % TILE if strip < TILE else 0
    tiles = lax.dynamic_slice_in_dim(tables, offset, part, axis=1)
    chosen = lax.dynamic_slice_in_dim(pattern_choice, first_row // TILE, blocks, axis=1)
    power = pl.pallas_call(
        power_kernel,
        out_shape=jax.ShapeDtypeStruct((steps, blocks, part, width), F32),
        in_specs=[
            pl.BlockSpec(memory_space=pltpu.SMEM),
            pl.BlockSpec(memory_space=pltpu.VMEM),
        ],
        out_specs=pl.BlockSpec(memory_space=pltpu.VMEM),
    )(chosen.reshape(steps, -1), tiles)
    return power.reshape(steps, strip, width)


def divergence(warmth, kappa, inner):
    def face(low, high):
        return 1.0 if kappa is None else 0.5 * (low + high)

    k = warmth if kappa is None else kappa
    upward = face(k[:, 1:], k[:, :-1]) * (warmth[:, 1:] - warmth[:, :-1])
    upward = jnp.where(inner[None, :, None], upward, 0.0)
    centre, k_mid = warmth[:, 1:-1], k[:, 1:-1]
    lateral = CROSS_WEIGHT * (
        face(k_mid[:, :, 1:], k_mid[:, :, :-1]) * (centre[:, :, 1:] - centre[:, :, :-1])
    )
    zero = jnp.zeros_like(centre[:, :, :1])
    across = jnp.concatenate([lateral, zero], 2) - jnp.concatenate([zero, lateral], 2)
    return upward[:, 1:] - upward[:, :-1] + across


def mode_factors(row_ids, column_ids, height, width, conduct):
    mu_rows = 2.0 - 2.0 * jnp.cos(row_ids.astype(F32) * (math.pi / height))
    mu_cols = 2.0 - 2.0 * jnp.cos(column_ids.astype(F32) * (math.pi / width))
    rate = conduct * (mu_rows[:, None] + CROSS_WEIGHT * mu_cols[None, :])
    gain = 1.0 / (1.0 / TIMESTEP_SIZE + rate)
    return gain, gain * (1.0 / TIMESTEP_SIZE)


def shards(
    initial_warmth,
    pattern_choice,
    dissipation_tables,
    material_label,
    intercept_kappa,
    sensitivity_coef,
):
    steps = pattern_choice.shape[0]
    strip, width = initial_warmth.shape
    tm_count = lax.axis_size("tm")
    rows_count = lax.axis_size("rows")
    height = strip * rows_count
    first_row = lax.axis_index("rows") * strip
    power = power_of(pattern_choice, dissipation_tables, first_row, strip, width)

    padded_rows = first_row - 1 + jnp.arange(strip + 2, dtype=jnp.int32)
    labels = jnp.take(material_label, jnp.clip(padded_rows, 0, height - 1) // TILE, axis=0)
    base_tiles = jnp.zeros(labels.shape, F32)
    slope_tiles = jnp.zeros(labels.shape, F32)
    for label in range(intercept_kappa.shape[0]):
        base_tiles = jnp.where(labels == label, intercept_kappa[label], base_tiles)
        slope_tiles = jnp.where(labels == label, sensitivity_coef[label], slope_tiles)
    base = jnp.repeat(base_tiles, TILE, axis=1)[None]
    slope = jnp.repeat(slope_tiles, TILE, axis=1)[None]
    upper_rows = padded_rows[:-1]
    inner = (upper_rows >= 0) & (upper_rows + 1 <= height - 1)
    conduct = jnp.mean(intercept_kappa)

    column_cos = cosine_table(width)
    row_cos = cosine_table(height)
    columns_out, columns_in = two_parts(column_cos.T), two_parts(column_cos)
    if height == width:
        rows_out, rows_in = columns_in, columns_out
    else:
        rows_out, rows_in = two_parts(row_cos), two_parts(row_cos.T)

    narrow = width // rows_count
    share = height // tm_count
    column_ids = lax.axis_index("rows") * narrow + jnp.arange(narrow, dtype=jnp.int32)
    all_rows = jnp.arange(height, dtype=jnp.int32)
    own_rows = lax.axis_index("tm") * share + jnp.arange(share, dtype=jnp.int32)
    gain, keep = mode_factors(all_rows, column_ids, height, width, conduct)
    weight = (jnp.where(all_rows == 0, 1.0, 2.0) / height)[:, None] * (
        jnp.where(column_ids == 0, 1.0, 2.0) / width
    )[None, :]
    _, own_keep = mode_factors(own_rows, column_ids, height, width, conduct)
    block_keep = own_keep
    for _ in range(steps - 1):
        block_keep = block_keep * own_keep
    around = block_keep
    for _ in range(tm_count - 1):
        around = around * block_keep
    closing = ALPHA / (1.0 - ALPHA * around)
    first_block = lax.axis_index("tm") == 0

    start = extended(initial_warmth[None], "rows", 1)
    start_div = divergence(start, base * (1.0 + slope * jnp.tanh(start)), inner)
    warmth = jnp.broadcast_to(initial_warmth[None], (steps, strip, width))
    wrapped = None
    for sweep in range(ITERS):
        if sweep == 0:
            resid = power + start_div
        else:
            grid = extended(warmth, "rows", 1)
            div = divergence(grid, base * (1.0 + slope * jnp.tanh(grid)), inner)
            resid = div - last_div - conduct * divergence(grid - last_grid, None, inner)
        modes = times_table(resid.reshape(steps * strip, width), columns_out)
        modes = lax.all_to_all(
            modes.reshape(steps, strip, width), "rows", split_axis=2, concat_axis=1, tiled=True
        )
        modes = table_times(rows_out, modes)
        sources = [modes[n] * weight for n in range(steps)]
        if wrapped is not None:
            sources[0] = sources[0] - jnp.where(first_block, wrapped / TIMESTEP_SIZE, 0.0)
        sources = [gain * source for source in sources]
        block_end = sources[0]
        for source in sources[1:]:
            block_end = source + keep * block_end
        ends = lax.all_to_all(block_end, "tm", split_axis=0, concat_axis=0, tiled=True)
        ends = ends.reshape(tm_count, share, narrow)
        last = ends[0]
        for k in range(1, tm_count):
            last = ends[k] + block_keep * last
        entry = [closing * last]
        for k in range(tm_count - 1):
            entry.append(ends[k] + block_keep * entry[k])
        entry = jnp.concatenate(entry, 0)
        carry = lax.all_to_all(entry, "tm", split_axis=0, concat_axis=0, tiled=True)
        wrapped = carry
        solved = []
        for source in sources:
            carry = source + keep * carry
            solved.append(carry)
        field = table_times(rows_in, jnp.stack(solved, 0))
        field = lax.all_to_all(field, "rows", split_axis=1, concat_axis=2, tiled=True)
        update = times_table(field.reshape(steps * strip, width), columns_in)
        if sweep == 0:
            last_grid, last_div = start, start_div
        else:
            last_grid, last_div = grid, div
        warmth = warmth + update.reshape(steps, strip, width)
    return warmth


LANES = 128
EDGE = 8
ROWS = 32
MESH = pl.DeviceIdType.MESH


def dot3(left_high, left_low, right_high, right_low):
    return mul(left_high, right_high) + mul(left_low, right_high) + mul(left_high, right_low)


def remote(src, dst, send_sem, recv_sem, device):
    return pltpu.make_async_remote_copy(
        src_ref=src,
        dst_ref=dst,
        send_sem=send_sem,
        recv_sem=recv_sem,
        device_id=device,
        device_id_type=MESH,
    )


def scratch_of(steps, strip, length, tm_count, rows_count):
    narrow = length // rows_count
    chunks = narrow // LANES
    half = length // 2
    units = half // LANES
    wide = steps * LANES
    padded = strip + 2 * EDGE
    peers = rows_count - 1

    def f32(*shape):
        return pltpu.VMEM(shape, F32)

    def b16(*shape):
        return pltpu.VMEM(shape, BF16)

    dma = pltpu.SemaphoreType.DMA
    return dict(
        ch=b16(length, length),
        cl=b16(length, length),
        cth=b16(length, length),
        ctl=b16(length, length),
        ph=b16(length, length),
        pl=b16(length, length),
        th=b16(8, TILE, TILE),
        tl=b16(8, TILE, TILE),
        base=f32(8, length),
        slope=f32(8, length),
        w0p=f32(padded, length),
        kp=f32(padded, length),
        div0=f32(strip, length),
        halo=f32(2, EDGE, length),
        dst=f32(peers, strip, narrow),
        xd=f32(length, narrow),
        xh=b16(chunks, length, wide),
        xl=b16(chunks, length, wide),
        fx=f32(chunks, rows_count, strip, wide),
        xr=f32(chunks, length, wide),
        ss=f32(chunks, length, wide),
        e=f32(ITERS, chunks, length, LANES),
        er=f32(ITERS, chunks, half, LANES),
        fin=f32(ITERS, chunks, half, LANES),
        sin=f32(ITERS, chunks, half, LANES),
        fout=f32(ITERS, chunks, half, LANES),
        sout=f32(ITERS, chunks, half, LANES),
        cs=f32(ITERS, chunks, half, LANES),
        zz=f32(half, LANES),
        carry=f32(ITERS, chunks, length, LANES),
        ctot=f32(chunks, length, LANES),
        gw=f32(chunks, length, LANES),
        keep=f32(chunks, length, LANES),
        rho=f32(chunks, length, LANES),
        sd=f32(chunks, length, LANES),
        k1=f32(chunks, half, LANES),
        k2=f32(chunks, half, LANES),
        pa=f32(chunks, half, LANES),
        pb=f32(chunks, half, LANES),
        pf=f32(chunks, half, LANES),
        iy=f32(ITERS, chunks, length + 2 * EDGE, wide),
        yr=f32(ITERS, chunks, rows_count, padded, wide),
        uh=b16(length, wide),
        ul=b16(length, wide),
        lh=b16(steps * padded, rows_count * LANES),
        ll=b16(steps * padded, rows_count * LANES),
        u1p=f32(steps * padded, length),
        tsem=dma((4,)),
        hs=dma((2,)),
        hr=dma((2,)),
        ds=dma((peers,)),
        dr=dma((peers,)),
        xs=dma((chunks * peers,)),
        xrs=dma((chunks * peers,)),
        ys=dma((ITERS * chunks * peers,)),
        yrs=dma((ITERS * chunks * peers,)),
        es=dma((ITERS * chunks * units,)),
        ers=dma((ITERS * chunks * units,)),
        fs=dma((ITERS * chunks * units,)),
        frs=dma((ITERS * chunks * units,)),
        gs=dma((ITERS * chunks * units,)),
        grs=dma((ITERS * chunks * units,)),
        cts=dma((ITERS * chunks * units,)),
        crs=dma((ITERS * chunks * units,)),
    )


INPUTS = [
    "w0",
    "choice",
    "tables",
    "label",
    "icpt",
    "sens",
    "mup",
    "muq",
    "chh",
    "clh",
    "cthh",
    "ctlh",
]


def fused_kernel(steps, strip, length, tm_count, rows_count, names, *refs):
    s = SimpleNamespace(**dict(zip(names, refs)))
    narrow = length // rows_count
    chunks = narrow // LANES
    half = length // 2
    units = half // LANES
    padded = strip + 2 * EDGE
    blocks = strip // TILE
    tiles = length // TILE
    big = 2 * LANES
    zs, ys_count = tm_count // 2, rows_count // 2

    t, r = lax.axis_index("tm"), lax.axis_index("rows")
    z, x = lax.div(t, 2), lax.rem(t, 2)
    y, c = lax.div(r, 2), lax.rem(r, 2)
    pair = t + 1 - 2 * x
    peers = [(dy, dc) for dy in range(1, ys_count) for dc in range(2)] + [(0, 1)]

    def to(dy, dc):
        return lax.rem(y + dy, ys_count) * 2 + lax.rem(c + dc, 2)

    def frm(dy, dc):
        return lax.rem(y + ys_count - dy, ys_count) * 2 + lax.rem(c + 2 - dc, 2)

    def rows_at(start, size):
        return pl.ds(pl.multiple_of(start, size), size)

    tables_in = [
        pltpu.make_async_copy(a, b, s.tsem.at[i])
        for i, (a, b) in enumerate(
            [(s.cthh, s.cth), (s.ctlh, s.ctl), (s.chh, s.ch), (s.clh, s.cl)]
        )
    ]
    for copy in tables_in:
        copy.start()

    barrier = pltpu.get_barrier_semaphore()
    for dy, dc in peers:
        pl.semaphore_signal(barrier, inc=1, device_id=(t, to(dy, dc)), device_id_type=MESH)
    pl.semaphore_signal(barrier, inc=1, device_id=(pair, r), device_id_type=MESH)

    @pl.when(z > 0)
    def _():
        pl.semaphore_signal(barrier, inc=1, device_id=(t - 2, r), device_id_type=MESH)

    @pl.when(z < zs - 1)
    def _():
        pl.semaphore_signal(barrier, inc=1, device_id=(t + 2, r), device_id_type=MESH)

    beside = lax.min(z, 1) + lax.min(zs - 1 - z, 1)
    pl.semaphore_wait(barrier, len(peers) + 1 + beside)

    def halo_down(to_row):
        return remote(
            s.w0.at[pl.ds(strip - EDGE, EDGE)], s.halo.at[0], s.hs.at[0], s.hr.at[0], (t, to_row)
        )

    def halo_up(to_row):
        return remote(s.w0.at[pl.ds(0, EDGE)], s.halo.at[1], s.hs.at[1], s.hr.at[1], (t, to_row))

    @pl.when(r < rows_count - 1)
    def _():
        halo_down(r + 1).start()

    @pl.when(r > 0)
    def _():
        halo_up(r - 1).start()

    count = s.icpt.shape[0]
    total = s.icpt[0]
    for i in range(1, count):
        total = total + s.icpt[i]
    conduct = total / count
    for i in range(blocks + 2):
        ty = lax.min(lax.max(r * blocks - 1 + i, 0), tiles - 1)
        for tx in range(tiles):
            label = s.label[ty, tx]
            s.base[i : i + 1, tx * TILE : (tx + 1) * TILE] = jnp.full((1, TILE), s.icpt[label], F32)
            s.slope[i : i + 1, tx * TILE : (tx + 1) * TILE] = jnp.full((1, TILE), s.sens[label], F32)

    for j in range(chunks):

        def factors(i, _, j=j):
            rows = rows_at(i * LANES, LANES)
            rate = conduct * (s.mup[rows] + CROSS_WEIGHT * s.muq[r * chunks + j, 0:1, :])
            gain = 1.0 / (1.0 / TIMESTEP_SIZE + rate)
            keep = gain * (1.0 / TIMESTEP_SIZE)
            p = i * LANES + lax.broadcasted_iota(jnp.int32, (LANES, LANES), 0)
            q = r * narrow + j * LANES + lax.broadcasted_iota(jnp.int32, (LANES, LANES), 1)
            weight = (jnp.where(p == 0, 1.0, 2.0) / length) * (jnp.where(q == 0, 1.0, 2.0) / length)
            s.gw[j, rows] = gain * weight
            s.keep[j, rows] = keep
            one = 1.0 + keep
            k = keep * keep
            around, power = one, k
            for _ in range(tm_count - 1):
                around = one + k * around
                power = power * k
            first = ALPHA * around / (1.0 - ALPHA * power)
            s.rho[j, rows] = lax.fori_loop(0, t, lambda _, a: one + k * a, first)
            return 0

        lax.fori_loop(0, length // LANES, factors, 0)

        def chain(i, _, j=j):
            rows = rows_at(i * LANES, LANES)
            keep = s.keep[j, rows_at(x * half + i * LANES, LANES)]
            k = keep * keep
            k2 = k * k
            ones = jnp.ones_like(k)
            whole = k2
            for _ in range(zs - 1):
                whole = whole * k2
            upper = lax.fori_loop(0, zs - 1 - z, lambda _, a: a * k2, ones)
            lower = lax.fori_loop(0, z, lambda _, a: a * k2, ones)
            close = lower * (ALPHA / (1.0 - ALPHA * whole))
            s.k1[j, rows] = k
            s.k2[j, rows] = k2
            s.pa[j, rows] = upper
            s.pb[j, rows] = close
            s.pf[j, rows] = 1.0 + close * (upper * k2)
            return 0

        lax.fori_loop(0, units, chain, 0)

    @pl.when(z == 0)
    def _():
        s.fin[...] = jnp.zeros_like(s.fin)

    @pl.when(z == zs - 1)
    def _():
        s.sin[...] = jnp.zeros_like(s.sin)

    for j in range(chunks):
        s.iy[0, j, 0:EDGE] = jnp.zeros((EDGE, steps * LANES), F32)
        s.iy[0, j, length + EDGE :] = jnp.zeros((EDGE, steps * LANES), F32)
    for k in range(s.tables.shape[0]):
        s.th[k], s.tl[k] = split(s.tables[k])

    s.w0p[EDGE : EDGE + strip] = s.w0[...]

    @pl.when(r > 0)
    def _():
        halo_down(r).wait_recv()
        s.w0p[0:EDGE] = s.halo[0]

    @pl.when(r == 0)
    def _():
        s.w0p[0:EDGE] = jnp.broadcast_to(s.w0[0:1], (EDGE, length))

    @pl.when(r < rows_count - 1)
    def _():
        halo_up(r).wait_recv()
        s.w0p[EDGE + strip :] = s.halo[1]

    @pl.when(r == rows_count - 1)
    def _():
        s.w0p[EDGE + strip :] = jnp.broadcast_to(s.w0[strip - 1 :], (EDGE, length))

    def kappa(offset):
        def part(start, size, i):
            rows = pl.ds(start, size)
            warmth = s.w0p[rows]
            if offset is not None:
                warmth = warmth + s.u1p[pl.ds(offset + start, size)]
            bent = s.slope[i : i + 1] * jnp.tanh(warmth)
            s.kp[rows] = s.base[i : i + 1] * (1.0 + bent)

        part(0, EDGE, 0)
        part(EDGE + strip, EDGE, blocks + 1)
        for b in range(blocks):

            def inner(i, _, b=b):
                part(pl.multiple_of(EDGE + b * TILE + i * ROWS, EDGE), ROWS, b + 1)
                return 0

            lax.fori_loop(0, TILE // ROWS, inner, 0)

    lane = lax.broadcasted_iota(jnp.int32, (ROWS, length), 1)
    ext = ROWS + 2 * EDGE

    def forcing(offset, out_row):
        def inner(i, _):
            rows = pl.ds(pl.multiple_of(i * ROWS, ROWS), ext)
            warmth, k = s.w0p[rows], s.kp[rows]
            mid = slice(EDGE, EDGE + ROWS)
            if offset is not None:
                u = s.u1p[pl.ds(pl.multiple_of(offset + i * ROWS, EDGE), ext)]
                warmth = warmth + u

            def flux(shift, w, k, u):
                value = 0.5 * (k + shift(k)) * (shift(w) - w)
                if u is not None:
                    value = value - conduct * (shift(u) - u)
                return value

            u = u if offset is not None else None
            down = flux(lambda v: pltpu.roll(v, ext - 1, 0), warmth, k, u)
            total = (down - pltpu.roll(down, 1, 0))[mid]
            right = flux(
                lambda v: pltpu.roll(v, length - 1, 1),
                warmth[mid],
                k[mid],
                None if u is None else u[mid],
            )
            right = jnp.where(lane < length - 1, right, 0.0)
            total = total + CROSS_WEIGHT * (right - pltpu.roll(right, 1, 1))
            home = pl.ds(pl.multiple_of(i * ROWS, ROWS), ROWS)
            if offset is None:
                s.div0[home] = total
            else:
                total = total - s.div0[home]
            rows = pl.ds(pl.multiple_of(out_row + i * ROWS, ROWS), ROWS)
            s.ph[rows], s.pl[rows] = split(total)
            return 0

        lax.fori_loop(0, strip // ROWS, inner, 0)

    kappa(None)
    forcing(None, 0)

    tables_in[0].wait()
    tables_in[1].wait()

    def send_d(k):
        return remote(
            s.dst.at[k],
            s.xd.at[rows_at(r * strip, strip)],
            s.ds.at[k],
            s.dr.at[k],
            (t, to(*peers[k])),
        )

    for k, peer in enumerate(peers + [(0, 0)]):
        columns = rows_at(to(*peer) * narrow, narrow)
        out = dot3(s.ph[0:strip], s.pl[0:strip], s.cth[:, columns], s.ctl[:, columns])
        if k < len(peers):
            s.dst[k] = out
            send_d(k).start()
        else:
            s.xd[rows_at(r * strip, strip)] = out

    own = rows_at(r * narrow, narrow)
    for n in range(steps):

        def place(ty, _, n=n):
            rows = rows_at(ty * TILE, TILE)
            for tx in range(tiles):
                picked = s.choice[n, ty, tx]
                s.ph[rows, tx * TILE : (tx + 1) * TILE] = s.th[picked]
                s.pl[rows, tx * TILE : (tx + 1) * TILE] = s.tl[picked]
            return 0

        lax.fori_loop(0, tiles, place, 0)

        def across(i, _, n=n):
            rows = rows_at(i * half, half)
            out = dot3(s.ph[rows], s.pl[rows], s.cth[:, own], s.ctl[:, own])
            high, low = split(out)
            for j in range(chunks):
                s.xh[j, rows, n * LANES : (n + 1) * LANES] = high[:, j * LANES : (j + 1) * LANES]
                s.xl[j, rows, n * LANES : (n + 1) * LANES] = low[:, j * LANES : (j + 1) * LANES]
            return 0

        lax.fori_loop(0, 2, across, 0)
    tables_in[2].wait()
    tables_in[3].wait()

    def unit(sweep, j, i):
        return (sweep * chunks + j) * units + i

    def send_e(sweep, j, i):
        n = unit(sweep, j, i)
        return remote(
            s.e.at[sweep, j, rows_at((1 - x) * half + i * LANES, LANES)],
            s.er.at[sweep, j, rows_at(i * LANES, LANES)],
            s.es.at[n],
            s.ers.at[n],
            (pair, r),
        )

    def send_f(sweep, j, i, device):
        n = unit(sweep, j, i)
        rows = rows_at(i * LANES, LANES)
        return remote(
            s.fout.at[sweep, j, rows], s.fin.at[sweep, j, rows], s.fs.at[n], s.frs.at[n], device
        )

    def send_s(sweep, j, i, device):
        n = unit(sweep, j, i)
        rows = rows_at(i * LANES, LANES)
        return remote(
            s.sout.at[sweep, j, rows], s.sin.at[sweep, j, rows], s.gs.at[n], s.grs.at[n], device
        )

    def send_c(sweep, j, i):
        n = unit(sweep, j, i)
        return remote(
            s.cs.at[sweep, j, rows_at(i * LANES, LANES)],
            s.carry.at[sweep, j, rows_at(x * half + i * LANES, LANES)],
            s.cts.at[n],
            s.crs.at[n],
            (pair, r),
        )

    is_first = jnp.where(t == 0, 1.0, 0.0)

    def rows_out(sweep, j):
        per = big // LANES
        parts = length // big

        def block(i, _):
            b = lax.rem(i + (1 - x) * (parts // 2), parts)
            rows = rows_at(b * big, big)
            out = dot3(s.ch[rows], s.cl[rows], s.xh[j], s.xl[j])
            gw, keep = s.gw[j, rows], s.keep[j, rows]
            first, second = out[:, :LANES] * gw, out[:, LANES:] * gw
            if sweep > 0:
                first = first - is_first * keep * s.ctot[j, rows]
            s.ss[j, rows, :LANES] = first
            s.ss[j, rows, LANES:] = second
            s.e[sweep, j, rows] = second + keep * first

            @pl.when(i < parts // 2)
            def _():
                for n in range(per):
                    send_e(sweep, j, i * per + n).start()

            return 0

        lax.fori_loop(0, parts, block, 0)

    def carries(sweep, j):
        def halves(i):
            mine = s.e[sweep, j, rows_at(x * half + i * LANES, LANES)]
            other = s.er[sweep, j, rows_at(i * LANES, LANES)]
            return jnp.where(x == 0, mine, other), jnp.where(x == 0, other, mine)

        def pairs(i, _):
            rows = rows_at(i * LANES, LANES)
            send_e(sweep, j, i).wait_recv()
            even, odd = halves(i)
            block = odd + s.k1[j, rows] * even
            s.zz[rows] = block

            @pl.when(z == 0)
            def _():
                s.fout[sweep, j, rows] = block
                send_f(sweep, j, i, (t + 2, r)).start()

            @pl.when(z == zs - 1)
            def _():
                s.sout[sweep, j, rows] = block
                send_s(sweep, j, i, (t - 2, r)).start()

            return 0

        lax.fori_loop(0, units, pairs, 0)

        def relay_f(i):
            rows = rows_at(i * LANES, LANES)

            @pl.when(z > 0)
            def _():
                send_f(sweep, j, i, (t, r)).wait_recv()

                @pl.when(z < zs - 1)
                def _():
                    s.fout[sweep, j, rows] = s.zz[rows] + s.k2[j, rows] * s.fin[sweep, j, rows]
                    send_f(sweep, j, i, (t + 2, r)).start()

        def relay_s(i):
            rows = rows_at(i * LANES, LANES)

            @pl.when(z < zs - 1)
            def _():
                send_s(sweep, j, i, (t, r)).wait_recv()
                s.sout[sweep, j, rows] = s.sin[sweep, j, rows] + s.pa[j, rows] * s.zz[rows]

                @pl.when(z > 0)
                def _():
                    send_s(sweep, j, i, (t - 2, r)).start()

        def finish(i):
            rows = rows_at(i * LANES, LANES)
            even, _ = halves(i)
            lower = s.fin[sweep, j, rows] * s.pf[j, rows] + s.pb[j, rows] * s.sout[sweep, j, rows]
            upper = even + s.k1[j, rows] * lower
            s.carry[sweep, j, rows_at(x * half + i * LANES, LANES)] = jnp.where(
                x == 0, lower, upper
            )
            s.cs[sweep, j, rows] = jnp.where(x == 0, upper, lower)
            send_c(sweep, j, i).start()

        def run(first, second):
            def one(i, _):
                first(i)
                return 0

            def two(i, _):
                second(i)
                finish(i)
                return 0

            lax.fori_loop(0, units, one, 0)
            lax.fori_loop(0, units, two, 0)

        @pl.when(z < zs // 2)
        def _():
            run(relay_f, relay_s)

        @pl.when(z >= zs // 2)
        def _():
            run(relay_s, relay_f)

    def send_y(sweep, j, k):
        n = (sweep * chunks + j) * len(peers) + k
        target = to(*peers[k])
        size = padded if sweep == 0 else strip
        start = target * strip if sweep == 0 else target * strip + EDGE
        return remote(
            s.iy.at[sweep, j, pl.ds(pl.multiple_of(start, EDGE), size)],
            s.yr.at[sweep, j, r, pl.ds(0, size)],
            s.ys.at[n],
            s.yrs.at[n],
            (t, target),
        )

    def rows_in(sweep, j):
        def wait(i, _):
            send_c(sweep, j, i).wait_recv()
            return 0

        lax.fori_loop(0, units, wait, 0)

        def solve(i, _):
            rows = rows_at(i * LANES, LANES)
            keep, carry = s.keep[j, rows], s.carry[sweep, j, rows]
            first, second = s.ss[j, rows, :LANES], s.ss[j, rows, LANES:]
            if sweep == 0:
                steady = s.sd[j, rows]
                first, second = first + steady, second + steady
                carry = carry + s.rho[j, rows] * steady
                s.ctot[j, rows] = carry
            first = first + keep * carry
            second = second + keep * first
            s.uh[rows, :LANES], s.ul[rows, :LANES] = split(first)
            s.uh[rows, LANES:], s.ul[rows, LANES:] = split(second)
            return 0

        lax.fori_loop(0, length // LANES, solve, 0)

        def block(target):
            rows = rows_at(target * strip, strip)
            out = dot3(s.cth[rows], s.ctl[rows], s.uh[...], s.ul[...])
            s.iy[sweep, j, pl.ds(pl.multiple_of(target * strip + EDGE, EDGE), strip)] = out

        if sweep == 0:

            def body(i, _):
                block(i)
                return 0

            lax.fori_loop(0, rows_count, body, 0)
            for k in range(len(peers)):
                send_y(sweep, j, k).start()
            s.yr[sweep, j, r] = s.iy[sweep, j, pl.ds(pl.multiple_of(r * strip, EDGE), padded)]
        else:
            for k, peer in enumerate(peers):
                block(to(*peer))
                send_y(sweep, j, k).start()
            block(r)
            mid = pl.ds(pl.multiple_of(r * strip + EDGE, EDGE), strip)
            s.yr[sweep, j, r, 0:strip] = s.iy[sweep, j, mid]

    def columns_in(sweep, j):
        for k in range(len(peers)):
            send_y(sweep, j, k).wait_recv()
        size = padded if sweep == 0 else strip
        for source in range(rows_count):
            high, low = split(s.yr[sweep, j, source, 0:size])
            lanes = slice(source * LANES, (source + 1) * LANES)
            for n in range(steps):
                part = slice(n * LANES, (n + 1) * LANES)
                s.lh[n * size : (n + 1) * size, lanes] = high[:, part]
                s.ll[n * size : (n + 1) * size, lanes] = low[:, part]

        def tile(i, _):
            columns = rows_at(i * big, big)

            def right(table):
                starts = [q * narrow + j * LANES for q in range(rows_count)]
                return jnp.concatenate([table[a : a + LANES, columns] for a in starts], 0)

            rows = slice(0, steps * size)
            out = dot3(s.lh[rows], s.ll[rows], right(s.ch), right(s.cl))
            if sweep == 0:
                if j > 0:
                    out = out + s.u1p[:, columns]
                s.u1p[:, columns] = out
            else:
                for n in range(steps):
                    value = out[n * size : (n + 1) * size]
                    if j == 0:
                        value = value + s.w0p[EDGE : EDGE + strip, columns]
                        value = value + s.u1p[n * padded + EDGE : n * padded + EDGE + strip, columns]
                    else:
                        value = value + s.out[n, :, columns]
                    s.out[n, :, columns] = value
            return 0

        lax.fori_loop(0, length // big, tile, 0)

    def send_x(j, k):
        n = j * len(peers) + k
        target = to(*peers[k])
        return remote(
            s.fx.at[j, target],
            s.xr.at[j, rows_at(r * strip, strip)],
            s.xs.at[n],
            s.xrs.at[n],
            (t, target),
        )

    def columns_out(j):
        for dy in list(range(1, ys_count)) + [0]:
            chip = lax.rem(y + dy, ys_count) * 2

            def right(table):
                starts = [rows_at((chip + q) * narrow + j * LANES, LANES) for q in range(2)]
                return jnp.concatenate([table[:, a] for a in starts], 1)

            rows = slice(0, steps * strip)
            out = dot3(s.ph[rows], s.pl[rows], right(s.cth), right(s.ctl))
            for q in range(2):
                for n in range(steps):
                    s.fx[j, chip + q, :, n * LANES : (n + 1) * LANES] = out[
                        n * strip : (n + 1) * strip, q * LANES : (q + 1) * LANES
                    ]
            for k, peer in enumerate(peers):
                if peer[0] == dy:
                    send_x(j, k).start()
        s.xr[j, rows_at(r * strip, strip)] = s.fx[j, r]

    def gather_x(j):
        for k in range(len(peers)):
            send_x(j, k).wait_recv()

        def body(i, _):
            rows = rows_at(i * LANES, LANES)
            s.xh[j, rows], s.xl[j, rows] = split(s.xr[j, rows])
            return 0

        lax.fori_loop(0, length // LANES, body, 0)

    def steady_modes():
        for k in range(len(peers)):
            send_d(k).wait_recv()

        def spread(i, _):
            rows = rows_at(i * LANES, LANES)
            s.xh[0, rows], s.xl[0, rows] = split(s.xd[rows])
            return 0

        lax.fori_loop(0, length // LANES, spread, 0)

        def block(i, _):
            rows = rows_at(i * big, big)
            out = dot3(s.ch[rows], s.cl[rows], s.xh[0], s.xl[0])
            for j in range(chunks):
                s.sd[j, rows] = out[:, j * LANES : (j + 1) * LANES] * s.gw[j, rows]
            return 0

        lax.fori_loop(0, length // big, block, 0)

    for j in range(chunks):
        rows_out(0, j)
    carries(0, 0)
    steady_modes()
    for j in range(chunks):
        if j > 0:
            carries(0, j)
        rows_in(0, j)
    for j in range(chunks):
        columns_in(0, j)
    for n in range(steps):
        offset = n * padded

        @pl.when(r == 0)
        def _():
            edge = s.u1p[offset + EDGE : offset + EDGE + 1]
            s.u1p[offset : offset + EDGE] = jnp.broadcast_to(edge, (EDGE, length))

        @pl.when(r == rows_count - 1)
        def _():
            last = offset + EDGE + strip
            edge = s.u1p[last - 1 : last]
            s.u1p[last : last + EDGE] = jnp.broadcast_to(edge, (EDGE, length))

        kappa(offset)
        forcing(offset, n * strip)
    for j in range(chunks):
        columns_out(j)
    gather_x(0)
    rows_out(1, 0)
    for j in range(chunks):
        carries(1, j)
        if j + 1 < chunks:
            gather_x(j + 1)
            rows_out(1, j + 1)
        rows_in(1, j)
    for j in range(chunks):
        columns_in(1, j)

    @pl.when(r < rows_count - 1)
    def _():
        halo_down(r + 1).wait_send()

    @pl.when(r > 0)
    def _():
        halo_up(r - 1).wait_send()

    for k in range(len(peers)):
        send_d(k).wait_send()
        for j in range(chunks):
            send_x(j, k).wait_send()
            for sweep in range(ITERS):
                send_y(sweep, j, k).wait_send()
    for sweep in range(ITERS):
        for j in range(chunks):

            def drain(i, _, sweep=sweep, j=j):
                send_e(sweep, j, i).wait_send()
                send_c(sweep, j, i).wait_send()

                @pl.when(z < zs - 1)
                def _():
                    send_f(sweep, j, i, (t + 2, r)).wait_send()

                @pl.when(z > 0)
                def _():
                    send_s(sweep, j, i, (t - 2, r)).wait_send()

                return 0

            lax.fori_loop(0, units, drain, 0)


def fused(
    initial_warmth,
    pattern_choice,
    dissipation_tables,
    material_label,
    intercept_kappa,
    sensitivity_coef,
):
    steps = pattern_choice.shape[0]
    strip, length = initial_warmth.shape
    tm_count, rows_count = lax.axis_size("tm"), lax.axis_size("rows")
    chunks = length // rows_count // LANES
    column_cos = cosine_table(length)
    forward, inverse = two_parts(column_cos.T), two_parts(column_cos)
    mu = 2.0 - 2.0 * np.cos(np.arange(length) * (math.pi / length))
    mup = np.broadcast_to(mu[:, None], (length, LANES)).astype(np.float32)
    muq = np.broadcast_to(mu.reshape(rows_count * chunks, 1, LANES), (rows_count * chunks, 8, LANES))
    scratch = scratch_of(steps, strip, length, tm_count, rows_count)
    names = INPUTS + ["out"] + list(scratch)
    smem, vmem, hbm = (
        pl.BlockSpec(memory_space=space) for space in (pltpu.SMEM, pltpu.VMEM, pl.ANY)
    )
    return pl.pallas_call(
        lambda *refs: fused_kernel(steps, strip, length, tm_count, rows_count, names, *refs),
        out_shape=jax.ShapeDtypeStruct((steps, strip, length), F32),
        in_specs=[vmem, smem, vmem, smem, smem, smem, vmem, vmem] + [hbm] * 4,
        out_specs=vmem,
        scratch_shapes=list(scratch.values()),
        compiler_params=pltpu.CompilerParams(
            collective_id=0, has_side_effects=True, vmem_limit_bytes=67043328
        ),
    )(
        initial_warmth,
        pattern_choice,
        dissipation_tables,
        material_label,
        intercept_kappa,
        sensitivity_coef,
        jnp.asarray(mup),
        jnp.asarray(muq.astype(np.float32)),
        *inverse,
        *forward,
    )


def pick(initial_warmth, pattern_choice, *rest):
    strip, width = initial_warmth.shape
    tm_count, rows_count = lax.axis_size("tm"), lax.axis_size("rows")
    aligned = (
        pattern_choice.shape[0] == 2
        and strip * rows_count == width
        and strip % TILE == 0
        and width == rows_count * 2 * LANES
        and width % (4 * LANES) == 0
        and tm_count % 2 == 0
        and rows_count % 2 == 0
    )
    return (fused if aligned else shards)(initial_warmth, pattern_choice, *rest)


def solution(mesh):
    in_specs = (P("rows", None), P("tm", None, None), P(), P(), P(), P())
    out_specs = P("tm", "rows", None)
    return jax.shard_map(pick, mesh=mesh, in_specs=in_specs, out_specs=out_specs, check_vma=False)
```

```python
import math
from types import SimpleNamespace

import jax
import jax.numpy as jnp
import numpy as np
from jax import lax
from jax.experimental import pallas as pl
from jax.experimental.pallas import tpu as pltpu
from jax.sharding import PartitionSpec as P

TILE = 128
ITERS = 2
TIMESTEP_SIZE = 2.0
ALPHA = 0.05
CROSS_WEIGHT = 1.0 / 64.0
F32 = jnp.float32
BF16 = jnp.bfloat16


def extended(block, axis, dim):
    count = lax.axis_size(axis)
    forward = [(i, i + 1) for i in range(count - 1)]
    backward = [(target, source) for source, target in forward]
    low = lax.ppermute(
        lax.slice_in_dim(block, block.shape[dim] - 1, None, axis=dim), axis, forward
    )
    high = lax.ppermute(lax.slice_in_dim(block, 0, 1, axis=dim), axis, backward)
    return jnp.concatenate([low, block, high], axis=dim)


def cosine_table(length):
    modes = np.arange(length, dtype=np.int64)[:, None]
    cells = np.arange(length, dtype=np.int64)[None, :]
    phase = modes * (2 * cells + 1) % (4 * length)
    return np.cos(phase * (math.pi / (2 * length)))


def two_parts(table):
    high = np.asarray(table, dtype=np.float32).astype(BF16)
    low = (table - high.astype(np.float64)).astype(np.float32).astype(BF16)
    return jnp.asarray(high), jnp.asarray(low)


def split(values):
    high = values.astype(BF16)
    return high, (values - high.astype(F32)).astype(BF16)


def mul(left, right):
    return jnp.dot(left, right, preferred_element_type=F32)


def columns_kernel(x_ref, high_ref, low_ref, out_ref, x_high, x_low):
    @pl.when(pl.program_id(0) == 0)
    def _():
        x_high[...], x_low[...] = split(x_ref[...])

    high = high_ref[...]
    out_ref[...] = (
        mul(x_high[...], high) + mul(x_low[...], high) + mul(x_high[...], low_ref[...])
    )


def times_table(values, table):
    rows, depth = values.shape
    width = table[0].shape[1]
    block = min(256, width)
    return pl.pallas_call(
        columns_kernel,
        grid=(width // block,),
        out_shape=jax.ShapeDtypeStruct((rows, width), F32),
        in_specs=[
            pl.BlockSpec((rows, depth), lambda i: (0, 0)),
            pl.BlockSpec((depth, block), lambda i: (0, i)),
            pl.BlockSpec((depth, block), lambda i: (0, i)),
        ],
        out_specs=pl.BlockSpec((rows, block), lambda i: (0, i)),
        scratch_shapes=[pltpu.VMEM((rows, depth), BF16)] * 2,
    )(values, *table)


def rows_kernel(high_ref, low_ref, x_ref, out_ref, x_high, x_low):
    @pl.when(pl.program_id(0) == 0)
    def _():
        x_high[...], x_low[...] = split(x_ref[...])

    for n in range(x_ref.shape[0]):
        out_ref[n] = (
            mul(high_ref[...], x_high[n])
            + mul(high_ref[...], x_low[n])
            + mul(low_ref[...], x_high[n])
        )


def table_times(table, values):
    steps, depth, width = values.shape
    height = table[0].shape[0]
    block = min(256, height)
    return pl.pallas_call(
        rows_kernel,
        grid=(height // block,),
        out_shape=jax.ShapeDtypeStruct((steps, height, width), F32),
        in_specs=[
            pl.BlockSpec((block, depth), lambda i: (i, 0)),
            pl.BlockSpec((block, depth), lambda i: (i, 0)),
            pl.BlockSpec((steps, depth, width), lambda i: (0, 0, 0)),
        ],
        out_specs=pl.BlockSpec((steps, block, width), lambda i: (0, i, 0)),
        scratch_shapes=[pltpu.VMEM((steps, depth, width), BF16)] * 2,
    )(*table, values)


def power_kernel(choice_ref, table_ref, out_ref):
    steps, blocks, _, width = out_ref.shape
    across = width // TILE
    for n in range(steps):
        for b in range(blocks):
            for x in range(across):
                picked = choice_ref[n, b * across + x]
                out_ref[n, b, :, x * TILE : (x + 1) * TILE] = table_ref[picked]


def power_of(pattern_choice, tables, first_row, strip, width):
    steps = pattern_choice.shape[0]
    part = min(TILE, strip)
    blocks = strip // part
    offset = first_row % TILE if strip < TILE else 0
    tiles = lax.dynamic_slice_in_dim(tables, offset, part, axis=1)
    chosen = lax.dynamic_slice_in_dim(pattern_choice, first_row // TILE, blocks, axis=1)
    power = pl.pallas_call(
        power_kernel,
        out_shape=jax.ShapeDtypeStruct((steps, blocks, part, width), F32),
        in_specs=[
            pl.BlockSpec(memory_space=pltpu.SMEM),
            pl.BlockSpec(memory_space=pltpu.VMEM),
        ],
        out_specs=pl.BlockSpec(memory_space=pltpu.VMEM),
    )(chosen.reshape(steps, -1), tiles)
    return power.reshape(steps, strip, width)


def divergence(warmth, kappa, inner):
    def face(low, high):
        return 1.0 if kappa is None else 0.5 * (low + high)

    k = warmth if kappa is None else kappa
    upward = face(k[:, 1:], k[:, :-1]) * (warmth[:, 1:] - warmth[:, :-1])
    upward = jnp.where(inner[None, :, None], upward, 0.0)
    centre, k_mid = warmth[:, 1:-1], k[:, 1:-1]
    lateral = CROSS_WEIGHT * (
        face(k_mid[:, :, 1:], k_mid[:, :, :-1]) * (centre[:, :, 1:] - centre[:, :, :-1])
    )
    zero = jnp.zeros_like(centre[:, :, :1])
    across = jnp.concatenate([lateral, zero], 2) - jnp.concatenate([zero, lateral], 2)
    return upward[:, 1:] - upward[:, :-1] + across


def mode_factors(row_ids, column_ids, height, width, conduct):
    mu_rows = 2.0 - 2.0 * jnp.cos(row_ids.astype(F32) * (math.pi / height))
    mu_cols = 2.0 - 2.0 * jnp.cos(column_ids.astype(F32) * (math.pi / width))
    rate = conduct * (mu_rows[:, None] + CROSS_WEIGHT * mu_cols[None, :])
    gain = 1.0 / (1.0 / TIMESTEP_SIZE + rate)
    return gain, gain * (1.0 / TIMESTEP_SIZE)


def shards(
    initial_warmth,
    pattern_choice,
    dissipation_tables,
    material_label,
    intercept_kappa,
    sensitivity_coef,
):
    steps = pattern_choice.shape[0]
    strip, width = initial_warmth.shape
    tm_count = lax.axis_size("tm")
    rows_count = lax.axis_size("rows")
    height = strip * rows_count
    first_row = lax.axis_index("rows") * strip
    power = power_of(pattern_choice, dissipation_tables, first_row, strip, width)

    padded_rows = first_row - 1 + jnp.arange(strip + 2, dtype=jnp.int32)
    labels = jnp.take(material_label, jnp.clip(padded_rows, 0, height - 1) // TILE, axis=0)
    base_tiles = jnp.zeros(labels.shape, F32)
    slope_tiles = jnp.zeros(labels.shape, F32)
    for label in range(intercept_kappa.shape[0]):
        base_tiles = jnp.where(labels == label, intercept_kappa[label], base_tiles)
        slope_tiles = jnp.where(labels == label, sensitivity_coef[label], slope_tiles)
    base = jnp.repeat(base_tiles, TILE, axis=1)[None]
    slope = jnp.repeat(slope_tiles, TILE, axis=1)[None]
    upper_rows = padded_rows[:-1]
    inner = (upper_rows >= 0) & (upper_rows + 1 <= height - 1)
    conduct = jnp.mean(intercept_kappa)

    column_cos = cosine_table(width)
    row_cos = cosine_table(height)
    columns_out, columns_in = two_parts(column_cos.T), two_parts(column_cos)
    if height == width:
        rows_out, rows_in = columns_in, columns_out
    else:
        rows_out, rows_in = two_parts(row_cos), two_parts(row_cos.T)

    narrow = width // rows_count
    share = height // tm_count
    column_ids = lax.axis_index("rows") * narrow + jnp.arange(narrow, dtype=jnp.int32)
    all_rows = jnp.arange(height, dtype=jnp.int32)
    own_rows = lax.axis_index("tm") * share + jnp.arange(share, dtype=jnp.int32)
    gain, keep = mode_factors(all_rows, column_ids, height, width, conduct)
    weight = (jnp.where(all_rows == 0, 1.0, 2.0) / height)[:, None] * (
        jnp.where(column_ids == 0, 1.0, 2.0) / width
    )[None, :]
    _, own_keep = mode_factors(own_rows, column_ids, height, width, conduct)
    block_keep = own_keep
    for _ in range(steps - 1):
        block_keep = block_keep * own_keep
    around = block_keep
    for _ in range(tm_count - 1):
        around = around * block_keep
    closing = ALPHA / (1.0 - ALPHA * around)
    first_block = lax.axis_index("tm") == 0

    start = extended(initial_warmth[None], "rows", 1)
    start_div = divergence(start, base * (1.0 + slope * jnp.tanh(start)), inner)
    warmth = jnp.broadcast_to(initial_warmth[None], (steps, strip, width))
    wrapped = None
    for sweep in range(ITERS):
        if sweep == 0:
            resid = power + start_div
        else:
            grid = extended(warmth, "rows", 1)
            div = divergence(grid, base * (1.0 + slope * jnp.tanh(grid)), inner)
            resid = div - last_div - conduct * divergence(grid - last_grid, None, inner)
        modes = times_table(resid.reshape(steps * strip, width), columns_out)
        modes = lax.all_to_all(
            modes.reshape(steps, strip, width), "rows", split_axis=2, concat_axis=1, tiled=True
        )
        modes = table_times(rows_out, modes)
        sources = [modes[n] * weight for n in range(steps)]
        if wrapped is not None:
            sources[0] = sources[0] - jnp.where(first_block, wrapped / TIMESTEP_SIZE, 0.0)
        sources = [gain * source for source in sources]
        block_end = sources[0]
        for source in sources[1:]:
            block_end = source + keep * block_end
        ends = lax.all_to_all(block_end, "tm", split_axis=0, concat_axis=0, tiled=True)
        ends = ends.reshape(tm_count, share, narrow)
        last = ends[0]
        for k in range(1, tm_count):
            last = ends[k] + block_keep * last
        entry = [closing * last]
        for k in range(tm_count - 1):
            entry.append(ends[k] + block_keep * entry[k])
        entry = jnp.concatenate(entry, 0)
        carry = lax.all_to_all(entry, "tm", split_axis=0, concat_axis=0, tiled=True)
        wrapped = carry
        solved = []
        for source in sources:
            carry = source + keep * carry
            solved.append(carry)
        field = table_times(rows_in, jnp.stack(solved, 0))
        field = lax.all_to_all(field, "rows", split_axis=1, concat_axis=2, tiled=True)
        update = times_table(field.reshape(steps * strip, width), columns_in)
        if sweep == 0:
            last_grid, last_div = start, start_div
        else:
            last_grid, last_div = grid, div
        warmth = warmth + update.reshape(steps, strip, width)
    return warmth


LANES = 128
EDGE = 8
ROWS = 32
UNIT = 64
MESH = pl.DeviceIdType.MESH


def dot3(left_high, left_low, right_high, right_low):
    return mul(left_high, right_high) + mul(left_low, right_high) + mul(left_high, right_low)


def remote(src, dst, send_sem, recv_sem, device):
    return pltpu.make_async_remote_copy(
        src_ref=src,
        dst_ref=dst,
        send_sem=send_sem,
        recv_sem=recv_sem,
        device_id=device,
        device_id_type=MESH,
    )


def scratch_of(steps, strip, length, tm_count, rows_count):
    narrow = length // rows_count
    chunks = narrow // LANES
    half = length // 2
    units = half // UNIT
    wide = steps * LANES
    padded = strip + 2 * EDGE

    def f32(*shape):
        return pltpu.VMEM(shape, F32)

    def b16(*shape):
        return pltpu.VMEM(shape, BF16)

    dma = pltpu.SemaphoreType.DMA
    return dict(
        ch=b16(length, length),
        cl=b16(length, length),
        cth=b16(length, length),
        ctl=b16(length, length),
        ph=b16(length, length),
        pl=b16(length, length),
        th=b16(8, TILE, TILE),
        tl=b16(8, TILE, TILE),
        base=f32(8, length),
        slope=f32(8, length),
        w0p=f32(padded, length),
        kp=f32(padded, length),
        div0=f32(strip, length),
        halo=f32(2, EDGE, length),
        dst=f32(rows_count, strip, narrow),
        oh=b16(length, narrow),
        ol=b16(length, narrow),
        xd=f32(length, narrow),
        xh=b16(chunks, length, wide),
        xl=b16(chunks, length, wide),
        fx=f32(chunks, rows_count, strip, wide),
        xr=f32(chunks, length, wide),
        ss=f32(chunks, length, wide),
        e=f32(ITERS, chunks, length, LANES),
        er=f32(ITERS, chunks, half, LANES),
        fin=f32(ITERS, chunks, half, LANES),
        sin=f32(ITERS, chunks, half, LANES),
        fout=f32(ITERS, chunks, half, LANES),
        sout=f32(ITERS, chunks, half, LANES),
        cs=f32(ITERS, chunks, half, LANES),
        zz=f32(chunks, half, LANES),
        carry=f32(ITERS, chunks, length, LANES),
        ctot=f32(chunks, length, LANES),
        gw=f32(chunks, length, LANES),
        keep=f32(chunks, length, LANES),
        rho=f32(chunks, length, LANES),
        sd=f32(chunks, length, LANES),
        k1=f32(chunks, half, LANES),
        k2=f32(chunks, half, LANES),
        pa=f32(chunks, half, LANES),
        pb=f32(chunks, half, LANES),
        pf=f32(chunks, half, LANES),
        iy=f32(ITERS, chunks, length + 2 * EDGE, wide),
        yr=f32(ITERS, chunks, rows_count, padded, wide),
        uh=b16(length, wide),
        ul=b16(length, wide),
        lh=b16(steps * padded, rows_count * LANES),
        ll=b16(steps * padded, rows_count * LANES),
        u1p=f32(steps * padded, length),
        outv=f32(steps, strip, length),
        osem=dma((length // (2 * LANES),)),
        tsem=dma((4,)),
        hs=dma((2,)),
        hr=dma((2,)),
        ds=dma((rows_count,)),
        dr=dma((rows_count,)),
        xs=dma((chunks * rows_count,)),
        xrs=dma((chunks * rows_count,)),
        ys=dma((ITERS * chunks * rows_count,)),
        yrs=dma((ITERS * chunks * rows_count,)),
        es=dma((ITERS * chunks * units,)),
        ers=dma((ITERS * chunks * units,)),
        fs=dma((ITERS * chunks * units,)),
        frs=dma((ITERS * chunks * units,)),
        gs=dma((ITERS * chunks * units,)),
        grs=dma((ITERS * chunks * units,)),
        cts=dma((ITERS * chunks * units,)),
        crs=dma((ITERS * chunks * units,)),
    )


INPUTS = [
    "w0",
    "choice",
    "tables",
    "label",
    "icpt",
    "sens",
    "mup",
    "muq",
    "chh",
    "clh",
    "cthh",
    "ctlh",
]


def fused_kernel(steps, strip, length, tm_count, rows_count, names, *refs):
    s = SimpleNamespace(**dict(zip(names, refs)))
    narrow = length // rows_count
    chunks = narrow // LANES
    half = length // 2
    units = half // UNIT
    padded = strip + 2 * EDGE
    blocks = strip // TILE
    tiles = length // TILE
    big = 2 * LANES
    zs, ys_count = tm_count // 2, rows_count // 2

    t, r = lax.axis_index("tm"), lax.axis_index("rows")
    z, x = lax.div(t, 2), lax.rem(t, 2)
    y, c = lax.div(r, 2), lax.rem(r, 2)
    pair = t + 1 - 2 * x
    peers = [(dy, dc) for dy in range(1, ys_count) for dc in range(2)] + [(0, 1)]

    def to(dy, dc):
        return lax.rem(y + dy, ys_count) * 2 + lax.rem(c + dc, 2)

    def frm(dy, dc):
        return lax.rem(y + ys_count - dy, ys_count) * 2 + lax.rem(c + 2 - dc, 2)

    def rows_at(start, size):
        return pl.ds(pl.multiple_of(start, size), size)

    tables_in = [
        pltpu.make_async_copy(a, b, s.tsem.at[i])
        for i, (a, b) in enumerate(
            [(s.cthh, s.cth), (s.ctlh, s.ctl), (s.chh, s.ch), (s.clh, s.cl)]
        )
    ]
    for copy in tables_in:
        copy.start()

    barrier = pltpu.get_barrier_semaphore()
    for dy, dc in peers:
        pl.semaphore_signal(barrier, inc=1, device_id=(t, to(dy, dc)), device_id_type=MESH)
    pl.semaphore_signal(barrier, inc=1, device_id=(pair, r), device_id_type=MESH)

    @pl.when(z > 0)
    def _():
        pl.semaphore_signal(barrier, inc=1, device_id=(t - 2, r), device_id_type=MESH)

    @pl.when(z < zs - 1)
    def _():
        pl.semaphore_signal(barrier, inc=1, device_id=(t + 2, r), device_id_type=MESH)

    def halo_down(to_row):
        return remote(
            s.w0.at[pl.ds(strip - EDGE, EDGE)], s.halo.at[0], s.hs.at[0], s.hr.at[0], (t, to_row)
        )

    def halo_up(to_row):
        return remote(s.w0.at[pl.ds(0, EDGE)], s.halo.at[1], s.hs.at[1], s.hr.at[1], (t, to_row))

    count = s.icpt.shape[0]
    total = s.icpt[0]
    for i in range(1, count):
        total = total + s.icpt[i]
    conduct = total / count
    for i in range(blocks + 2):
        ty = lax.min(lax.max(r * blocks - 1 + i, 0), tiles - 1)
        for tx in range(tiles):
            label = s.label[ty, tx]
            s.base[i : i + 1, tx * TILE : (tx + 1) * TILE] = jnp.full((1, TILE), s.icpt[label], F32)
            s.slope[i : i + 1, tx * TILE : (tx + 1) * TILE] = jnp.full((1, TILE), s.sens[label], F32)

    for j in range(chunks):

        def factors(i, _, j=j):
            rows = rows_at(i * LANES, LANES)
            rate = conduct * (s.mup[rows] + CROSS_WEIGHT * s.muq[j * rows_count + r, 0:1, :])
            gain = 1.0 / (1.0 / TIMESTEP_SIZE + rate)
            keep = gain * (1.0 / TIMESTEP_SIZE)
            p = i * LANES + lax.broadcasted_iota(jnp.int32, (LANES, LANES), 0)
            q = (j * rows_count + r) * LANES + lax.broadcasted_iota(jnp.int32, (LANES, LANES), 1)
            weight = (jnp.where(p == 0, 1.0, 2.0) / length) * (jnp.where(q == 0, 1.0, 2.0) / length)
            s.gw[j, rows] = gain * weight
            s.keep[j, rows] = keep
            one = 1.0 + keep
            k = keep * keep
            around, power = one, k
            for _ in range(tm_count - 1):
                around = one + k * around
                power = power * k
            first = ALPHA * around / (1.0 - ALPHA * power)
            s.rho[j, rows] = lax.fori_loop(0, t, lambda _, a: one + k * a, first)
            return 0

        lax.fori_loop(0, length // LANES, factors, 0)

        def chain(i, _, j=j):
            rows = rows_at(i * UNIT, UNIT)
            keep = s.keep[j, rows_at(x * half + i * UNIT, UNIT)]
            k = keep * keep
            k2 = k * k
            ones = jnp.ones_like(k)
            whole = k2
            for _ in range(zs - 1):
                whole = whole * k2
            upper = lax.fori_loop(0, zs - 1 - z, lambda _, a: a * k2, ones)
            lower = lax.fori_loop(0, z, lambda _, a: a * k2, ones)
            close = lower * (ALPHA / (1.0 - ALPHA * whole))
            s.k1[j, rows] = k
            s.k2[j, rows] = k2
            s.pa[j, rows] = upper
            s.pb[j, rows] = close
            s.pf[j, rows] = 1.0 + close * (upper * k2)
            return 0

        lax.fori_loop(0, units, chain, 0)

    @pl.when(z == 0)
    def _():
        s.fin[...] = jnp.zeros_like(s.fin)

    @pl.when(z == zs - 1)
    def _():
        s.sin[...] = jnp.zeros_like(s.sin)

    for j in range(chunks):
        s.iy[0, j, 0:EDGE] = jnp.zeros((EDGE, steps * LANES), F32)
        s.iy[0, j, length + EDGE :] = jnp.zeros((EDGE, steps * LANES), F32)
    for k in range(s.tables.shape[0]):
        s.th[k], s.tl[k] = split(s.tables[k])

    def kappa(offset):
        def part(start, size, i):
            rows = pl.ds(start, size)
            warmth = s.w0p[rows]
            if offset is not None:
                warmth = warmth + s.u1p[pl.ds(pl.multiple_of(offset + start, EDGE), size)]
            bent = s.slope[i : i + 1] * jnp.tanh(warmth)
            s.kp[rows] = s.base[i : i + 1] * (1.0 + bent)

        part(0, EDGE, 0)
        part(EDGE + strip, EDGE, blocks + 1)
        for b in range(blocks):

            def inner(i, _, b=b):
                part(pl.multiple_of(EDGE + b * TILE + i * ROWS, EDGE), ROWS, b + 1)
                return 0

            lax.fori_loop(0, TILE // ROWS, inner, 0)

    lane = lax.broadcasted_iota(jnp.int32, (ROWS, length), 1)
    ext = ROWS + 2 * EDGE

    def forcing(offset, out_row):
        def inner(i, _):
            rows = pl.ds(pl.multiple_of(i * ROWS, ROWS), ext)
            warmth, k = s.w0p[rows], s.kp[rows]
            mid = slice(EDGE, EDGE + ROWS)
            if offset is not None:
                u = s.u1p[pl.ds(pl.multiple_of(offset + i * ROWS, EDGE), ext)]
                warmth = warmth + u

            def flux(shift, w, k, u):
                value = 0.5 * (k + shift(k)) * (shift(w) - w)
                if u is not None:
                    value = value - conduct * (shift(u) - u)
                return value

            u = u if offset is not None else None
            down = flux(lambda v: pltpu.roll(v, ext - 1, 0), warmth, k, u)
            total = (down - pltpu.roll(down, 1, 0))[mid]
            right = flux(
                lambda v: pltpu.roll(v, length - 1, 1),
                warmth[mid],
                k[mid],
                None if u is None else u[mid],
            )
            right = jnp.where(lane < length - 1, right, 0.0)
            total = total + CROSS_WEIGHT * (right - pltpu.roll(right, 1, 1))
            home = pl.ds(pl.multiple_of(i * ROWS, ROWS), ROWS)
            if offset is None:
                s.div0[home] = total
            else:
                total = total - s.div0[home]
            rows = pl.ds(pl.multiple_of(out_row + i * ROWS, ROWS), ROWS)
            s.ph[rows], s.pl[rows] = split(total)
            return 0

        lax.fori_loop(0, strip // ROWS, inner, 0)

    def send_d(dy, dc):
        n, target = dy * 2 + dc, to(dy, dc)
        rows = rows_at(r * strip, strip)
        return remote(s.dst.at[target], s.xd.at[rows], s.ds.at[n], s.dr.at[n], (t, target))

    beside = lax.min(z, 1) + lax.min(zs - 1 - z, 1)
    pl.semaphore_wait(barrier, len(peers) + 1 + beside)

    @pl.when(r < rows_count - 1)
    def _():
        halo_down(r + 1).start()

    @pl.when(r > 0)
    def _():
        halo_up(r - 1).start()

    tables_in[0].wait()
    tables_in[1].wait()

    for j in range(chunks):
        columns = rows_at((j * rows_count + r) * LANES, LANES)
        s.oh[:, j * LANES : (j + 1) * LANES] = s.cth[:, columns]
        s.ol[:, j * LANES : (j + 1) * LANES] = s.ctl[:, columns]

    def power(n, _):
        def place(ty, _):
            rows = rows_at(ty * TILE, TILE)
            for tx in range(tiles):
                picked = s.choice[n, ty, tx]
                s.ph[rows, tx * TILE : (tx + 1) * TILE] = s.th[picked]
                s.pl[rows, tx * TILE : (tx + 1) * TILE] = s.tl[picked]
            return 0

        lax.fori_loop(0, tiles, place, 0)

        def across(i, _):
            rows = rows_at(i * half, half)
            out = dot3(s.ph[rows], s.pl[rows], s.oh[...], s.ol[...])
            high, low = split(out)
            lanes = rows_at(n * LANES, LANES)
            for j in range(chunks):
                s.xh[j, rows, lanes] = high[:, j * LANES : (j + 1) * LANES]
                s.xl[j, rows, lanes] = low[:, j * LANES : (j + 1) * LANES]
            return 0

        lax.fori_loop(0, 2, across, 0)
        return 0

    lax.fori_loop(0, steps, power, 0)
    tables_in[2].wait()
    tables_in[3].wait()

    def unit(sweep, j, i):
        return (sweep * chunks + j) * units + i

    def send_e(sweep, j, i):
        n = unit(sweep, j, i)
        return remote(
            s.e.at[sweep, j, rows_at((1 - x) * half + i * UNIT, UNIT)],
            s.er.at[sweep, j, rows_at(i * UNIT, UNIT)],
            s.es.at[n],
            s.ers.at[n],
            (pair, r),
        )

    def send_f(sweep, j, i, device):
        n = unit(sweep, j, i)
        rows = rows_at(i * UNIT, UNIT)
        return remote(
            s.fout.at[sweep, j, rows], s.fin.at[sweep, j, rows], s.fs.at[n], s.frs.at[n], device
        )

    def send_s(sweep, j, i, device):
        n = unit(sweep, j, i)
        rows = rows_at(i * UNIT, UNIT)
        return remote(
            s.sout.at[sweep, j, rows], s.sin.at[sweep, j, rows], s.gs.at[n], s.grs.at[n], device
        )

    def send_c(sweep, j, i):
        n = unit(sweep, j, i)
        return remote(
            s.cs.at[sweep, j, rows_at(i * UNIT, UNIT)],
            s.carry.at[sweep, j, rows_at(x * half + i * UNIT, UNIT)],
            s.cts.at[n],
            s.crs.at[n],
            (pair, r),
        )

    is_first = jnp.where(t == 0, 1.0, 0.0)

    def rows_out(sweep, j, action=None, beside_j=0):
        parts = length // big
        per = big // UNIT

        def part(i, _):
            rows = rows_at(lax.rem(i + (1 - x) * (parts // 2), parts) * big, big)
            out = dot3(s.ch[rows], s.cl[rows], s.xh[j], s.xl[j])
            gw, keep = s.gw[j, rows], s.keep[j, rows]
            first, second = out[:, :LANES] * gw, out[:, LANES:] * gw
            if sweep > 0:
                first = first - is_first * keep * s.ctot[j, rows]
            s.ss[j, rows, :LANES] = first
            s.ss[j, rows, LANES:] = second
            s.e[sweep, j, rows] = second + keep * first

            @pl.when(i < parts // 2)
            def _():
                for n in range(per):
                    send_e(sweep, j, i * per + n).start()

            share(action, sweep, beside_j, i, parts)
            return 0

        lax.fori_loop(0, parts, part, 0)

    def halves(sweep, j, i):
        mine = s.e[sweep, j, rows_at(x * half + i * UNIT, UNIT)]
        other = s.er[sweep, j, rows_at(i * UNIT, UNIT)]
        return jnp.where(x == 0, mine, other), jnp.where(x == 0, other, mine)

    def repeat(sweep, j, *actions):
        def body(i, _):
            for action in actions:
                action(sweep, j, i)
            return 0

        lax.fori_loop(0, units, body, 0)

    def pair_up(sweep, j, i):
        rows = rows_at(i * UNIT, UNIT)
        send_e(sweep, j, i).wait_recv()
        even, odd = halves(sweep, j, i)
        block = odd + s.k1[j, rows] * even
        s.zz[j, rows] = block

        @pl.when(z == 0)
        def _():
            s.fout[sweep, j, rows] = block
            send_f(sweep, j, i, (t + 2, r)).start()

        @pl.when(z == zs - 1)
        def _():
            s.sout[sweep, j, rows] = block
            send_s(sweep, j, i, (t - 2, r)).start()

    def relay_f(sweep, j, i):
        rows = rows_at(i * UNIT, UNIT)

        @pl.when(z > 0)
        def _():
            send_f(sweep, j, i, (t, r)).wait_recv()

            @pl.when(z < zs - 1)
            def _():
                s.fout[sweep, j, rows] = s.zz[j, rows] + s.k2[j, rows] * s.fin[sweep, j, rows]
                send_f(sweep, j, i, (t + 2, r)).start()

    def relay_s(sweep, j, i):
        rows = rows_at(i * UNIT, UNIT)

        @pl.when(z < zs - 1)
        def _():
            send_s(sweep, j, i, (t, r)).wait_recv()
            s.sout[sweep, j, rows] = s.sin[sweep, j, rows] + s.pa[j, rows] * s.zz[j, rows]

            @pl.when(z > 0)
            def _():
                send_s(sweep, j, i, (t - 2, r)).start()

    def finish(sweep, j, i):
        rows = rows_at(i * UNIT, UNIT)
        even, _ = halves(sweep, j, i)
        lower = s.fin[sweep, j, rows] * s.pf[j, rows] + s.pb[j, rows] * s.sout[sweep, j, rows]
        upper = even + s.k1[j, rows] * lower
        s.carry[sweep, j, rows_at(x * half + i * UNIT, UNIT)] = jnp.where(x == 0, lower, upper)
        s.cs[sweep, j, rows] = jnp.where(x == 0, upper, lower)
        send_c(sweep, j, i).start()

    def relay_near(sweep, j, i):
        @pl.when(z < zs // 2)
        def _():
            relay_f(sweep, j, i)

        @pl.when(z >= zs // 2)
        def _():
            relay_s(sweep, j, i)

    def relay_away(sweep, j, i):
        @pl.when(z < zs // 2)
        def _():
            relay_s(sweep, j, i)

        @pl.when(z >= zs // 2)
        def _():
            relay_f(sweep, j, i)

        finish(sweep, j, i)

    def some(action, sweep, j, first, last):
        def body(i, _):
            action(sweep, j, i)
            return 0

        lax.fori_loop(first, last, body, 0)

    def share(action, sweep, j, i, parts):
        if action is not None:
            some(action, sweep, j, i * (units // parts), (i + 1) * (units // parts))

    def send_y(sweep, j, dy, dc):
        n, target = (sweep * chunks + j) * rows_count + dy * 2 + dc, to(dy, dc)
        size = padded if sweep == 0 else strip
        start = target * strip if sweep == 0 else target * strip + EDGE
        return remote(
            s.iy.at[sweep, j, pl.ds(pl.multiple_of(start, EDGE), size)],
            s.yr.at[sweep, j, r, pl.ds(0, size)],
            s.ys.at[n],
            s.yrs.at[n],
            (t, target),
        )

    def rows_in(sweep, j, action=None):
        some(lambda *which: send_c(*which).wait_recv(), sweep, j, 0, units)

        def solve(i, _):
            rows = rows_at(i * LANES, LANES)
            keep, carry = s.keep[j, rows], s.carry[sweep, j, rows]
            first, second = s.ss[j, rows, :LANES], s.ss[j, rows, LANES:]
            if sweep == 0:
                steady = s.sd[j, rows]
                first, second = first + steady, second + steady
                carry = carry + s.rho[j, rows] * steady
                s.ctot[j, rows] = carry
            first = first + keep * carry
            second = second + keep * first
            s.uh[rows, :LANES], s.ul[rows, :LANES] = split(first)
            s.uh[rows, LANES:], s.ul[rows, LANES:] = split(second)
            return 0

        lax.fori_loop(0, length // LANES, solve, 0)

        def part(i, _):
            dy, q = lax.rem(lax.div(i, 2) + 1, ys_count), lax.rem(i, 2)
            target = lax.rem(y + dy, ys_count) * 2 + q
            rows = rows_at(target * strip, strip)
            out = dot3(s.cth[rows], s.ctl[rows], s.uh[...], s.ul[...])
            s.iy[sweep, j, pl.ds(pl.multiple_of(target * strip + EDGE, EDGE), strip)] = out
            if sweep > 0:

                @pl.when(target != r)
                def _():
                    send_y(sweep, j, dy, lax.rem(q + c, 2)).start()

            share(action, sweep, j + 1, i, rows_count)
            return 0

        lax.fori_loop(0, rows_count, part, 0)
        if sweep == 0:
            for dy, dc in peers:
                send_y(sweep, j, dy, dc).start()
            s.yr[sweep, j, r] = s.iy[sweep, j, pl.ds(pl.multiple_of(r * strip, EDGE), padded)]
        else:
            mid = pl.ds(pl.multiple_of(r * strip + EDGE, EDGE), strip)
            s.yr[sweep, j, r, 0:strip] = s.iy[sweep, j, mid]

    def store(i):
        columns = rows_at(i * big, big)
        return pltpu.make_async_copy(
            s.outv.at[:, :, columns], s.out.at[:, :, columns], s.osem.at[i]
        )

    def columns_in(sweep):
        size = padded if sweep == 0 else strip

        def chunk(j, _):
            for dy, dc in peers:
                send_y(sweep, j, dy, dc).wait_recv()
            for source in range(rows_count):
                high, low = split(s.yr[sweep, j, source, 0:size])
                lanes = slice(source * LANES, (source + 1) * LANES)
                for n in range(steps):
                    part = slice(n * LANES, (n + 1) * LANES)
                    s.lh[n * size : (n + 1) * size, lanes] = high[:, part]
                    s.ll[n * size : (n + 1) * size, lanes] = low[:, part]

            def tile(i, _):
                columns = rows_at(i * big, big)
                depth = rows_at(j * rows_count * LANES, rows_count * LANES)
                rows = slice(0, steps * size)
                out = dot3(s.lh[rows], s.ll[rows], s.ch[depth, columns], s.cl[depth, columns])
                if sweep == 0:
                    s.u1p[:, columns] = s.u1p[:, columns] + out
                else:
                    for n in range(steps):
                        value = s.outv[n, :, columns] + out[n * size : (n + 1) * size]
                        s.outv[n, :, columns] = value

                    @pl.when(j == chunks - 1)
                    def _():
                        store(i).start()

                return 0

            lax.fori_loop(0, length // big, tile, 0)
            return 0

        lax.fori_loop(0, chunks, chunk, 0)

    def send_x(j, dy, dc):
        n, target = j * rows_count + dy * 2 + dc, to(dy, dc)
        rows = rows_at(r * strip, strip)
        return remote(
            s.fx.at[j, target], s.xr.at[j, rows], s.xs.at[n], s.xrs.at[n], (t, target)
        )

    def send_chip(send, dy):
        for q in range(2):
            dc = lax.rem(q + c, 2)

            @pl.when(dy * 2 + dc > 0)
            def _():
                send(dy, dc).start()

    def columns_out():
        def part(i, _):
            n, g = lax.rem(i, steps), lax.div(i, steps)
            dy, j = lax.rem(g + 1, ys_count), lax.div(g, ys_count)
            chip = lax.rem(y + dy, ys_count) * 2
            rows = rows_at(n * strip, strip)
            columns = rows_at((j * rows_count + chip) * LANES, big)
            out = dot3(s.ph[rows], s.pl[rows], s.cth[:, columns], s.ctl[:, columns])
            for q in range(2):
                s.fx[j, chip + q, :, rows_at(n * LANES, LANES)] = out[
                    :, q * LANES : (q + 1) * LANES
                ]

            @pl.when(n == steps - 1)
            def _():
                send_chip(lambda *to_: send_x(j, *to_), dy)

            return 0

        lax.fori_loop(0, chunks * ys_count * steps, part, 0)

    def gather_x(j):
        own = rows_at(r * strip, strip)
        s.xr[j, own] = s.fx[j, r]
        for dy, dc in peers:
            send_x(j, dy, dc).wait_recv()

        def body(i, _):
            rows = rows_at(i * LANES, LANES)
            s.xh[j, rows], s.xl[j, rows] = split(s.xr[j, rows])
            return 0

        lax.fori_loop(0, length // LANES, body, 0)

    def steady_out(action, sweep, beside_j):
        s.w0p[EDGE : EDGE + strip] = s.w0[...]

        @pl.when(r > 0)
        def _():
            halo_down(r).wait_recv()
            s.w0p[0:EDGE] = s.halo[0]

        @pl.when(r == 0)
        def _():
            s.w0p[0:EDGE] = jnp.broadcast_to(s.w0[0:1], (EDGE, length))

        @pl.when(r < rows_count - 1)
        def _():
            halo_up(r).wait_recv()
            s.w0p[EDGE + strip :] = s.halo[1]

        @pl.when(r == rows_count - 1)
        def _():
            s.w0p[EDGE + strip :] = jnp.broadcast_to(s.w0[strip - 1 :], (EDGE, length))

        kappa(None)
        forcing(None, 0)

        def part(i, _):
            j, dy = lax.rem(i, chunks), lax.rem(lax.div(i, chunks) + 1, ys_count)
            chip = lax.rem(y + dy, ys_count) * 2
            columns = rows_at((j * rows_count + chip) * LANES, big)
            out = dot3(s.ph[0:strip], s.pl[0:strip], s.cth[:, columns], s.ctl[:, columns])
            for q in range(2):
                s.dst[chip + q, :, rows_at(j * LANES, LANES)] = out[:, q * LANES : (q + 1) * LANES]

            @pl.when(j == chunks - 1)
            def _():
                send_chip(send_d, dy)

            share(action, sweep, beside_j, i, chunks * ys_count)
            return 0

        lax.fori_loop(0, chunks * ys_count, part, 0)
        s.xd[rows_at(r * strip, strip)] = s.dst[r]

    def steady_in():
        for dy, dc in peers:
            send_d(dy, dc).wait_recv()

        def spread(i, _):
            rows = rows_at(i * LANES, LANES)
            s.xh[0, rows], s.xl[0, rows] = split(s.xd[rows])
            return 0

        lax.fori_loop(0, length // LANES, spread, 0)

        def block(i, _):
            rows = rows_at(i * big, big)
            out = dot3(s.ch[rows], s.cl[rows], s.xh[0], s.xl[0])
            for j in range(chunks):
                s.sd[j, rows] = out[:, j * LANES : (j + 1) * LANES] * s.gw[j, rows]
            return 0

        lax.fori_loop(0, length // big, block, 0)

    rows_out(0, 0)
    steady_out(pair_up, 0, 0)
    rows_out(0, 1, relay_near, 0)
    some(relay_away, 0, 0, 0, units)
    some(pair_up, 0, 1, 0, units)
    steady_in()
    rows_in(0, 0, relay_near)
    some(relay_away, 0, 1, 0, units)
    rows_in(0, 1)
    s.u1p[...] = jnp.zeros_like(s.u1p)
    columns_in(0)

    def force(n, _):
        offset = n * padded

        @pl.when(r == 0)
        def _():
            edge = s.u1p[pl.ds(pl.multiple_of(offset + EDGE, EDGE), EDGE)][0:1]
            home = pl.ds(pl.multiple_of(offset, EDGE), EDGE)
            s.u1p[home] = jnp.broadcast_to(edge, (EDGE, length))

        @pl.when(r == rows_count - 1)
        def _():
            edge = s.u1p[pl.ds(pl.multiple_of(offset + strip, EDGE), EDGE)][EDGE - 1 :]
            home = pl.ds(pl.multiple_of(offset + strip + EDGE, EDGE), EDGE)
            s.u1p[home] = jnp.broadcast_to(edge, (EDGE, length))

        kappa(offset)
        forcing(offset, n * strip)
        return 0

    lax.fori_loop(0, steps, force, 0)
    columns_out()
    for n in range(steps):
        first = n * padded + EDGE
        s.outv[n] = s.w0[...] + s.u1p[first : first + strip]
    gather_x(0)
    rows_out(1, 0)
    some(pair_up, 1, 0, 0, units)
    some(relay_near, 1, 0, 0, units)
    gather_x(1)
    rows_out(1, 1, relay_away, 0)
    some(pair_up, 1, 1, 0, units)
    rows_in(1, 0, relay_near)
    some(relay_away, 1, 1, 0, units)
    rows_in(1, 1)
    columns_in(1)
    for i in range(length // big):
        store(i).wait()

    @pl.when(r < rows_count - 1)
    def _():
        halo_down(r + 1).wait_send()

    @pl.when(r > 0)
    def _():
        halo_up(r - 1).wait_send()

    for dy, dc in peers:
        send_d(dy, dc).wait_send()
        for j in range(chunks):
            send_x(j, dy, dc).wait_send()
            for sweep in range(ITERS):
                send_y(sweep, j, dy, dc).wait_send()
    for sweep in range(ITERS):
        for j in range(chunks):

            def drain(i, _, sweep=sweep, j=j):
                send_e(sweep, j, i).wait_send()
                send_c(sweep, j, i).wait_send()

                @pl.when(z < zs - 1)
                def _():
                    send_f(sweep, j, i, (t + 2, r)).wait_send()

                @pl.when(z > 0)
                def _():
                    send_s(sweep, j, i, (t - 2, r)).wait_send()

                return 0

            lax.fori_loop(0, units, drain, 0)


def fused(
    initial_warmth,
    pattern_choice,
    dissipation_tables,
    material_label,
    intercept_kappa,
    sensitivity_coef,
):
    steps = pattern_choice.shape[0]
    strip, length = initial_warmth.shape
    tm_count, rows_count = lax.axis_size("tm"), lax.axis_size("rows")
    chunks = length // rows_count // LANES
    column_cos = cosine_table(length)
    forward, inverse = two_parts(column_cos.T), two_parts(column_cos)
    mu = 2.0 - 2.0 * np.cos(np.arange(length) * (math.pi / length))
    mup = np.broadcast_to(mu[:, None], (length, LANES)).astype(np.float32)
    muq = np.broadcast_to(mu.reshape(rows_count * chunks, 1, LANES), (rows_count * chunks, 8, LANES))
    scratch = scratch_of(steps, strip, length, tm_count, rows_count)
    names = INPUTS + ["out"] + list(scratch)
    smem, vmem, hbm = (
        pl.BlockSpec(memory_space=space) for space in (pltpu.SMEM, pltpu.VMEM, pl.ANY)
    )
    return pl.pallas_call(
        lambda *refs: fused_kernel(steps, strip, length, tm_count, rows_count, names, *refs),
        out_shape=jax.ShapeDtypeStruct((steps, strip, length), F32),
        in_specs=[vmem, smem, vmem, smem, smem, smem, vmem, vmem] + [hbm] * 4,
        out_specs=hbm,
        scratch_shapes=list(scratch.values()),
        compiler_params=pltpu.CompilerParams(
            collective_id=0, has_side_effects=True, vmem_limit_bytes=67043328
        ),
    )(
        initial_warmth,
        pattern_choice,
        dissipation_tables,
        material_label,
        intercept_kappa,
        sensitivity_coef,
        jnp.asarray(mup),
        jnp.asarray(muq.astype(np.float32)),
        *inverse,
        *forward,
    )


def pick(initial_warmth, pattern_choice, *rest):
    strip, width = initial_warmth.shape
    tm_count, rows_count = lax.axis_size("tm"), lax.axis_size("rows")
    aligned = (
        pattern_choice.shape[0] == 2
        and strip * rows_count == width
        and strip % TILE == 0
        and width == rows_count * 2 * LANES
        and width % (4 * LANES) == 0
        and tm_count % 2 == 0
        and rows_count % 2 == 0
    )
    return (fused if aligned else shards)(initial_warmth, pattern_choice, *rest)


def solution(mesh):
    in_specs = (P("rows", None), P("tm", None, None), P(), P(), P(), P())
    out_specs = P("tm", "rows", None)
    return jax.shard_map(pick, mesh=mesh, in_specs=in_specs, out_specs=out_specs, check_vma=False)
```

```python
import math
from types import SimpleNamespace

import jax
import jax.numpy as jnp
import numpy as np
from jax import lax
from jax.experimental import pallas as pl
from jax.experimental.pallas import tpu as pltpu
from jax.sharding import PartitionSpec as P

TILE = 128
ITERS = 2
TIMESTEP_SIZE = 2.0
ALPHA = 0.05
CROSS_WEIGHT = 1.0 / 64.0
F32 = jnp.float32
BF16 = jnp.bfloat16


def extended(block, axis, dim):
    count = lax.axis_size(axis)
    forward = [(i, i + 1) for i in range(count - 1)]
    backward = [(target, source) for source, target in forward]
    low = lax.ppermute(
        lax.slice_in_dim(block, block.shape[dim] - 1, None, axis=dim), axis, forward
    )
    high = lax.ppermute(lax.slice_in_dim(block, 0, 1, axis=dim), axis, backward)
    return jnp.concatenate([low, block, high], axis=dim)


def cosine_table(length):
    modes = np.arange(length, dtype=np.int64)[:, None]
    cells = np.arange(length, dtype=np.int64)[None, :]
    phase = modes * (2 * cells + 1) % (4 * length)
    return np.cos(phase * (math.pi / (2 * length)))


def two_parts(table):
    high = np.asarray(table, dtype=np.float32).astype(BF16)
    low = (table - high.astype(np.float64)).astype(np.float32).astype(BF16)
    return jnp.asarray(high), jnp.asarray(low)


def split(values):
    high = values.astype(BF16)
    return high, (values - high.astype(F32)).astype(BF16)


def mul(left, right):
    return jnp.dot(left, right, preferred_element_type=F32)


def columns_kernel(x_ref, high_ref, low_ref, out_ref, x_high, x_low):
    @pl.when(pl.program_id(0) == 0)
    def _():
        x_high[...], x_low[...] = split(x_ref[...])

    high = high_ref[...]
    out_ref[...] = (
        mul(x_high[...], high) + mul(x_low[...], high) + mul(x_high[...], low_ref[...])
    )


def times_table(values, table):
    rows, depth = values.shape
    width = table[0].shape[1]
    block = min(256, width)
    return pl.pallas_call(
        columns_kernel,
        grid=(width // block,),
        out_shape=jax.ShapeDtypeStruct((rows, width), F32),
        in_specs=[
            pl.BlockSpec((rows, depth), lambda i: (0, 0)),
            pl.BlockSpec((depth, block), lambda i: (0, i)),
            pl.BlockSpec((depth, block), lambda i: (0, i)),
        ],
        out_specs=pl.BlockSpec((rows, block), lambda i: (0, i)),
        scratch_shapes=[pltpu.VMEM((rows, depth), BF16)] * 2,
    )(values, *table)


def rows_kernel(high_ref, low_ref, x_ref, out_ref, x_high, x_low):
    @pl.when(pl.program_id(0) == 0)
    def _():
        x_high[...], x_low[...] = split(x_ref[...])

    for n in range(x_ref.shape[0]):
        out_ref[n] = (
            mul(high_ref[...], x_high[n])
            + mul(high_ref[...], x_low[n])
            + mul(low_ref[...], x_high[n])
        )


def table_times(table, values):
    steps, depth, width = values.shape
    height = table[0].shape[0]
    block = min(256, height)
    return pl.pallas_call(
        rows_kernel,
        grid=(height // block,),
        out_shape=jax.ShapeDtypeStruct((steps, height, width), F32),
        in_specs=[
            pl.BlockSpec((block, depth), lambda i: (i, 0)),
            pl.BlockSpec((block, depth), lambda i: (i, 0)),
            pl.BlockSpec((steps, depth, width), lambda i: (0, 0, 0)),
        ],
        out_specs=pl.BlockSpec((steps, block, width), lambda i: (0, i, 0)),
        scratch_shapes=[pltpu.VMEM((steps, depth, width), BF16)] * 2,
    )(*table, values)


def power_kernel(choice_ref, table_ref, out_ref):
    steps, blocks, _, width = out_ref.shape
    across = width // TILE
    for n in range(steps):
        for b in range(blocks):
            for x in range(across):
                picked = choice_ref[n, b * across + x]
                out_ref[n, b, :, x * TILE : (x + 1) * TILE] = table_ref[picked]


def power_of(pattern_choice, tables, first_row, strip, width):
    steps = pattern_choice.shape[0]
    part = min(TILE, strip)
    blocks = strip // part
    offset = first_row % TILE if strip < TILE else 0
    tiles = lax.dynamic_slice_in_dim(tables, offset, part, axis=1)
    chosen = lax.dynamic_slice_in_dim(pattern_choice, first_row // TILE, blocks, axis=1)
    power = pl.pallas_call(
        power_kernel,
        out_shape=jax.ShapeDtypeStruct((steps, blocks, part, width), F32),
        in_specs=[
            pl.BlockSpec(memory_space=pltpu.SMEM),
            pl.BlockSpec(memory_space=pltpu.VMEM),
        ],
        out_specs=pl.BlockSpec(memory_space=pltpu.VMEM),
    )(chosen.reshape(steps, -1), tiles)
    return power.reshape(steps, strip, width)


def divergence(warmth, kappa, inner):
    def face(low, high):
        return 1.0 if kappa is None else 0.5 * (low + high)

    k = warmth if kappa is None else kappa
    upward = face(k[:, 1:], k[:, :-1]) * (warmth[:, 1:] - warmth[:, :-1])
    upward = jnp.where(inner[None, :, None], upward, 0.0)
    centre, k_mid = warmth[:, 1:-1], k[:, 1:-1]
    lateral = CROSS_WEIGHT * (
        face(k_mid[:, :, 1:], k_mid[:, :, :-1]) * (centre[:, :, 1:] - centre[:, :, :-1])
    )
    zero = jnp.zeros_like(centre[:, :, :1])
    across = jnp.concatenate([lateral, zero], 2) - jnp.concatenate([zero, lateral], 2)
    return upward[:, 1:] - upward[:, :-1] + across


def mode_factors(row_ids, column_ids, height, width, conduct):
    mu_rows = 2.0 - 2.0 * jnp.cos(row_ids.astype(F32) * (math.pi / height))
    mu_cols = 2.0 - 2.0 * jnp.cos(column_ids.astype(F32) * (math.pi / width))
    rate = conduct * (mu_rows[:, None] + CROSS_WEIGHT * mu_cols[None, :])
    gain = 1.0 / (1.0 / TIMESTEP_SIZE + rate)
    return gain, gain * (1.0 / TIMESTEP_SIZE)


def shards(
    initial_warmth,
    pattern_choice,
    dissipation_tables,
    material_label,
    intercept_kappa,
    sensitivity_coef,
):
    steps = pattern_choice.shape[0]
    strip, width = initial_warmth.shape
    tm_count = lax.axis_size("tm")
    rows_count = lax.axis_size("rows")
    height = strip * rows_count
    first_row = lax.axis_index("rows") * strip
    power = power_of(pattern_choice, dissipation_tables, first_row, strip, width)

    padded_rows = first_row - 1 + jnp.arange(strip + 2, dtype=jnp.int32)
    labels = jnp.take(material_label, jnp.clip(padded_rows, 0, height - 1) // TILE, axis=0)
    base_tiles = jnp.zeros(labels.shape, F32)
    slope_tiles = jnp.zeros(labels.shape, F32)
    for label in range(intercept_kappa.shape[0]):
        base_tiles = jnp.where(labels == label, intercept_kappa[label], base_tiles)
        slope_tiles = jnp.where(labels == label, sensitivity_coef[label], slope_tiles)
    base = jnp.repeat(base_tiles, TILE, axis=1)[None]
    slope = jnp.repeat(slope_tiles, TILE, axis=1)[None]
    upper_rows = padded_rows[:-1]
    inner = (upper_rows >= 0) & (upper_rows + 1 <= height - 1)
    conduct = jnp.mean(intercept_kappa)

    column_cos = cosine_table(width)
    row_cos = cosine_table(height)
    columns_out, columns_in = two_parts(column_cos.T), two_parts(column_cos)
    if height == width:
        rows_out, rows_in = columns_in, columns_out
    else:
        rows_out, rows_in = two_parts(row_cos), two_parts(row_cos.T)

    narrow = width // rows_count
    share = height // tm_count
    column_ids = lax.axis_index("rows") * narrow + jnp.arange(narrow, dtype=jnp.int32)
    all_rows = jnp.arange(height, dtype=jnp.int32)
    own_rows = lax.axis_index("tm") * share + jnp.arange(share, dtype=jnp.int32)
    gain, keep = mode_factors(all_rows, column_ids, height, width, conduct)
    weight = (jnp.where(all_rows == 0, 1.0, 2.0) / height)[:, None] * (
        jnp.where(column_ids == 0, 1.0, 2.0) / width
    )[None, :]
    _, own_keep = mode_factors(own_rows, column_ids, height, width, conduct)
    block_keep = own_keep
    for _ in range(steps - 1):
        block_keep = block_keep * own_keep
    around = block_keep
    for _ in range(tm_count - 1):
        around = around * block_keep
    closing = ALPHA / (1.0 - ALPHA * around)
    first_block = lax.axis_index("tm") == 0

    start = extended(initial_warmth[None], "rows", 1)
    start_div = divergence(start, base * (1.0 + slope * jnp.tanh(start)), inner)
    warmth = jnp.broadcast_to(initial_warmth[None], (steps, strip, width))
    wrapped = None
    for sweep in range(ITERS):
        if sweep == 0:
            resid = power + start_div
        else:
            grid = extended(warmth, "rows", 1)
            div = divergence(grid, base * (1.0 + slope * jnp.tanh(grid)), inner)
            resid = div - last_div - conduct * divergence(grid - last_grid, None, inner)
        modes = times_table(resid.reshape(steps * strip, width), columns_out)
        modes = lax.all_to_all(
            modes.reshape(steps, strip, width), "rows", split_axis=2, concat_axis=1, tiled=True
        )
        modes = table_times(rows_out, modes)
        sources = [modes[n] * weight for n in range(steps)]
        if wrapped is not None:
            sources[0] = sources[0] - jnp.where(first_block, wrapped / TIMESTEP_SIZE, 0.0)
        sources = [gain * source for source in sources]
        block_end = sources[0]
        for source in sources[1:]:
            block_end = source + keep * block_end
        ends = lax.all_to_all(block_end, "tm", split_axis=0, concat_axis=0, tiled=True)
        ends = ends.reshape(tm_count, share, narrow)
        last = ends[0]
        for k in range(1, tm_count):
            last = ends[k] + block_keep * last
        entry = [closing * last]
        for k in range(tm_count - 1):
            entry.append(ends[k] + block_keep * entry[k])
        entry = jnp.concatenate(entry, 0)
        carry = lax.all_to_all(entry, "tm", split_axis=0, concat_axis=0, tiled=True)
        wrapped = carry
        solved = []
        for source in sources:
            carry = source + keep * carry
            solved.append(carry)
        field = table_times(rows_in, jnp.stack(solved, 0))
        field = lax.all_to_all(field, "rows", split_axis=1, concat_axis=2, tiled=True)
        update = times_table(field.reshape(steps * strip, width), columns_in)
        if sweep == 0:
            last_grid, last_div = start, start_div
        else:
            last_grid, last_div = grid, div
        warmth = warmth + update.reshape(steps, strip, width)
    return warmth


LANES = 128
EDGE = 8
ROWS = 32
UNIT = 64
MESH = pl.DeviceIdType.MESH


def dot3(left_high, left_low, right_high, right_low):
    return mul(left_high, right_high) + mul(left_low, right_high) + mul(left_high, right_low)


def remote(src, dst, send_sem, recv_sem, device):
    return pltpu.make_async_remote_copy(
        src_ref=src,
        dst_ref=dst,
        send_sem=send_sem,
        recv_sem=recv_sem,
        device_id=device,
        device_id_type=MESH,
    )


def scratch_of(steps, strip, length, tm_count, rows_count):
    narrow = length // rows_count
    chunks = narrow // LANES
    half = length // 2
    units = half // UNIT
    wide = steps * LANES
    padded = strip + 2 * EDGE

    def f32(*shape):
        return pltpu.VMEM(shape, F32)

    def b16(*shape):
        return pltpu.VMEM(shape, BF16)

    dma = pltpu.SemaphoreType.DMA
    return dict(
        ch=b16(length, length),
        cl=b16(length, length),
        cth=b16(length, length),
        ctl=b16(length, length),
        ph=b16(length, length),
        pl=b16(length, length),
        th=b16(8, TILE, TILE),
        tl=b16(8, TILE, TILE),
        base=f32(8, length),
        slope=f32(8, length),
        w0p=f32(padded, length),
        kp=f32(padded, length),
        halo=f32(2, EDGE, length),
        dst=f32(rows_count, strip, narrow),
        oh=b16(length, narrow),
        ol=b16(length, narrow),
        xd=f32(length, narrow),
        xh=b16(chunks, length, wide),
        xl=b16(chunks, length, wide),
        fx=f32(chunks, rows_count, strip, wide),
        xr=f32(chunks, length, wide),
        ss=f32(chunks, length, wide),
        e=f32(ITERS, chunks, length, LANES),
        er=f32(ITERS, chunks, half, LANES),
        fin=f32(ITERS, chunks, half, LANES),
        sin=f32(ITERS, chunks, half, LANES),
        fout=f32(ITERS, chunks, half, LANES),
        sout=f32(ITERS, chunks, half, LANES),
        cs=f32(ITERS, chunks, half, LANES),
        zz=f32(chunks, half, LANES),
        carry=f32(ITERS, chunks, length, LANES),
        gw=f32(chunks, length, LANES),
        keep=f32(chunks, length, LANES),
        rho=f32(chunks, length, LANES),
        sd=f32(chunks, length, LANES),
        k1=f32(chunks, half, LANES),
        k2=f32(chunks, half, LANES),
        pa=f32(chunks, half, LANES),
        pb=f32(chunks, half, LANES),
        pf=f32(chunks, half, LANES),
        iy=f32(ITERS, chunks, length + 2 * EDGE, wide),
        yr=f32(ITERS, chunks, rows_count, padded, wide),
        uh=b16(length, wide),
        ul=b16(length, wide),
        lh=b16(steps * padded, rows_count * LANES),
        ll=b16(steps * padded, rows_count * LANES),
        u1p=f32(steps * padded, length),
        outv=f32(steps, strip, length),
        osem=dma((length // (2 * LANES),)),
        tsem=dma((4,)),
        hs=dma((2,)),
        hr=dma((2,)),
        ds=dma((rows_count,)),
        dr=dma((rows_count,)),
        xs=dma((chunks * rows_count,)),
        xrs=dma((chunks * rows_count,)),
        ys=dma((ITERS * chunks * rows_count,)),
        yrs=dma((ITERS * chunks * rows_count,)),
        es=dma((ITERS * chunks,)),
        ers=dma((chunks * units,)),
        fs=dma((ITERS * chunks,)),
        frs=dma((chunks * units,)),
        gs=dma((ITERS * chunks,)),
        grs=dma((chunks * units,)),
        cts=dma((ITERS * chunks,)),
        crs=dma((chunks * units,)),
    )


INPUTS = [
    "w0",
    "choice",
    "tables",
    "label",
    "icpt",
    "sens",
    "mup",
    "muq",
    "chh",
    "clh",
    "cthh",
    "ctlh",
]


def fused_kernel(steps, strip, length, tm_count, rows_count, names, *refs):
    s = SimpleNamespace(**dict(zip(names, refs)))
    narrow = length // rows_count
    chunks = narrow // LANES
    half = length // 2
    units = half // UNIT
    padded = strip + 2 * EDGE
    blocks = strip // TILE
    tiles = length // TILE
    big = 2 * LANES
    zs, ys_count = tm_count // 2, rows_count // 2

    t, r = lax.axis_index("tm"), lax.axis_index("rows")
    z, x = lax.div(t, 2), lax.rem(t, 2)
    y, c = lax.div(r, 2), lax.rem(r, 2)
    pair = t + 1 - 2 * x
    peers = [(dy, dc) for dy in range(1, ys_count) for dc in range(2)] + [(0, 1)]

    def to(dy, dc):
        return lax.rem(y + dy, ys_count) * 2 + lax.rem(c + dc, 2)

    def frm(dy, dc):
        return lax.rem(y + ys_count - dy, ys_count) * 2 + lax.rem(c + 2 - dc, 2)

    def rows_at(start, size):
        return pl.ds(pl.multiple_of(start, size), size)

    tables_in = [
        pltpu.make_async_copy(a, b, s.tsem.at[i])
        for i, (a, b) in enumerate(
            [(s.cthh, s.cth), (s.ctlh, s.ctl), (s.chh, s.ch), (s.clh, s.cl)]
        )
    ]
    for copy in tables_in:
        copy.start()

    barrier = pltpu.get_barrier_semaphore()
    for dy, dc in peers:
        pl.semaphore_signal(barrier, inc=1, device_id=(t, to(dy, dc)), device_id_type=MESH)
    pl.semaphore_signal(barrier, inc=1, device_id=(pair, r), device_id_type=MESH)

    @pl.when(z > 0)
    def _():
        pl.semaphore_signal(barrier, inc=1, device_id=(t - 2, r), device_id_type=MESH)

    @pl.when(z < zs - 1)
    def _():
        pl.semaphore_signal(barrier, inc=1, device_id=(t + 2, r), device_id_type=MESH)

    def halo_down(to_row):
        return remote(
            s.w0.at[pl.ds(strip - EDGE, EDGE)], s.halo.at[0], s.hs.at[0], s.hr.at[0], (t, to_row)
        )

    def halo_up(to_row):
        return remote(s.w0.at[pl.ds(0, EDGE)], s.halo.at[1], s.hs.at[1], s.hr.at[1], (t, to_row))

    count = s.icpt.shape[0]
    total = s.icpt[0]
    for i in range(1, count):
        total = total + s.icpt[i]
    conduct = total / count
    for i in range(blocks + 2):
        ty = lax.min(lax.max(r * blocks - 1 + i, 0), tiles - 1)
        for tx in range(tiles):
            label = s.label[ty, tx]
            s.base[i : i + 1, tx * TILE : (tx + 1) * TILE] = jnp.full((1, TILE), s.icpt[label], F32)
            s.slope[i : i + 1, tx * TILE : (tx + 1) * TILE] = jnp.full((1, TILE), s.sens[label], F32)

    def factors_of(j):

        def factors(i, _):
            rows = rows_at(i * LANES, LANES)
            rate = conduct * (s.mup[rows] + CROSS_WEIGHT * s.muq[j * rows_count + r, 0:1, :])
            gain = 1.0 / (1.0 / TIMESTEP_SIZE + rate)
            keep = gain * (1.0 / TIMESTEP_SIZE)
            p = i * LANES + lax.broadcasted_iota(jnp.int32, (LANES, LANES), 0)
            q = (j * rows_count + r) * LANES + lax.broadcasted_iota(jnp.int32, (LANES, LANES), 1)
            weight = (jnp.where(p == 0, 1.0, 2.0) / length) * (jnp.where(q == 0, 1.0, 2.0) / length)
            s.gw[j, rows] = gain * weight
            s.keep[j, rows] = keep
            one = 1.0 + keep
            k = keep * keep
            around, power = one, k
            for _ in range(tm_count - 1):
                around = one + k * around
                power = power * k
            first = ALPHA * around / (1.0 - ALPHA * power)
            s.rho[j, rows] = lax.fori_loop(0, t, lambda _, a: one + k * a, first)
            return 0

        lax.fori_loop(0, length // LANES, factors, 0)

        def chain(i, _):
            rows = rows_at(i * UNIT, UNIT)
            keep = s.keep[j, rows_at(x * half + i * UNIT, UNIT)]
            k = keep * keep
            k2 = k * k
            ones = jnp.ones_like(k)
            whole = k2
            for _ in range(zs - 1):
                whole = whole * k2
            upper = lax.fori_loop(0, zs - 1 - z, lambda _, a: a * k2, ones)
            lower = lax.fori_loop(0, z, lambda _, a: a * k2, ones)
            close = lower * (ALPHA / (1.0 - ALPHA * whole))
            s.k1[j, rows] = k
            s.k2[j, rows] = k2
            s.pa[j, rows] = upper
            s.pb[j, rows] = close
            s.pf[j, rows] = 1.0 + close * (upper * k2)
            return 0

        lax.fori_loop(0, units, chain, 0)

    factors_of(0)

    @pl.when(z == 0)
    def _():
        s.fin[...] = jnp.zeros_like(s.fin)

    @pl.when(z == zs - 1)
    def _():
        s.sin[...] = jnp.zeros_like(s.sin)

    for j in range(chunks):
        s.iy[0, j, 0:EDGE] = jnp.zeros((EDGE, steps * LANES), F32)
        s.iy[0, j, length + EDGE :] = jnp.zeros((EDGE, steps * LANES), F32)
    for k in range(s.tables.shape[0]):
        s.th[k], s.tl[k] = split(s.tables[k])

    def kappa(offset):
        def part(start, size, i):
            rows = pl.ds(start, size)
            warmth = s.w0p[rows]
            if offset is not None:
                warmth = warmth + s.u1p[pl.ds(pl.multiple_of(offset + start, EDGE), size)]
            bent = s.slope[i : i + 1] * jnp.tanh(warmth)
            s.kp[rows] = s.base[i : i + 1] * (1.0 + bent)

        part(0, EDGE, 0)
        part(EDGE + strip, EDGE, blocks + 1)
        for b in range(blocks):

            def inner(i, _, b=b):
                part(pl.multiple_of(EDGE + b * TILE + i * ROWS, EDGE), ROWS, b + 1)
                return 0

            lax.fori_loop(0, TILE // ROWS, inner, 0)

    lane = lax.broadcasted_iota(jnp.int32, (ROWS, length), 1)
    ext = ROWS + 2 * EDGE

    def forcing(offset, out_row):
        def inner(i, _):
            rows = pl.ds(pl.multiple_of(i * ROWS, ROWS), ext)
            warmth, k = s.w0p[rows], s.kp[rows]
            mid = slice(EDGE, EDGE + ROWS)
            if offset is not None:
                warmth = warmth + s.u1p[pl.ds(pl.multiple_of(offset + i * ROWS, EDGE), ext)]

            def flux(shift, w, k):
                return 0.5 * (k + shift(k)) * (shift(w) - w)

            down = flux(lambda v: pltpu.roll(v, ext - 1, 0), warmth, k)
            total = (down - pltpu.roll(down, 1, 0))[mid]
            right = flux(lambda v: pltpu.roll(v, length - 1, 1), warmth[mid], k[mid])
            right = jnp.where(lane < length - 1, right, 0.0)
            total = total + CROSS_WEIGHT * (right - pltpu.roll(right, 1, 1))
            rows = pl.ds(pl.multiple_of(out_row + i * ROWS, ROWS), ROWS)
            s.ph[rows], s.pl[rows] = split(total)
            return 0

        lax.fori_loop(0, strip // ROWS, inner, 0)

    def send_d(dy, dc):
        n, target = dy * 2 + dc, to(dy, dc)
        rows = rows_at(r * strip, strip)
        return remote(s.dst.at[target], s.xd.at[rows], s.ds.at[n], s.dr.at[n], (t, target))

    beside = lax.min(z, 1) + lax.min(zs - 1 - z, 1)
    pl.semaphore_wait(barrier, len(peers) + 1 + beside)

    @pl.when(r < rows_count - 1)
    def _():
        halo_down(r + 1).start()

    @pl.when(r > 0)
    def _():
        halo_up(r - 1).start()

    tables_in[0].wait()
    tables_in[1].wait()

    for j in range(chunks):
        columns = rows_at((j * rows_count + r) * LANES, LANES)
        s.oh[:, j * LANES : (j + 1) * LANES] = s.cth[:, columns]
        s.ol[:, j * LANES : (j + 1) * LANES] = s.ctl[:, columns]

    def power(n, _):
        def place(ty, _):
            rows = rows_at(ty * TILE, TILE)
            for tx in range(tiles):
                picked = s.choice[n, ty, tx]
                s.ph[rows, tx * TILE : (tx + 1) * TILE] = s.th[picked]
                s.pl[rows, tx * TILE : (tx + 1) * TILE] = s.tl[picked]
            return 0

        lax.fori_loop(0, tiles, place, 0)

        def across(i, _):
            rows = rows_at(i * half, half)
            out = dot3(s.ph[rows], s.pl[rows], s.oh[...], s.ol[...])
            high, low = split(out)
            lanes = rows_at(n * LANES, LANES)
            for j in range(chunks):
                s.xh[j, rows, lanes] = high[:, j * LANES : (j + 1) * LANES]
                s.xl[j, rows, lanes] = low[:, j * LANES : (j + 1) * LANES]
            return 0

        lax.fori_loop(0, 2, across, 0)
        return 0

    lax.fori_loop(0, steps, power, 0)
    tables_in[2].wait()
    tables_in[3].wait()

    def unit(sweep, j, i):
        return j * units + i

    def send_e(sweep, j, i, size=UNIT):
        n = unit(sweep, j, i)
        return remote(
            s.e.at[sweep, j, rows_at((1 - x) * half + i * size, size)],
            s.er.at[sweep, j, rows_at(i * size, size)],
            s.es.at[sweep * chunks + j],
            s.ers.at[n],
            (pair, r),
        )

    def send_f(sweep, j, i, device, size=UNIT):
        n = unit(sweep, j, i)
        rows = rows_at(i * size, size)
        return remote(
            s.fout.at[sweep, j, rows], s.fin.at[sweep, j, rows], s.fs.at[sweep * chunks + j], s.frs.at[n], device
        )

    def send_s(sweep, j, i, device, size=UNIT):
        n = unit(sweep, j, i)
        rows = rows_at(i * size, size)
        return remote(
            s.sout.at[sweep, j, rows], s.sin.at[sweep, j, rows], s.gs.at[sweep * chunks + j], s.grs.at[n], device
        )

    def send_c(sweep, j, i, size=UNIT):
        n = unit(sweep, j, i)
        return remote(
            s.cs.at[sweep, j, rows_at(i * size, size)],
            s.carry.at[sweep, j, rows_at(x * half + i * size, size)],
            s.cts.at[sweep * chunks + j],
            s.crs.at[n],
            (pair, r),
        )

    is_first = jnp.where(t == 0, 1.0, 0.0)

    def rows_out(sweep, j, action=None, beside_j=0, at_once=False):
        parts = length // big
        per = big // UNIT

        def part(i, _):
            rows = rows_at(lax.rem(i + (1 - x) * (parts // 2), parts) * big, big)
            out = dot3(s.ch[rows], s.cl[rows], s.xh[j], s.xl[j])
            gw, keep = s.gw[j, rows], s.keep[j, rows]
            first, second = out[:, :LANES] * gw, out[:, LANES:] * gw
            if sweep > 0:
                first = first + s.ss[j, rows, :LANES]
                second = second + s.ss[j, rows, LANES:]
            s.ss[j, rows, :LANES] = first
            s.ss[j, rows, LANES:] = second
            s.e[sweep, j, rows] = second + keep * first

            @pl.when(i < parts // 2)
            def _():
                for n in range(per):
                    send_e(sweep, j, i * per + n).start()

            if at_once:

                @pl.when(i == 0)
                def _():
                    some(action, sweep, beside_j, 0, units)
            else:
                share(action, sweep, beside_j, i, parts)
            return 0

        lax.fori_loop(0, parts, part, 0)

    def halves(sweep, j, i):
        mine = s.e[sweep, j, rows_at(x * half + i * UNIT, UNIT)]
        other = s.er[sweep, j, rows_at(i * UNIT, UNIT)]
        return jnp.where(x == 0, mine, other), jnp.where(x == 0, other, mine)

    def repeat(sweep, j, *actions):
        def body(i, _):
            for action in actions:
                action(sweep, j, i)
            return 0

        lax.fori_loop(0, units, body, 0)

    def pair_up(sweep, j, i):
        rows = rows_at(i * UNIT, UNIT)
        send_e(sweep, j, i).wait_recv()
        even, odd = halves(sweep, j, i)
        block = odd + s.k1[j, rows] * even
        s.zz[j, rows] = block

        @pl.when(z == 0)
        def _():
            s.fout[sweep, j, rows] = block
            send_f(sweep, j, i, (t + 2, r)).start()

        @pl.when(z == zs - 1)
        def _():
            s.sout[sweep, j, rows] = block
            send_s(sweep, j, i, (t - 2, r)).start()

    def relay_f(sweep, j, i):
        rows = rows_at(i * UNIT, UNIT)

        @pl.when(z > 0)
        def _():
            send_f(sweep, j, i, (t, r)).wait_recv()

            @pl.when(z < zs - 1)
            def _():
                s.fout[sweep, j, rows] = s.zz[j, rows] + s.k2[j, rows] * s.fin[sweep, j, rows]
                send_f(sweep, j, i, (t + 2, r)).start()

    def relay_s(sweep, j, i):
        rows = rows_at(i * UNIT, UNIT)

        @pl.when(z < zs - 1)
        def _():
            send_s(sweep, j, i, (t, r)).wait_recv()
            s.sout[sweep, j, rows] = s.sin[sweep, j, rows] + s.pa[j, rows] * s.zz[j, rows]

            @pl.when(z > 0)
            def _():
                send_s(sweep, j, i, (t - 2, r)).start()

    def finish(sweep, j, i):
        rows = rows_at(i * UNIT, UNIT)
        even, _ = halves(sweep, j, i)
        lower = s.fin[sweep, j, rows] * s.pf[j, rows] + s.pb[j, rows] * s.sout[sweep, j, rows]
        upper = even + s.k1[j, rows] * lower
        s.carry[sweep, j, rows_at(x * half + i * UNIT, UNIT)] = jnp.where(x == 0, lower, upper)
        s.cs[sweep, j, rows] = jnp.where(x == 0, upper, lower)
        send_c(sweep, j, i).start()

    def relay_near(sweep, j, i):
        @pl.when(z < zs // 2)
        def _():
            relay_f(sweep, j, i)

        @pl.when(z >= zs // 2)
        def _():
            relay_s(sweep, j, i)

    def relay_away(sweep, j, i):
        @pl.when(z < zs // 2)
        def _():
            relay_s(sweep, j, i)

        @pl.when(z >= zs // 2)
        def _():
            relay_f(sweep, j, i)

        finish(sweep, j, i)

    def some(action, sweep, j, first, last):
        def body(i, _):
            action(sweep, j, i)
            return 0

        lax.fori_loop(first, last, body, 0)

    def share(action, sweep, j, i, parts):
        if action is not None:
            some(action, sweep, j, i * (units // parts), (i + 1) * (units // parts))

    inner = (z > 0) & (z < zs - 1)

    def by_place(relaying, ending):
        @pl.when(inner)
        def _():
            relaying()

        @pl.when(jnp.logical_not(inner))
        def _():
            ending()

    def send_y(sweep, j, dy, dc):
        n, target = (sweep * chunks + j) * rows_count + dy * 2 + dc, to(dy, dc)
        size = padded if sweep == 0 else strip
        start = target * strip if sweep == 0 else target * strip + EDGE
        return remote(
            s.iy.at[sweep, j, pl.ds(pl.multiple_of(start, EDGE), size)],
            s.yr.at[sweep, j, r, pl.ds(0, size)],
            s.ys.at[n],
            s.yrs.at[n],
            (t, target),
        )

    def rows_in(sweep, j, action=None):
        some(lambda *which: send_c(*which).wait_recv(), sweep, j, 0, units)

        def solve(i, _):
            rows = rows_at(i * LANES, LANES)
            keep, carry = s.keep[j, rows], s.carry[sweep, j, rows]
            first, second = s.ss[j, rows, :LANES], s.ss[j, rows, LANES:]
            if sweep == 0:
                steady = s.sd[j, rows]
                first, second = first + steady, second + steady
                carry = carry + s.rho[j, rows] * steady
            first = first + keep * carry
            second = second + keep * first
            if sweep == 0:
                left = (1.0 - keep) * first - steady
                s.ss[j, rows, :LANES] = left - is_first * keep * carry
                s.ss[j, rows, LANES:] = (1.0 - keep) * second - steady
            s.uh[rows, :LANES], s.ul[rows, :LANES] = split(first)
            s.uh[rows, LANES:], s.ul[rows, LANES:] = split(second)
            return 0

        lax.fori_loop(0, length // LANES, solve, 0)

        def part(i, _):
            dy, q = lax.rem(lax.div(i, 2) + 1, ys_count), lax.rem(i, 2)
            target = lax.rem(y + dy, ys_count) * 2 + q
            rows = rows_at(target * strip, strip)
            out = dot3(s.cth[rows], s.ctl[rows], s.uh[...], s.ul[...])
            s.iy[sweep, j, pl.ds(pl.multiple_of(target * strip + EDGE, EDGE), strip)] = out
            if sweep > 0:

                @pl.when(target != r)
                def _():
                    send_y(sweep, j, dy, lax.rem(q + c, 2)).start()

            share(action, sweep, j + 1, i, rows_count)
            return 0

        lax.fori_loop(0, rows_count, part, 0)
        if sweep == 0:
            for dy, dc in peers:
                send_y(sweep, j, dy, dc).start()
            s.yr[sweep, j, r] = s.iy[sweep, j, pl.ds(pl.multiple_of(r * strip, EDGE), padded)]
        else:
            mid = pl.ds(pl.multiple_of(r * strip + EDGE, EDGE), strip)
            s.yr[sweep, j, r, 0:strip] = s.iy[sweep, j, mid]

    def store(i):
        columns = rows_at(i * big, big)
        return pltpu.make_async_copy(
            s.outv.at[:, :, columns], s.out.at[:, :, columns], s.osem.at[i]
        )

    def columns_in(sweep):
        size = padded if sweep == 0 else strip

        def chunk(j, _):
            for dy, dc in peers:
                send_y(sweep, j, dy, dc).wait_recv()
            for source in range(rows_count):
                high, low = split(s.yr[sweep, j, source, 0:size])
                lanes = slice(source * LANES, (source + 1) * LANES)
                for n in range(steps):
                    part = slice(n * LANES, (n + 1) * LANES)
                    s.lh[n * size : (n + 1) * size, lanes] = high[:, part]
                    s.ll[n * size : (n + 1) * size, lanes] = low[:, part]

            def tile(i, _):
                columns = rows_at(i * big, big)
                depth = rows_at(j * rows_count * LANES, rows_count * LANES)
                rows = slice(0, steps * size)
                out = dot3(s.lh[rows], s.ll[rows], s.ch[depth, columns], s.cl[depth, columns])
                if sweep == 0:
                    s.u1p[:, columns] = s.u1p[:, columns] + out
                else:
                    for n in range(steps):
                        value = s.outv[n, :, columns] + out[n * size : (n + 1) * size]
                        s.outv[n, :, columns] = value

                    @pl.when(j == chunks - 1)
                    def _():
                        store(i).start()

                return 0

            lax.fori_loop(0, length // big, tile, 0)
            return 0

        lax.fori_loop(0, chunks, chunk, 0)

    def send_x(j, dy, dc):
        n, target = j * rows_count + dy * 2 + dc, to(dy, dc)
        rows = rows_at(r * strip, strip)
        return remote(
            s.fx.at[j, target], s.xr.at[j, rows], s.xs.at[n], s.xrs.at[n], (t, target)
        )

    def send_chip(send, dy):
        for q in range(2):
            dc = lax.rem(q + c, 2)

            @pl.when(dy * 2 + dc > 0)
            def _():
                send(dy, dc).start()

    def columns_out():
        def part(i, _):
            n, g = lax.rem(i, steps), lax.div(i, steps)
            dy, j = lax.rem(g + 1, ys_count), lax.div(g, ys_count)
            chip = lax.rem(y + dy, ys_count) * 2
            rows = rows_at(n * strip, strip)
            columns = rows_at((j * rows_count + chip) * LANES, big)
            out = dot3(s.ph[rows], s.pl[rows], s.cth[:, columns], s.ctl[:, columns])
            for q in range(2):
                s.fx[j, chip + q, :, rows_at(n * LANES, LANES)] = out[
                    :, q * LANES : (q + 1) * LANES
                ]

            @pl.when(n == steps - 1)
            def _():
                send_chip(lambda *to_: send_x(j, *to_), dy)

            return 0

        lax.fori_loop(0, chunks * ys_count * steps, part, 0)

    def gather_x(j):
        own = rows_at(r * strip, strip)
        s.xr[j, own] = s.fx[j, r]
        for dy, dc in peers:
            send_x(j, dy, dc).wait_recv()

        def body(i, _):
            rows = rows_at(i * LANES, LANES)
            s.xh[j, rows], s.xl[j, rows] = split(s.xr[j, rows])
            return 0

        lax.fori_loop(0, length // LANES, body, 0)

    def steady_out(action, sweep, beside_j):
        s.w0p[EDGE : EDGE + strip] = s.w0[...]

        @pl.when(r > 0)
        def _():
            halo_down(r).wait_recv()
            s.w0p[0:EDGE] = s.halo[0]

        @pl.when(r == 0)
        def _():
            s.w0p[0:EDGE] = jnp.broadcast_to(s.w0[0:1], (EDGE, length))

        @pl.when(r < rows_count - 1)
        def _():
            halo_up(r).wait_recv()
            s.w0p[EDGE + strip :] = s.halo[1]

        @pl.when(r == rows_count - 1)
        def _():
            s.w0p[EDGE + strip :] = jnp.broadcast_to(s.w0[strip - 1 :], (EDGE, length))

        kappa(None)
        forcing(None, 0)

        def part(i, _):
            j, dy = lax.rem(i, chunks), lax.rem(lax.div(i, chunks) + 1, ys_count)
            chip = lax.rem(y + dy, ys_count) * 2
            columns = rows_at((j * rows_count + chip) * LANES, big)
            out = dot3(s.ph[0:strip], s.pl[0:strip], s.cth[:, columns], s.ctl[:, columns])
            for q in range(2):
                s.dst[chip + q, :, rows_at(j * LANES, LANES)] = out[:, q * LANES : (q + 1) * LANES]

            @pl.when(j == chunks - 1)
            def _():
                send_chip(send_d, dy)

            share(action, sweep, beside_j, i, chunks * ys_count)
            return 0

        lax.fori_loop(0, chunks * ys_count, part, 0)
        s.xd[rows_at(r * strip, strip)] = s.dst[r]

    def steady_in():
        for dy, dc in peers:
            send_d(dy, dc).wait_recv()

        def spread(i, _):
            rows = rows_at(i * LANES, LANES)
            s.xh[0, rows], s.xl[0, rows] = split(s.xd[rows])
            return 0

        lax.fori_loop(0, length // LANES, spread, 0)

        def block(i, _):
            rows = rows_at(i * big, big)
            out = dot3(s.ch[rows], s.cl[rows], s.xh[0], s.xl[0])
            for j in range(chunks):
                s.sd[j, rows] = out[:, j * LANES : (j + 1) * LANES] * s.gw[j, rows]
            return 0

        lax.fori_loop(0, length // big, block, 0)

    rows_out(0, 0)
    for j in range(1, chunks):
        factors_of(j)
    steady_out(pair_up, 0, 0)
    rows_out(0, 1, relay_near, 0)
    some(relay_away, 0, 0, 0, units)
    some(pair_up, 0, 1, 0, units)
    steady_in()
    rows_in(0, 0, relay_near)
    some(relay_away, 0, 1, 0, units)
    rows_in(0, 1)
    s.u1p[...] = jnp.zeros_like(s.u1p)
    columns_in(0)

    def force(n, _):
        offset = n * padded

        @pl.when(r == 0)
        def _():
            edge = s.u1p[pl.ds(pl.multiple_of(offset + EDGE, EDGE), EDGE)][0:1]
            home = pl.ds(pl.multiple_of(offset, EDGE), EDGE)
            s.u1p[home] = jnp.broadcast_to(edge, (EDGE, length))

        @pl.when(r == rows_count - 1)
        def _():
            edge = s.u1p[pl.ds(pl.multiple_of(offset + strip, EDGE), EDGE)][EDGE - 1 :]
            home = pl.ds(pl.multiple_of(offset + strip + EDGE, EDGE), EDGE)
            s.u1p[home] = jnp.broadcast_to(edge, (EDGE, length))

        kappa(offset)
        forcing(offset, n * strip)
        return 0

    lax.fori_loop(0, steps, force, 0)
    columns_out()
    for n in range(steps):
        first = n * padded + EDGE
        s.outv[n] = s.w0[...] + s.u1p[first : first + strip]
    gather_x(0)
    rows_out(1, 0)
    some(pair_up, 1, 0, 0, units)
    some(relay_near, 1, 0, 0, units)

    def relay_then_rows():
        some(relay_away, 1, 0, 0, units)
        gather_x(1)
        rows_out(1, 1)

    def rows_then_end():
        gather_x(1)
        rows_out(1, 1, relay_away, 0, at_once=True)

    by_place(relay_then_rows, rows_then_end)
    some(pair_up, 1, 1, 0, units)
    rows_in(1, 0, relay_near)
    some(relay_away, 1, 1, 0, units)
    rows_in(1, 1)
    @pl.when(r < rows_count - 1)
    def _():
        halo_down(r + 1).wait_send()

    @pl.when(r > 0)
    def _():
        halo_up(r - 1).wait_send()

    for dy, dc in peers:
        send_d(dy, dc).wait_send()
        for j in range(chunks):
            send_x(j, dy, dc).wait_send()
            send_y(0, j, dy, dc).wait_send()
    for sweep in range(ITERS):
        for j in range(chunks):
            send_e(sweep, j, 0, half).wait_send()
            send_c(sweep, j, 0, half).wait_send()

            @pl.when(z < zs - 1)
            def _():
                send_f(sweep, j, 0, (t + 2, r), half).wait_send()

            @pl.when(z > 0)
            def _():
                send_s(sweep, j, 0, (t - 2, r), half).wait_send()
    columns_in(1)
    for i in range(length // big):
        store(i).wait()
    for dy, dc in peers:
        for j in range(chunks):
            send_y(1, j, dy, dc).wait_send()


def pass_on_kernel(in_ref, out_ref, held, in_sem, out_sem):
    count = in_sem.shape[0]
    rows = in_ref.shape[0] // count

    def part(i):
        return pl.ds(i * rows, rows)

    loads = [
        pltpu.make_async_copy(in_ref.at[part(i)], held.at[part(i)], in_sem.at[i])
        for i in range(count)
    ]
    stores = [
        pltpu.make_async_copy(held.at[part(i)], out_ref.at[part(i)], out_sem.at[i])
        for i in range(count)
    ]
    for load in loads:
        load.start()
    for load, store in zip(loads, stores):
        load.wait()
        store.start()
    for store in stores:
        store.wait()


def pass_on(values, parts=8):
    flat = values.reshape(-1, values.shape[-1])
    hbm = pl.BlockSpec(memory_space=pl.ANY)
    dma = pltpu.SemaphoreType.DMA
    return pl.pallas_call(
        pass_on_kernel,
        out_shape=jax.ShapeDtypeStruct(flat.shape, flat.dtype),
        in_specs=[hbm],
        out_specs=hbm,
        scratch_shapes=[pltpu.VMEM(flat.shape, flat.dtype), dma((parts,)), dma((parts,))],
    )(flat).reshape(values.shape)


def fused(
    initial_warmth,
    pattern_choice,
    dissipation_tables,
    material_label,
    intercept_kappa,
    sensitivity_coef,
):
    steps = pattern_choice.shape[0]
    strip, length = initial_warmth.shape
    tm_count, rows_count = lax.axis_size("tm"), lax.axis_size("rows")
    chunks = length // rows_count // LANES
    column_cos = cosine_table(length)
    forward, inverse = two_parts(column_cos.T), two_parts(column_cos)
    mu = 2.0 - 2.0 * np.cos(np.arange(length) * (math.pi / length))
    mup = np.broadcast_to(mu[:, None], (length, LANES)).astype(np.float32)
    muq = np.broadcast_to(mu.reshape(rows_count * chunks, 1, LANES), (rows_count * chunks, 8, LANES))
    scratch = scratch_of(steps, strip, length, tm_count, rows_count)
    names = INPUTS + ["out"] + list(scratch)
    smem, vmem, hbm = (
        pl.BlockSpec(memory_space=space) for space in (pltpu.SMEM, pltpu.VMEM, pl.ANY)
    )
    result = pl.pallas_call(
        lambda *refs: fused_kernel(steps, strip, length, tm_count, rows_count, names, *refs),
        out_shape=jax.ShapeDtypeStruct((steps, strip, length), F32),
        in_specs=[vmem, smem, vmem, smem, smem, smem, vmem, vmem] + [hbm] * 4,
        out_specs=hbm,
        scratch_shapes=list(scratch.values()),
        compiler_params=pltpu.CompilerParams(
            collective_id=0, has_side_effects=True, vmem_limit_bytes=67043328
        ),
    )(
        initial_warmth,
        pattern_choice,
        dissipation_tables,
        material_label,
        intercept_kappa,
        sensitivity_coef,
        jnp.asarray(mup),
        jnp.asarray(muq.astype(np.float32)),
        *inverse,
        *forward,
    )
    return pass_on(result)


def pick(initial_warmth, pattern_choice, *rest):
    strip, width = initial_warmth.shape
    tm_count, rows_count = lax.axis_size("tm"), lax.axis_size("rows")
    aligned = (
        pattern_choice.shape[0] == 2
        and strip * rows_count == width
        and strip % TILE == 0
        and width == rows_count * 2 * LANES
        and width % (4 * LANES) == 0
        and tm_count % 2 == 0
        and rows_count % 2 == 0
    )
    return (fused if aligned else shards)(initial_warmth, pattern_choice, *rest)


def solution(mesh):
    in_specs = (P("rows", None), P("tm", None, None), P(), P(), P(), P())
    out_specs = P("tm", "rows", None)
    return jax.shard_map(pick, mesh=mesh, in_specs=in_specs, out_specs=out_specs, check_vma=False)
```

```python
import math
from types import SimpleNamespace

import jax
import jax.numpy as jnp
import numpy as np
from jax import lax
from jax.experimental import pallas as pl
from jax.experimental.pallas import tpu as pltpu
from jax.sharding import PartitionSpec as P

TILE = 128
ITERS = 2
TIMESTEP_SIZE = 2.0
ALPHA = 0.05
CROSS_WEIGHT = 1.0 / 64.0
F32 = jnp.float32
BF16 = jnp.bfloat16


def extended(block, axis, dim):
    count = lax.axis_size(axis)
    forward = [(i, i + 1) for i in range(count - 1)]
    backward = [(target, source) for source, target in forward]
    low = lax.ppermute(
        lax.slice_in_dim(block, block.shape[dim] - 1, None, axis=dim), axis, forward
    )
    high = lax.ppermute(lax.slice_in_dim(block, 0, 1, axis=dim), axis, backward)
    return jnp.concatenate([low, block, high], axis=dim)


def cosine_table(length):
    modes = np.arange(length, dtype=np.int64)[:, None]
    cells = np.arange(length, dtype=np.int64)[None, :]
    phase = modes * (2 * cells + 1) % (4 * length)
    return np.cos(phase * (math.pi / (2 * length)))


def two_parts(table):
    high = np.asarray(table, dtype=np.float32).astype(BF16)
    low = (table - high.astype(np.float64)).astype(np.float32).astype(BF16)
    return jnp.asarray(high), jnp.asarray(low)


def split(values):
    high = values.astype(BF16)
    return high, (values - high.astype(F32)).astype(BF16)


def mul(left, right):
    return jnp.dot(left, right, preferred_element_type=F32)


def columns_kernel(x_ref, high_ref, low_ref, out_ref, x_high, x_low):
    @pl.when(pl.program_id(0) == 0)
    def _():
        x_high[...], x_low[...] = split(x_ref[...])

    high = high_ref[...]
    out_ref[...] = (
        mul(x_high[...], high) + mul(x_low[...], high) + mul(x_high[...], low_ref[...])
    )


def times_table(values, table):
    rows, depth = values.shape
    width = table[0].shape[1]
    block = min(256, width)
    return pl.pallas_call(
        columns_kernel,
        grid=(width // block,),
        out_shape=jax.ShapeDtypeStruct((rows, width), F32),
        in_specs=[
            pl.BlockSpec((rows, depth), lambda i: (0, 0)),
            pl.BlockSpec((depth, block), lambda i: (0, i)),
            pl.BlockSpec((depth, block), lambda i: (0, i)),
        ],
        out_specs=pl.BlockSpec((rows, block), lambda i: (0, i)),
        scratch_shapes=[pltpu.VMEM((rows, depth), BF16)] * 2,
    )(values, *table)


def rows_kernel(high_ref, low_ref, x_ref, out_ref, x_high, x_low):
    @pl.when(pl.program_id(0) == 0)
    def _():
        x_high[...], x_low[...] = split(x_ref[...])

    for n in range(x_ref.shape[0]):
        out_ref[n] = (
            mul(high_ref[...], x_high[n])
            + mul(high_ref[...], x_low[n])
            + mul(low_ref[...], x_high[n])
        )


def table_times(table, values):
    steps, depth, width = values.shape
    height = table[0].shape[0]
    block = min(256, height)
    return pl.pallas_call(
        rows_kernel,
        grid=(height // block,),
        out_shape=jax.ShapeDtypeStruct((steps, height, width), F32),
        in_specs=[
            pl.BlockSpec((block, depth), lambda i: (i, 0)),
            pl.BlockSpec((block, depth), lambda i: (i, 0)),
            pl.BlockSpec((steps, depth, width), lambda i: (0, 0, 0)),
        ],
        out_specs=pl.BlockSpec((steps, block, width), lambda i: (0, i, 0)),
        scratch_shapes=[pltpu.VMEM((steps, depth, width), BF16)] * 2,
    )(*table, values)


def power_kernel(choice_ref, table_ref, out_ref):
    steps, blocks, _, width = out_ref.shape
    across = width // TILE
    for n in range(steps):
        for b in range(blocks):
            for x in range(across):
                picked = choice_ref[n, b * across + x]
                out_ref[n, b, :, x * TILE : (x + 1) * TILE] = table_ref[picked]


def power_of(pattern_choice, tables, first_row, strip, width):
    steps = pattern_choice.shape[0]
    part = min(TILE, strip)
    blocks = strip // part
    offset = first_row % TILE if strip < TILE else 0
    tiles = lax.dynamic_slice_in_dim(tables, offset, part, axis=1)
    chosen = lax.dynamic_slice_in_dim(pattern_choice, first_row // TILE, blocks, axis=1)
    power = pl.pallas_call(
        power_kernel,
        out_shape=jax.ShapeDtypeStruct((steps, blocks, part, width), F32),
        in_specs=[
            pl.BlockSpec(memory_space=pltpu.SMEM),
            pl.BlockSpec(memory_space=pltpu.VMEM),
        ],
        out_specs=pl.BlockSpec(memory_space=pltpu.VMEM),
    )(chosen.reshape(steps, -1), tiles)
    return power.reshape(steps, strip, width)


def divergence(warmth, kappa, inner):
    def face(low, high):
        return 1.0 if kappa is None else 0.5 * (low + high)

    k = warmth if kappa is None else kappa
    upward = face(k[:, 1:], k[:, :-1]) * (warmth[:, 1:] - warmth[:, :-1])
    upward = jnp.where(inner[None, :, None], upward, 0.0)
    centre, k_mid = warmth[:, 1:-1], k[:, 1:-1]
    lateral = CROSS_WEIGHT * (
        face(k_mid[:, :, 1:], k_mid[:, :, :-1]) * (centre[:, :, 1:] - centre[:, :, :-1])
    )
    zero = jnp.zeros_like(centre[:, :, :1])
    across = jnp.concatenate([lateral, zero], 2) - jnp.concatenate([zero, lateral], 2)
    return upward[:, 1:] - upward[:, :-1] + across


def mode_factors(row_ids, column_ids, height, width, conduct):
    mu_rows = 2.0 - 2.0 * jnp.cos(row_ids.astype(F32) * (math.pi / height))
    mu_cols = 2.0 - 2.0 * jnp.cos(column_ids.astype(F32) * (math.pi / width))
    rate = conduct * (mu_rows[:, None] + CROSS_WEIGHT * mu_cols[None, :])
    gain = 1.0 / (1.0 / TIMESTEP_SIZE + rate)
    return gain, gain * (1.0 / TIMESTEP_SIZE)


def shards(
    initial_warmth,
    pattern_choice,
    dissipation_tables,
    material_label,
    intercept_kappa,
    sensitivity_coef,
):
    steps = pattern_choice.shape[0]
    strip, width = initial_warmth.shape
    tm_count = lax.axis_size("tm")
    rows_count = lax.axis_size("rows")
    height = strip * rows_count
    first_row = lax.axis_index("rows") * strip
    power = power_of(pattern_choice, dissipation_tables, first_row, strip, width)

    padded_rows = first_row - 1 + jnp.arange(strip + 2, dtype=jnp.int32)
    labels = jnp.take(material_label, jnp.clip(padded_rows, 0, height - 1) // TILE, axis=0)
    base_tiles = jnp.zeros(labels.shape, F32)
    slope_tiles = jnp.zeros(labels.shape, F32)
    for label in range(intercept_kappa.shape[0]):
        base_tiles = jnp.where(labels == label, intercept_kappa[label], base_tiles)
        slope_tiles = jnp.where(labels == label, sensitivity_coef[label], slope_tiles)
    base = jnp.repeat(base_tiles, TILE, axis=1)[None]
    slope = jnp.repeat(slope_tiles, TILE, axis=1)[None]
    upper_rows = padded_rows[:-1]
    inner = (upper_rows >= 0) & (upper_rows + 1 <= height - 1)
    conduct = jnp.mean(intercept_kappa)

    column_cos = cosine_table(width)
    row_cos = cosine_table(height)
    columns_out, columns_in = two_parts(column_cos.T), two_parts(column_cos)
    if height == width:
        rows_out, rows_in = columns_in, columns_out
    else:
        rows_out, rows_in = two_parts(row_cos), two_parts(row_cos.T)

    narrow = width // rows_count
    share = height // tm_count
    column_ids = lax.axis_index("rows") * narrow + jnp.arange(narrow, dtype=jnp.int32)
    all_rows = jnp.arange(height, dtype=jnp.int32)
    own_rows = lax.axis_index("tm") * share + jnp.arange(share, dtype=jnp.int32)
    gain, keep = mode_factors(all_rows, column_ids, height, width, conduct)
    weight = (jnp.where(all_rows == 0, 1.0, 2.0) / height)[:, None] * (
        jnp.where(column_ids == 0, 1.0, 2.0) / width
    )[None, :]
    _, own_keep = mode_factors(own_rows, column_ids, height, width, conduct)
    block_keep = own_keep
    for _ in range(steps - 1):
        block_keep = block_keep * own_keep
    around = block_keep
    for _ in range(tm_count - 1):
        around = around * block_keep
    closing = ALPHA / (1.0 - ALPHA * around)
    first_block = lax.axis_index("tm") == 0

    start = extended(initial_warmth[None], "rows", 1)
    start_div = divergence(start, base * (1.0 + slope * jnp.tanh(start)), inner)
    warmth = jnp.broadcast_to(initial_warmth[None], (steps, strip, width))
    wrapped = None
    for sweep in range(ITERS):
        if sweep == 0:
            resid = power + start_div
        else:
            grid = extended(warmth, "rows", 1)
            div = divergence(grid, base * (1.0 + slope * jnp.tanh(grid)), inner)
            resid = div - last_div - conduct * divergence(grid - last_grid, None, inner)
        modes = times_table(resid.reshape(steps * strip, width), columns_out)
        modes = lax.all_to_all(
            modes.reshape(steps, strip, width), "rows", split_axis=2, concat_axis=1, tiled=True
        )
        modes = table_times(rows_out, modes)
        sources = [modes[n] * weight for n in range(steps)]
        if wrapped is not None:
            sources[0] = sources[0] - jnp.where(first_block, wrapped / TIMESTEP_SIZE, 0.0)
        sources = [gain * source for source in sources]
        block_end = sources[0]
        for source in sources[1:]:
            block_end = source + keep * block_end
        ends = lax.all_to_all(block_end, "tm", split_axis=0, concat_axis=0, tiled=True)
        ends = ends.reshape(tm_count, share, narrow)
        last = ends[0]
        for k in range(1, tm_count):
            last = ends[k] + block_keep * last
        entry = [closing * last]
        for k in range(tm_count - 1):
            entry.append(ends[k] + block_keep * entry[k])
        entry = jnp.concatenate(entry, 0)
        carry = lax.all_to_all(entry, "tm", split_axis=0, concat_axis=0, tiled=True)
        wrapped = carry
        solved = []
        for source in sources:
            carry = source + keep * carry
            solved.append(carry)
        field = table_times(rows_in, jnp.stack(solved, 0))
        field = lax.all_to_all(field, "rows", split_axis=1, concat_axis=2, tiled=True)
        update = times_table(field.reshape(steps * strip, width), columns_in)
        if sweep == 0:
            last_grid, last_div = start, start_div
        else:
            last_grid, last_div = grid, div
        warmth = warmth + update.reshape(steps, strip, width)
    return warmth


LANES = 128
EDGE = 8
ROWS = 32
UNIT = 64
MESH = pl.DeviceIdType.MESH


def dot3(left_high, left_low, right_high, right_low):
    return mul(left_high, right_high) + mul(left_low, right_high) + mul(left_high, right_low)


def remote(src, dst, send_sem, recv_sem, device):
    return pltpu.make_async_remote_copy(
        src_ref=src,
        dst_ref=dst,
        send_sem=send_sem,
        recv_sem=recv_sem,
        device_id=device,
        device_id_type=MESH,
    )


def scratch_of(steps, strip, length, tm_count, rows_count):
    narrow = length // rows_count
    chunks = narrow // LANES
    half = length // 2
    units = half // UNIT
    wide = steps * LANES
    padded = strip + 2 * EDGE

    def f32(*shape):
        return pltpu.VMEM(shape, F32)

    def b16(*shape):
        return pltpu.VMEM(shape, BF16)

    dma = pltpu.SemaphoreType.DMA
    return dict(
        ch=b16(length, length),
        cl=b16(length, length),
        cth=b16(length, length),
        ctl=b16(length, length),
        ph=b16(length, length),
        pl=b16(length, length),
        th=b16(8, TILE, TILE),
        tl=b16(8, TILE, TILE),
        base=f32(8, length),
        slope=f32(8, length),
        w0p=f32(padded, length),
        kp=f32(padded, length),
        halo=f32(2, EDGE, length),
        dst=f32(rows_count, strip, narrow),
        oh=b16(length, narrow),
        ol=b16(length, narrow),
        xd=f32(length, narrow),
        xh=b16(chunks, length, wide),
        xl=b16(chunks, length, wide),
        fx=f32(chunks, rows_count, strip, wide),
        xr=f32(chunks, length, wide),
        ss=f32(chunks, length, wide),
        e=f32(ITERS, chunks, length, LANES),
        er=f32(ITERS, chunks, half, LANES),
        fin=f32(ITERS, chunks, half, LANES),
        sin=f32(ITERS, chunks, half, LANES),
        fout=f32(ITERS, chunks, half, LANES),
        sout=f32(ITERS, chunks, half, LANES),
        cs=f32(ITERS, chunks, half, LANES),
        zz=f32(chunks, half, LANES),
        carry=f32(ITERS, chunks, length, LANES),
        gw=f32(chunks, length, LANES),
        keep=f32(chunks, length, LANES),
        rho=f32(chunks, length, LANES),
        sd=f32(chunks, length, LANES),
        k1=f32(chunks, half, LANES),
        k2=f32(chunks, half, LANES),
        pa=f32(chunks, half, LANES),
        pb=f32(chunks, half, LANES),
        pf=f32(chunks, half, LANES),
        iy=f32(ITERS, chunks, length + 2 * EDGE, wide),
        yr=f32(ITERS, chunks, rows_count, padded, wide),
        uh=b16(length, wide),
        ul=b16(length, wide),
        lh=b16(steps * padded, rows_count * LANES),
        ll=b16(steps * padded, rows_count * LANES),
        u1p=f32(steps * padded, length),
        outv=f32(steps, strip, length),
        osem=dma((length // (2 * LANES),)),
        tsem=dma((4,)),
        hs=dma((2,)),
        hr=dma((2,)),
        ds=dma((rows_count,)),
        dr=dma((rows_count,)),
        xs=dma((chunks * rows_count,)),
        xrs=dma((chunks * rows_count,)),
        ys=dma((ITERS * chunks * rows_count,)),
        yrs=dma((ITERS * chunks * rows_count,)),
        es=dma((ITERS * chunks,)),
        ers=dma((chunks * units,)),
        fs=dma((ITERS * chunks,)),
        frs=dma((chunks * units,)),
        gs=dma((ITERS * chunks,)),
        grs=dma((chunks * units,)),
        cts=dma((ITERS * chunks,)),
        crs=dma((chunks * units,)),
    )


INPUTS = [
    "w0",
    "choice",
    "tables",
    "label",
    "icpt",
    "sens",
    "mup",
    "muq",
    "chh",
    "clh",
    "cthh",
    "ctlh",
]


def fused_kernel(steps, strip, length, tm_count, rows_count, names, *refs):
    s = SimpleNamespace(**dict(zip(names, refs)))
    narrow = length // rows_count
    chunks = narrow // LANES
    half = length // 2
    units = half // UNIT
    padded = strip + 2 * EDGE
    blocks = strip // TILE
    tiles = length // TILE
    big = 2 * LANES
    zs, ys_count = tm_count // 2, rows_count // 2

    t, r = lax.axis_index("tm"), lax.axis_index("rows")
    z, x = lax.div(t, 2), lax.rem(t, 2)
    y, c = lax.div(r, 2), lax.rem(r, 2)
    pair = t + 1 - 2 * x
    peers = [(dy, dc) for dy in range(1, ys_count) for dc in range(2)] + [(0, 1)]

    def to(dy, dc):
        return lax.rem(y + dy, ys_count) * 2 + lax.rem(c + dc, 2)

    def frm(dy, dc):
        return lax.rem(y + ys_count - dy, ys_count) * 2 + lax.rem(c + 2 - dc, 2)

    def rows_at(start, size):
        return pl.ds(pl.multiple_of(start, size), size)

    tables_in = [
        pltpu.make_async_copy(a, b, s.tsem.at[i])
        for i, (a, b) in enumerate(
            [(s.cthh, s.cth), (s.ctlh, s.ctl), (s.chh, s.ch), (s.clh, s.cl)]
        )
    ]
    for copy in tables_in:
        copy.start()

    barrier = pltpu.get_barrier_semaphore()
    for dy, dc in peers:
        pl.semaphore_signal(barrier, inc=1, device_id=(t, to(dy, dc)), device_id_type=MESH)
    pl.semaphore_signal(barrier, inc=1, device_id=(pair, r), device_id_type=MESH)

    @pl.when(z > 0)
    def _():
        pl.semaphore_signal(barrier, inc=1, device_id=(t - 2, r), device_id_type=MESH)

    @pl.when(z < zs - 1)
    def _():
        pl.semaphore_signal(barrier, inc=1, device_id=(t + 2, r), device_id_type=MESH)

    def halo_down(to_row):
        return remote(
            s.w0.at[pl.ds(strip - EDGE, EDGE)], s.halo.at[0], s.hs.at[0], s.hr.at[0], (t, to_row)
        )

    def halo_up(to_row):
        return remote(s.w0.at[pl.ds(0, EDGE)], s.halo.at[1], s.hs.at[1], s.hr.at[1], (t, to_row))

    count = s.icpt.shape[0]
    total = s.icpt[0]
    for i in range(1, count):
        total = total + s.icpt[i]
    conduct = total / count
    for i in range(blocks + 2):
        ty = lax.min(lax.max(r * blocks - 1 + i, 0), tiles - 1)
        for tx in range(tiles):
            label = s.label[ty, tx]
            s.base[i : i + 1, tx * TILE : (tx + 1) * TILE] = jnp.full((1, TILE), s.icpt[label], F32)
            s.slope[i : i + 1, tx * TILE : (tx + 1) * TILE] = jnp.full((1, TILE), s.sens[label], F32)

    def factors_of(j):

        def factors(i, _):
            rows = rows_at(i * LANES, LANES)
            rate = conduct * (s.mup[rows] + CROSS_WEIGHT * s.muq[j * rows_count + r, 0:1, :])
            gain = 1.0 / (1.0 / TIMESTEP_SIZE + rate)
            keep = gain * (1.0 / TIMESTEP_SIZE)
            p = i * LANES + lax.broadcasted_iota(jnp.int32, (LANES, LANES), 0)
            q = (j * rows_count + r) * LANES + lax.broadcasted_iota(jnp.int32, (LANES, LANES), 1)
            weight = (jnp.where(p == 0, 1.0, 2.0) / length) * (jnp.where(q == 0, 1.0, 2.0) / length)
            s.gw[j, rows] = gain * weight
            s.keep[j, rows] = keep
            one = 1.0 + keep
            k = keep * keep
            around, power = one, k
            for _ in range(tm_count - 1):
                around = one + k * around
                power = power * k
            first = ALPHA * around / (1.0 - ALPHA * power)
            s.rho[j, rows] = lax.fori_loop(0, t, lambda _, a: one + k * a, first)
            return 0

        lax.fori_loop(0, length // LANES, factors, 0)

        def chain(i, _):
            rows = rows_at(i * UNIT, UNIT)
            keep = s.keep[j, rows_at(x * half + i * UNIT, UNIT)]
            k = keep * keep
            k2 = k * k
            ones = jnp.ones_like(k)
            whole = k2
            for _ in range(zs - 1):
                whole = whole * k2
            upper = lax.fori_loop(0, zs - 1 - z, lambda _, a: a * k2, ones)
            lower = lax.fori_loop(0, z, lambda _, a: a * k2, ones)
            close = lower * (ALPHA / (1.0 - ALPHA * whole))
            s.k1[j, rows] = k
            s.k2[j, rows] = k2
            s.pa[j, rows] = upper
            s.pb[j, rows] = close
            s.pf[j, rows] = 1.0 + close * (upper * k2)
            return 0

        lax.fori_loop(0, units, chain, 0)

    factors_of(0)

    @pl.when(z == 0)
    def _():
        s.fin[...] = jnp.zeros_like(s.fin)

    @pl.when(z == zs - 1)
    def _():
        s.sin[...] = jnp.zeros_like(s.sin)

    for j in range(chunks):
        s.iy[0, j, 0:EDGE] = jnp.zeros((EDGE, steps * LANES), F32)
        s.iy[0, j, length + EDGE :] = jnp.zeros((EDGE, steps * LANES), F32)
    for k in range(s.tables.shape[0]):
        s.th[k], s.tl[k] = split(s.tables[k])

    def kappa(offset):
        def part(start, size, i):
            rows = pl.ds(start, size)
            warmth = s.w0p[rows]
            if offset is not None:
                warmth = warmth + s.u1p[pl.ds(pl.multiple_of(offset + start, EDGE), size)]
            bent = s.slope[i : i + 1] * jnp.tanh(warmth)
            s.kp[rows] = s.base[i : i + 1] * (1.0 + bent)

        part(0, EDGE, 0)
        part(EDGE + strip, EDGE, blocks + 1)
        for b in range(blocks):

            def inner(i, _, b=b):
                part(pl.multiple_of(EDGE + b * TILE + i * ROWS, EDGE), ROWS, b + 1)
                return 0

            lax.fori_loop(0, TILE // ROWS, inner, 0)

    lane = lax.broadcasted_iota(jnp.int32, (ROWS, length), 1)
    ext = ROWS + 2 * EDGE

    def forcing(offset, out_row):
        def inner(i, _):
            rows = pl.ds(pl.multiple_of(i * ROWS, ROWS), ext)
            warmth, k = s.w0p[rows], s.kp[rows]
            mid = slice(EDGE, EDGE + ROWS)
            if offset is not None:
                warmth = warmth + s.u1p[pl.ds(pl.multiple_of(offset + i * ROWS, EDGE), ext)]

            def flux(shift, w, k):
                return 0.5 * (k + shift(k)) * (shift(w) - w)

            down = flux(lambda v: pltpu.roll(v, ext - 1, 0), warmth, k)
            total = (down - pltpu.roll(down, 1, 0))[mid]
            right = flux(lambda v: pltpu.roll(v, length - 1, 1), warmth[mid], k[mid])
            right = jnp.where(lane < length - 1, right, 0.0)
            total = total + CROSS_WEIGHT * (right - pltpu.roll(right, 1, 1))
            rows = pl.ds(pl.multiple_of(out_row + i * ROWS, ROWS), ROWS)
            s.ph[rows], s.pl[rows] = split(total)
            return 0

        lax.fori_loop(0, strip // ROWS, inner, 0)

    def send_d(dy, dc):
        n, target = dy * 2 + dc, to(dy, dc)
        rows = rows_at(r * strip, strip)
        return remote(s.dst.at[target], s.xd.at[rows], s.ds.at[n], s.dr.at[n], (t, target))

    beside = lax.min(z, 1) + lax.min(zs - 1 - z, 1)
    pl.semaphore_wait(barrier, len(peers) + 1 + beside)

    @pl.when(r < rows_count - 1)
    def _():
        halo_down(r + 1).start()

    @pl.when(r > 0)
    def _():
        halo_up(r - 1).start()

    tables_in[0].wait()
    tables_in[1].wait()

    for j in range(chunks):
        columns = rows_at((j * rows_count + r) * LANES, LANES)
        s.oh[:, j * LANES : (j + 1) * LANES] = s.cth[:, columns]
        s.ol[:, j * LANES : (j + 1) * LANES] = s.ctl[:, columns]

    def power(n, _):
        def place(ty, _):
            rows = rows_at(ty * TILE, TILE)
            for tx in range(tiles):
                picked = s.choice[n, ty, tx]
                s.ph[rows, tx * TILE : (tx + 1) * TILE] = s.th[picked]
                s.pl[rows, tx * TILE : (tx + 1) * TILE] = s.tl[picked]
            return 0

        lax.fori_loop(0, tiles, place, 0)

        def across(i, _):
            rows = rows_at(i * half, half)
            out = dot3(s.ph[rows], s.pl[rows], s.oh[...], s.ol[...])
            high, low = split(out)
            lanes = rows_at(n * LANES, LANES)
            for j in range(chunks):
                s.xh[j, rows, lanes] = high[:, j * LANES : (j + 1) * LANES]
                s.xl[j, rows, lanes] = low[:, j * LANES : (j + 1) * LANES]
            return 0

        lax.fori_loop(0, 2, across, 0)
        return 0

    lax.fori_loop(0, steps, power, 0)
    tables_in[2].wait()
    tables_in[3].wait()

    def unit(sweep, j, i):
        return j * units + i

    def send_e(sweep, j, i, size=UNIT):
        n = unit(sweep, j, i)
        return remote(
            s.e.at[sweep, j, rows_at((1 - x) * half + i * size, size)],
            s.er.at[sweep, j, rows_at(i * size, size)],
            s.es.at[sweep * chunks + j],
            s.ers.at[n],
            (pair, r),
        )

    def send_f(sweep, j, i, device, size=UNIT):
        n = unit(sweep, j, i)
        rows = rows_at(i * size, size)
        return remote(
            s.fout.at[sweep, j, rows], s.fin.at[sweep, j, rows], s.fs.at[sweep * chunks + j], s.frs.at[n], device
        )

    def send_s(sweep, j, i, device, size=UNIT):
        n = unit(sweep, j, i)
        rows = rows_at(i * size, size)
        return remote(
            s.sout.at[sweep, j, rows], s.sin.at[sweep, j, rows], s.gs.at[sweep * chunks + j], s.grs.at[n], device
        )

    def send_c(sweep, j, i, size=UNIT):
        n = unit(sweep, j, i)
        return remote(
            s.cs.at[sweep, j, rows_at(i * size, size)],
            s.carry.at[sweep, j, rows_at(x * half + i * size, size)],
            s.cts.at[sweep * chunks + j],
            s.crs.at[n],
            (pair, r),
        )

    is_first = jnp.where(t == 0, 1.0, 0.0)

    def rows_out(sweep, j, action=None, beside_j=0, at_once=False):
        parts = length // big
        per = big // UNIT

        def part(i, _):
            rows = rows_at(lax.rem(i + (1 - x) * (parts // 2), parts) * big, big)
            out = dot3(s.ch[rows], s.cl[rows], s.xh[j], s.xl[j])
            gw, keep = s.gw[j, rows], s.keep[j, rows]
            first, second = out[:, :LANES] * gw, out[:, LANES:] * gw
            if sweep > 0:
                first = first + s.ss[j, rows, :LANES]
                second = second + s.ss[j, rows, LANES:]
            s.ss[j, rows, :LANES] = first
            s.ss[j, rows, LANES:] = second
            s.e[sweep, j, rows] = second + keep * first

            @pl.when(i < parts // 2)
            def _():
                for n in range(per):
                    send_e(sweep, j, i * per + n).start()

            if at_once:

                @pl.when(i == 0)
                def _():
                    some(action, sweep, beside_j, 0, units)
            else:
                share(action, sweep, beside_j, i, parts)
            return 0

        lax.fori_loop(0, parts, part, 0)

    def halves(sweep, j, i):
        mine = s.e[sweep, j, rows_at(x * half + i * UNIT, UNIT)]
        other = s.er[sweep, j, rows_at(i * UNIT, UNIT)]
        return jnp.where(x == 0, mine, other), jnp.where(x == 0, other, mine)

    def repeat(sweep, j, *actions):
        def body(i, _):
            for action in actions:
                action(sweep, j, i)
            return 0

        lax.fori_loop(0, units, body, 0)

    def pair_up(sweep, j, i):
        rows = rows_at(i * UNIT, UNIT)
        send_e(sweep, j, i).wait_recv()
        even, odd = halves(sweep, j, i)
        block = odd + s.k1[j, rows] * even
        s.zz[j, rows] = block

        @pl.when(z == 0)
        def _():
            s.fout[sweep, j, rows] = block
            send_f(sweep, j, i, (t + 2, r)).start()

        @pl.when(z == zs - 1)
        def _():
            s.sout[sweep, j, rows] = block
            send_s(sweep, j, i, (t - 2, r)).start()

    def relay_f(sweep, j, i):
        rows = rows_at(i * UNIT, UNIT)

        @pl.when(z > 0)
        def _():
            send_f(sweep, j, i, (t, r)).wait_recv()

            @pl.when(z < zs - 1)
            def _():
                s.fout[sweep, j, rows] = s.zz[j, rows] + s.k2[j, rows] * s.fin[sweep, j, rows]
                send_f(sweep, j, i, (t + 2, r)).start()

    def relay_s(sweep, j, i):
        rows = rows_at(i * UNIT, UNIT)

        @pl.when(z < zs - 1)
        def _():
            send_s(sweep, j, i, (t, r)).wait_recv()
            s.sout[sweep, j, rows] = s.sin[sweep, j, rows] + s.pa[j, rows] * s.zz[j, rows]

            @pl.when(z > 0)
            def _():
                send_s(sweep, j, i, (t - 2, r)).start()

    def finish(sweep, j, i):
        rows = rows_at(i * UNIT, UNIT)
        even, _ = halves(sweep, j, i)
        lower = s.fin[sweep, j, rows] * s.pf[j, rows] + s.pb[j, rows] * s.sout[sweep, j, rows]
        upper = even + s.k1[j, rows] * lower
        s.carry[sweep, j, rows_at(x * half + i * UNIT, UNIT)] = jnp.where(x == 0, lower, upper)
        s.cs[sweep, j, rows] = jnp.where(x == 0, upper, lower)
        send_c(sweep, j, i).start()

    def relay_near(sweep, j, i):
        @pl.when(z < zs // 2)
        def _():
            relay_f(sweep, j, i)

        @pl.when(z >= zs // 2)
        def _():
            relay_s(sweep, j, i)

    def relay_away(sweep, j, i):
        @pl.when(z < zs // 2)
        def _():
            relay_s(sweep, j, i)

        @pl.when(z >= zs // 2)
        def _():
            relay_f(sweep, j, i)

        finish(sweep, j, i)

    def some(action, sweep, j, first, last):
        def body(i, _):
            action(sweep, j, i)
            return 0

        lax.fori_loop(first, last, body, 0)

    def share(action, sweep, j, i, parts):
        if action is not None:
            some(action, sweep, j, i * (units // parts), (i + 1) * (units // parts))

    inner = (z > 0) & (z < zs - 1)

    def by_place(relaying, ending):
        @pl.when(inner)
        def _():
            relaying()

        @pl.when(jnp.logical_not(inner))
        def _():
            ending()

    def send_y(sweep, j, dy, dc):
        n, target = (sweep * chunks + j) * rows_count + dy * 2 + dc, to(dy, dc)
        size = padded if sweep == 0 else strip
        start = target * strip if sweep == 0 else target * strip + EDGE
        return remote(
            s.iy.at[sweep, j, pl.ds(pl.multiple_of(start, EDGE), size)],
            s.yr.at[sweep, j, r, pl.ds(0, size)],
            s.ys.at[n],
            s.yrs.at[n],
            (t, target),
        )

    def rows_in(sweep, j, action=None):
        some(lambda *which: send_c(*which).wait_recv(), sweep, j, 0, units)

        def solve(i, _):
            rows = rows_at(i * LANES, LANES)
            keep, carry = s.keep[j, rows], s.carry[sweep, j, rows]
            first, second = s.ss[j, rows, :LANES], s.ss[j, rows, LANES:]
            if sweep == 0:
                steady = s.sd[j, rows]
                first, second = first + steady, second + steady
                carry = carry + s.rho[j, rows] * steady
            first = first + keep * carry
            second = second + keep * first
            if sweep == 0:
                left = (1.0 - keep) * first - steady
                s.ss[j, rows, :LANES] = left - is_first * keep * carry
                s.ss[j, rows, LANES:] = (1.0 - keep) * second - steady
            s.uh[rows, :LANES], s.ul[rows, :LANES] = split(first)
            s.uh[rows, LANES:], s.ul[rows, LANES:] = split(second)
            return 0

        lax.fori_loop(0, length // LANES, solve, 0)

        def along(i):
            return jnp.where(y < ys_count // 2, rows_count - 1 - i, i)

        def leave(target):
            @pl.when(target != r)
            def _():
                dy = lax.rem(lax.div(target, 2) + ys_count - y, ys_count)
                send_y(sweep, j, dy, lax.rem(target + c, 2)).start()

        def part(i, _):
            dy, q = lax.rem(lax.div(i, 2) + 1, ys_count), lax.rem(i, 2)
            target = along(i) if sweep == 0 else lax.rem(y + dy, ys_count) * 2 + q
            rows = rows_at(target * strip, strip)
            out = dot3(s.cth[rows], s.ctl[rows], s.uh[...], s.ul[...])
            s.iy[sweep, j, pl.ds(pl.multiple_of(target * strip + EDGE, EDGE), strip)] = out
            if sweep > 0:
                leave(target)
            else:

                @pl.when(i > 0)
                def _():
                    leave(along(i - 1))

            share(action, sweep, j + 1, i, rows_count)
            return 0

        lax.fori_loop(0, rows_count, part, 0)
        if sweep == 0:
            leave(along(rows_count - 1))
            s.yr[sweep, j, r] = s.iy[sweep, j, pl.ds(pl.multiple_of(r * strip, EDGE), padded)]
        else:
            mid = pl.ds(pl.multiple_of(r * strip + EDGE, EDGE), strip)
            s.yr[sweep, j, r, 0:strip] = s.iy[sweep, j, mid]

    def store(i):
        columns = rows_at(i * big, big)
        return pltpu.make_async_copy(
            s.outv.at[:, :, columns], s.out.at[:, :, columns], s.osem.at[i]
        )

    def columns_in(sweep):
        size = padded if sweep == 0 else strip

        def chunk(j, _):
            for dy, dc in peers:
                send_y(sweep, j, dy, dc).wait_recv()
            for source in range(rows_count):
                high, low = split(s.yr[sweep, j, source, 0:size])
                lanes = slice(source * LANES, (source + 1) * LANES)
                for n in range(steps):
                    part = slice(n * LANES, (n + 1) * LANES)
                    s.lh[n * size : (n + 1) * size, lanes] = high[:, part]
                    s.ll[n * size : (n + 1) * size, lanes] = low[:, part]

            def tile(i, _):
                columns = rows_at(i * big, big)
                depth = rows_at(j * rows_count * LANES, rows_count * LANES)
                rows = slice(0, steps * size)
                out = dot3(s.lh[rows], s.ll[rows], s.ch[depth, columns], s.cl[depth, columns])
                if sweep == 0:
                    s.u1p[:, columns] = s.u1p[:, columns] + out
                else:
                    for n in range(steps):
                        value = s.outv[n, :, columns] + out[n * size : (n + 1) * size]
                        s.outv[n, :, columns] = value

                    @pl.when(j == chunks - 1)
                    def _():
                        store(i).start()

                return 0

            lax.fori_loop(0, length // big, tile, 0)
            return 0

        lax.fori_loop(0, chunks, chunk, 0)

    def send_x(j, dy, dc):
        n, target = j * rows_count + dy * 2 + dc, to(dy, dc)
        rows = rows_at(r * strip, strip)
        return remote(
            s.fx.at[j, target], s.xr.at[j, rows], s.xs.at[n], s.xrs.at[n], (t, target)
        )

    def send_chip(send, dy):
        for q in range(2):
            dc = lax.rem(q + c, 2)

            @pl.when(dy * 2 + dc > 0)
            def _():
                send(dy, dc).start()

    def columns_out():
        def part(i, _):
            n, g = lax.rem(i, steps), lax.div(i, steps)
            dy, j = lax.rem(g + 1, ys_count), lax.div(g, ys_count)
            chip = lax.rem(y + dy, ys_count) * 2
            rows = rows_at(n * strip, strip)
            columns = rows_at((j * rows_count + chip) * LANES, big)
            out = dot3(s.ph[rows], s.pl[rows], s.cth[:, columns], s.ctl[:, columns])
            for q in range(2):
                s.fx[j, chip + q, :, rows_at(n * LANES, LANES)] = out[
                    :, q * LANES : (q + 1) * LANES
                ]

            @pl.when(n == steps - 1)
            def _():
                send_chip(lambda *to_: send_x(j, *to_), dy)

            return 0

        lax.fori_loop(0, chunks * ys_count * steps, part, 0)

    def gather_x(j):
        own = rows_at(r * strip, strip)
        s.xr[j, own] = s.fx[j, r]
        for dy, dc in peers:
            send_x(j, dy, dc).wait_recv()

        def body(i, _):
            rows = rows_at(i * LANES, LANES)
            s.xh[j, rows], s.xl[j, rows] = split(s.xr[j, rows])
            return 0

        lax.fori_loop(0, length // LANES, body, 0)

    def steady_out(action, sweep, beside_j):
        s.w0p[EDGE : EDGE + strip] = s.w0[...]

        @pl.when(r > 0)
        def _():
            halo_down(r).wait_recv()
            s.w0p[0:EDGE] = s.halo[0]

        @pl.when(r == 0)
        def _():
            s.w0p[0:EDGE] = jnp.broadcast_to(s.w0[0:1], (EDGE, length))

        @pl.when(r < rows_count - 1)
        def _():
            halo_up(r).wait_recv()
            s.w0p[EDGE + strip :] = s.halo[1]

        @pl.when(r == rows_count - 1)
        def _():
            s.w0p[EDGE + strip :] = jnp.broadcast_to(s.w0[strip - 1 :], (EDGE, length))

        kappa(None)
        forcing(None, 0)

        def part(i, _):
            j, dy = lax.rem(i, chunks), lax.rem(lax.div(i, chunks) + 1, ys_count)
            chip = lax.rem(y + dy, ys_count) * 2
            columns = rows_at((j * rows_count + chip) * LANES, big)
            out = dot3(s.ph[0:strip], s.pl[0:strip], s.cth[:, columns], s.ctl[:, columns])
            for q in range(2):
                s.dst[chip + q, :, rows_at(j * LANES, LANES)] = out[:, q * LANES : (q + 1) * LANES]

            @pl.when(j == chunks - 1)
            def _():
                send_chip(send_d, dy)

            share(action, sweep, beside_j, i, chunks * ys_count)
            return 0

        lax.fori_loop(0, chunks * ys_count, part, 0)
        s.xd[rows_at(r * strip, strip)] = s.dst[r]

    def steady_in():
        for dy, dc in peers:
            send_d(dy, dc).wait_recv()

        def spread(i, _):
            rows = rows_at(i * LANES, LANES)
            s.xh[0, rows], s.xl[0, rows] = split(s.xd[rows])
            return 0

        lax.fori_loop(0, length // LANES, spread, 0)

        def block(i, _):
            rows = rows_at(i * big, big)
            out = dot3(s.ch[rows], s.cl[rows], s.xh[0], s.xl[0])
            for j in range(chunks):
                s.sd[j, rows] = out[:, j * LANES : (j + 1) * LANES] * s.gw[j, rows]
            return 0

        lax.fori_loop(0, length // big, block, 0)

    rows_out(0, 0)
    for j in range(1, chunks):
        factors_of(j)
    steady_out(pair_up, 0, 0)
    rows_out(0, 1, relay_near, 0)
    some(relay_away, 0, 0, 0, units)
    some(pair_up, 0, 1, 0, units)
    steady_in()
    rows_in(0, 0, relay_near)
    some(relay_away, 0, 1, 0, units)
    rows_in(0, 1)
    s.u1p[...] = jnp.zeros_like(s.u1p)
    columns_in(0)

    def force(n, _):
        offset = n * padded

        @pl.when(r == 0)
        def _():
            edge = s.u1p[pl.ds(pl.multiple_of(offset + EDGE, EDGE), EDGE)][0:1]
            home = pl.ds(pl.multiple_of(offset, EDGE), EDGE)
            s.u1p[home] = jnp.broadcast_to(edge, (EDGE, length))

        @pl.when(r == rows_count - 1)
        def _():
            edge = s.u1p[pl.ds(pl.multiple_of(offset + strip, EDGE), EDGE)][EDGE - 1 :]
            home = pl.ds(pl.multiple_of(offset + strip + EDGE, EDGE), EDGE)
            s.u1p[home] = jnp.broadcast_to(edge, (EDGE, length))

        kappa(offset)
        forcing(offset, n * strip)
        return 0

    lax.fori_loop(0, steps, force, 0)
    columns_out()
    for n in range(steps):
        first = n * padded + EDGE
        s.outv[n] = s.w0[...] + s.u1p[first : first + strip]
    gather_x(0)
    rows_out(1, 0)
    some(pair_up, 1, 0, 0, units)
    some(relay_near, 1, 0, 0, units)

    def relay_then_rows():
        some(relay_away, 1, 0, 0, units)
        gather_x(1)
        rows_out(1, 1)

    def rows_then_end():
        gather_x(1)
        rows_out(1, 1, relay_away, 0, at_once=True)

    by_place(relay_then_rows, rows_then_end)
    rows_in(1, 0, pair_up)
    some(relay_near, 1, 1, 0, units)
    some(relay_away, 1, 1, 0, units)
    rows_in(1, 1)
    @pl.when(r < rows_count - 1)
    def _():
        halo_down(r + 1).wait_send()

    @pl.when(r > 0)
    def _():
        halo_up(r - 1).wait_send()

    for dy, dc in peers:
        send_d(dy, dc).wait_send()
        for j in range(chunks):
            send_x(j, dy, dc).wait_send()
            send_y(0, j, dy, dc).wait_send()
    for sweep in range(ITERS):
        for j in range(chunks):
            send_e(sweep, j, 0, half).wait_send()
            send_c(sweep, j, 0, half).wait_send()

            @pl.when(z < zs - 1)
            def _():
                send_f(sweep, j, 0, (t + 2, r), half).wait_send()

            @pl.when(z > 0)
            def _():
                send_s(sweep, j, 0, (t - 2, r), half).wait_send()
    columns_in(1)
    for i in range(length // big):
        store(i).wait()
    for dy, dc in peers:
        for j in range(chunks):
            send_y(1, j, dy, dc).wait_send()


def pass_on_kernel(in_ref, out_ref, held, in_sem, out_sem):
    count = in_sem.shape[0]
    rows = in_ref.shape[0] // count

    def part(i):
        return pl.ds(i * rows, rows)

    loads = [
        pltpu.make_async_copy(in_ref.at[part(i)], held.at[part(i)], in_sem.at[i])
        for i in range(count)
    ]
    stores = [
        pltpu.make_async_copy(held.at[part(i)], out_ref.at[part(i)], out_sem.at[i])
        for i in range(count)
    ]
    for load in loads:
        load.start()
    for load, store in zip(loads, stores):
        load.wait()
        store.start()
    for store in stores:
        store.wait()


def pass_on(values, parts=8):
    flat = values.reshape(-1, values.shape[-1])
    hbm = pl.BlockSpec(memory_space=pl.ANY)
    dma = pltpu.SemaphoreType.DMA
    return pl.pallas_call(
        pass_on_kernel,
        out_shape=jax.ShapeDtypeStruct(flat.shape, flat.dtype),
        in_specs=[hbm],
        out_specs=hbm,
        scratch_shapes=[pltpu.VMEM(flat.shape, flat.dtype), dma((parts,)), dma((parts,))],
    )(flat).reshape(values.shape)


def fused(
    initial_warmth,
    pattern_choice,
    dissipation_tables,
    material_label,
    intercept_kappa,
    sensitivity_coef,
):
    steps = pattern_choice.shape[0]
    strip, length = initial_warmth.shape
    tm_count, rows_count = lax.axis_size("tm"), lax.axis_size("rows")
    chunks = length // rows_count // LANES
    column_cos = cosine_table(length)
    forward, inverse = two_parts(column_cos.T), two_parts(column_cos)
    mu = 2.0 - 2.0 * np.cos(np.arange(length) * (math.pi / length))
    mup = np.broadcast_to(mu[:, None], (length, LANES)).astype(np.float32)
    muq = np.broadcast_to(mu.reshape(rows_count * chunks, 1, LANES), (rows_count * chunks, 8, LANES))
    scratch = scratch_of(steps, strip, length, tm_count, rows_count)
    names = INPUTS + ["out"] + list(scratch)
    smem, vmem, hbm = (
        pl.BlockSpec(memory_space=space) for space in (pltpu.SMEM, pltpu.VMEM, pl.ANY)
    )
    result = pl.pallas_call(
        lambda *refs: fused_kernel(steps, strip, length, tm_count, rows_count, names, *refs),
        out_shape=jax.ShapeDtypeStruct((steps, strip, length), F32),
        in_specs=[vmem, smem, vmem, smem, smem, smem, vmem, vmem] + [hbm] * 4,
        out_specs=hbm,
        scratch_shapes=list(scratch.values()),
        compiler_params=pltpu.CompilerParams(
            collective_id=0, has_side_effects=True, vmem_limit_bytes=67043328
        ),
    )(
        initial_warmth,
        pattern_choice,
        dissipation_tables,
        material_label,
        intercept_kappa,
        sensitivity_coef,
        jnp.asarray(mup),
        jnp.asarray(muq.astype(np.float32)),
        *inverse,
        *forward,
    )
    return pass_on(result)


def pick(initial_warmth, pattern_choice, *rest):
    strip, width = initial_warmth.shape
    tm_count, rows_count = lax.axis_size("tm"), lax.axis_size("rows")
    aligned = (
        pattern_choice.shape[0] == 2
        and strip * rows_count == width
        and strip % TILE == 0
        and width == rows_count * 2 * LANES
        and width % (4 * LANES) == 0
        and tm_count % 2 == 0
        and rows_count % 2 == 0
    )
    return (fused if aligned else shards)(initial_warmth, pattern_choice, *rest)


def solution(mesh):
    in_specs = (P("rows", None), P("tm", None, None), P(), P(), P(), P())
    out_specs = P("tm", "rows", None)
    return jax.shard_map(pick, mesh=mesh, in_specs=in_specs, out_specs=out_specs, check_vma=False)
```

```python
import math
from types import SimpleNamespace

import jax
import jax.numpy as jnp
import numpy as np
from jax import lax
from jax.experimental import pallas as pl
from jax.experimental.pallas import tpu as pltpu
from jax.sharding import PartitionSpec as P

TILE = 128
ITERS = 2
TIMESTEP_SIZE = 2.0
ALPHA = 0.05
CROSS_WEIGHT = 1.0 / 64.0
F32 = jnp.float32
BF16 = jnp.bfloat16


def extended(block, axis, dim):
    count = lax.axis_size(axis)
    forward = [(i, i + 1) for i in range(count - 1)]
    backward = [(target, source) for source, target in forward]
    low = lax.ppermute(
        lax.slice_in_dim(block, block.shape[dim] - 1, None, axis=dim), axis, forward
    )
    high = lax.ppermute(lax.slice_in_dim(block, 0, 1, axis=dim), axis, backward)
    return jnp.concatenate([low, block, high], axis=dim)


def cosine_table(length):
    modes = np.arange(length, dtype=np.int64)[:, None]
    cells = np.arange(length, dtype=np.int64)[None, :]
    phase = modes * (2 * cells + 1) % (4 * length)
    return np.cos(phase * (math.pi / (2 * length)))


def two_parts(table):
    high = np.asarray(table, dtype=np.float32).astype(BF16)
    low = (table - high.astype(np.float64)).astype(np.float32).astype(BF16)
    return jnp.asarray(high), jnp.asarray(low)


def split(values):
    high = values.astype(BF16)
    return high, (values - high.astype(F32)).astype(BF16)


def mul(left, right):
    return jnp.dot(left, right, preferred_element_type=F32)


def columns_kernel(x_ref, high_ref, low_ref, out_ref, x_high, x_low):
    @pl.when(pl.program_id(0) == 0)
    def _():
        x_high[...], x_low[...] = split(x_ref[...])

    high = high_ref[...]
    out_ref[...] = (
        mul(x_high[...], high) + mul(x_low[...], high) + mul(x_high[...], low_ref[...])
    )


def times_table(values, table):
    rows, depth = values.shape
    width = table[0].shape[1]
    block = min(256, width)
    return pl.pallas_call(
        columns_kernel,
        grid=(width // block,),
        out_shape=jax.ShapeDtypeStruct((rows, width), F32),
        in_specs=[
            pl.BlockSpec((rows, depth), lambda i: (0, 0)),
            pl.BlockSpec((depth, block), lambda i: (0, i)),
            pl.BlockSpec((depth, block), lambda i: (0, i)),
        ],
        out_specs=pl.BlockSpec((rows, block), lambda i: (0, i)),
        scratch_shapes=[pltpu.VMEM((rows, depth), BF16)] * 2,
    )(values, *table)


def rows_kernel(high_ref, low_ref, x_ref, out_ref, x_high, x_low):
    @pl.when(pl.program_id(0) == 0)
    def _():
        x_high[...], x_low[...] = split(x_ref[...])

    for n in range(x_ref.shape[0]):
        out_ref[n] = (
            mul(high_ref[...], x_high[n])
            + mul(high_ref[...], x_low[n])
            + mul(low_ref[...], x_high[n])
        )


def table_times(table, values):
    steps, depth, width = values.shape
    height = table[0].shape[0]
    block = min(256, height)
    return pl.pallas_call(
        rows_kernel,
        grid=(height // block,),
        out_shape=jax.ShapeDtypeStruct((steps, height, width), F32),
        in_specs=[
            pl.BlockSpec((block, depth), lambda i: (i, 0)),
            pl.BlockSpec((block, depth), lambda i: (i, 0)),
            pl.BlockSpec((steps, depth, width), lambda i: (0, 0, 0)),
        ],
        out_specs=pl.BlockSpec((steps, block, width), lambda i: (0, i, 0)),
        scratch_shapes=[pltpu.VMEM((steps, depth, width), BF16)] * 2,
    )(*table, values)


def power_kernel(choice_ref, table_ref, out_ref):
    steps, blocks, _, width = out_ref.shape
    across = width // TILE
    for n in range(steps):
        for b in range(blocks):
            for x in range(across):
                picked = choice_ref[n, b * across + x]
                out_ref[n, b, :, x * TILE : (x + 1) * TILE] = table_ref[picked]


def power_of(pattern_choice, tables, first_row, strip, width):
    steps = pattern_choice.shape[0]
    part = min(TILE, strip)
    blocks = strip // part
    offset = first_row % TILE if strip < TILE else 0
    tiles = lax.dynamic_slice_in_dim(tables, offset, part, axis=1)
    chosen = lax.dynamic_slice_in_dim(pattern_choice, first_row // TILE, blocks, axis=1)
    power = pl.pallas_call(
        power_kernel,
        out_shape=jax.ShapeDtypeStruct((steps, blocks, part, width), F32),
        in_specs=[
            pl.BlockSpec(memory_space=pltpu.SMEM),
            pl.BlockSpec(memory_space=pltpu.VMEM),
        ],
        out_specs=pl.BlockSpec(memory_space=pltpu.VMEM),
    )(chosen.reshape(steps, -1), tiles)
    return power.reshape(steps, strip, width)


def divergence(warmth, kappa, inner):
    def face(low, high):
        return 1.0 if kappa is None else 0.5 * (low + high)

    k = warmth if kappa is None else kappa
    upward = face(k[:, 1:], k[:, :-1]) * (warmth[:, 1:] - warmth[:, :-1])
    upward = jnp.where(inner[None, :, None], upward, 0.0)
    centre, k_mid = warmth[:, 1:-1], k[:, 1:-1]
    lateral = CROSS_WEIGHT * (
        face(k_mid[:, :, 1:], k_mid[:, :, :-1]) * (centre[:, :, 1:] - centre[:, :, :-1])
    )
    zero = jnp.zeros_like(centre[:, :, :1])
    across = jnp.concatenate([lateral, zero], 2) - jnp.concatenate([zero, lateral], 2)
    return upward[:, 1:] - upward[:, :-1] + across


def mode_factors(row_ids, column_ids, height, width, conduct):
    mu_rows = 2.0 - 2.0 * jnp.cos(row_ids.astype(F32) * (math.pi / height))
    mu_cols = 2.0 - 2.0 * jnp.cos(column_ids.astype(F32) * (math.pi / width))
    rate = conduct * (mu_rows[:, None] + CROSS_WEIGHT * mu_cols[None, :])
    gain = 1.0 / (1.0 / TIMESTEP_SIZE + rate)
    return gain, gain * (1.0 / TIMESTEP_SIZE)


def shards(
    initial_warmth,
    pattern_choice,
    dissipation_tables,
    material_label,
    intercept_kappa,
    sensitivity_coef,
):
    steps = pattern_choice.shape[0]
    strip, width = initial_warmth.shape
    tm_count = lax.axis_size("tm")
    rows_count = lax.axis_size("rows")
    height = strip * rows_count
    first_row = lax.axis_index("rows") * strip
    power = power_of(pattern_choice, dissipation_tables, first_row, strip, width)

    padded_rows = first_row - 1 + jnp.arange(strip + 2, dtype=jnp.int32)
    labels = jnp.take(material_label, jnp.clip(padded_rows, 0, height - 1) // TILE, axis=0)
    base_tiles = jnp.zeros(labels.shape, F32)
    slope_tiles = jnp.zeros(labels.shape, F32)
    for label in range(intercept_kappa.shape[0]):
        base_tiles = jnp.where(labels == label, intercept_kappa[label], base_tiles)
        slope_tiles = jnp.where(labels == label, sensitivity_coef[label], slope_tiles)
    base = jnp.repeat(base_tiles, TILE, axis=1)[None]
    slope = jnp.repeat(slope_tiles, TILE, axis=1)[None]
    upper_rows = padded_rows[:-1]
    inner = (upper_rows >= 0) & (upper_rows + 1 <= height - 1)
    conduct = jnp.mean(intercept_kappa)

    column_cos = cosine_table(width)
    row_cos = cosine_table(height)
    columns_out, columns_in = two_parts(column_cos.T), two_parts(column_cos)
    if height == width:
        rows_out, rows_in = columns_in, columns_out
    else:
        rows_out, rows_in = two_parts(row_cos), two_parts(row_cos.T)

    narrow = width // rows_count
    share = height // tm_count
    column_ids = lax.axis_index("rows") * narrow + jnp.arange(narrow, dtype=jnp.int32)
    all_rows = jnp.arange(height, dtype=jnp.int32)
    own_rows = lax.axis_index("tm") * share + jnp.arange(share, dtype=jnp.int32)
    gain, keep = mode_factors(all_rows, column_ids, height, width, conduct)
    weight = (jnp.where(all_rows == 0, 1.0, 2.0) / height)[:, None] * (
        jnp.where(column_ids == 0, 1.0, 2.0) / width
    )[None, :]
    _, own_keep = mode_factors(own_rows, column_ids, height, width, conduct)
    block_keep = own_keep
    for _ in range(steps - 1):
        block_keep = block_keep * own_keep
    around = block_keep
    for _ in range(tm_count - 1):
        around = around * block_keep
    closing = ALPHA / (1.0 - ALPHA * around)
    first_block = lax.axis_index("tm") == 0

    start = extended(initial_warmth[None], "rows", 1)
    start_div = divergence(start, base * (1.0 + slope * jnp.tanh(start)), inner)
    warmth = jnp.broadcast_to(initial_warmth[None], (steps, strip, width))
    wrapped = None
    for sweep in range(ITERS):
        if sweep == 0:
            resid = power + start_div
        else:
            grid = extended(warmth, "rows", 1)
            div = divergence(grid, base * (1.0 + slope * jnp.tanh(grid)), inner)
            resid = div - last_div - conduct * divergence(grid - last_grid, None, inner)
        modes = times_table(resid.reshape(steps * strip, width), columns_out)
        modes = lax.all_to_all(
            modes.reshape(steps, strip, width), "rows", split_axis=2, concat_axis=1, tiled=True
        )
        modes = table_times(rows_out, modes)
        sources = [modes[n] * weight for n in range(steps)]
        if wrapped is not None:
            sources[0] = sources[0] - jnp.where(first_block, wrapped / TIMESTEP_SIZE, 0.0)
        sources = [gain * source for source in sources]
        block_end = sources[0]
        for source in sources[1:]:
            block_end = source + keep * block_end
        ends = lax.all_to_all(block_end, "tm", split_axis=0, concat_axis=0, tiled=True)
        ends = ends.reshape(tm_count, share, narrow)
        last = ends[0]
        for k in range(1, tm_count):
            last = ends[k] + block_keep * last
        entry = [closing * last]
        for k in range(tm_count - 1):
            entry.append(ends[k] + block_keep * entry[k])
        entry = jnp.concatenate(entry, 0)
        carry = lax.all_to_all(entry, "tm", split_axis=0, concat_axis=0, tiled=True)
        wrapped = carry
        solved = []
        for source in sources:
            carry = source + keep * carry
            solved.append(carry)
        field = table_times(rows_in, jnp.stack(solved, 0))
        field = lax.all_to_all(field, "rows", split_axis=1, concat_axis=2, tiled=True)
        update = times_table(field.reshape(steps * strip, width), columns_in)
        if sweep == 0:
            last_grid, last_div = start, start_div
        else:
            last_grid, last_div = grid, div
        warmth = warmth + update.reshape(steps, strip, width)
    return warmth


LANES = 128
EDGE = 8
ROWS = 32
UNIT = 128
MESH = pl.DeviceIdType.MESH


def dot3(left_high, left_low, right_high, right_low):
    return mul(left_high, right_high) + mul(left_low, right_high) + mul(left_high, right_low)


def remote(src, dst, send_sem, recv_sem, device):
    return pltpu.make_async_remote_copy(
        src_ref=src,
        dst_ref=dst,
        send_sem=send_sem,
        recv_sem=recv_sem,
        device_id=device,
        device_id_type=MESH,
    )


def scratch_of(steps, strip, length, tm_count, rows_count):
    narrow = length // rows_count
    chunks = narrow // LANES
    half = length // 2
    units = half // UNIT
    wide = steps * LANES
    padded = strip + 2 * EDGE

    def f32(*shape):
        return pltpu.VMEM(shape, F32)

    def b16(*shape):
        return pltpu.VMEM(shape, BF16)

    dma = pltpu.SemaphoreType.DMA
    return dict(
        ch=b16(length, length),
        cl=b16(length, length),
        cth=b16(length, length),
        ctl=b16(length, length),
        ph=b16(length, length),
        pl=b16(length, length),
        th=b16(8, TILE, TILE),
        tl=b16(8, TILE, TILE),
        base=f32(8, length),
        slope=f32(8, length),
        w0p=f32(padded, length),
        kp=f32(padded, length),
        halo=f32(2, EDGE, length),
        dst=f32(rows_count, strip, narrow),
        oh=b16(length, narrow),
        ol=b16(length, narrow),
        xd=f32(length, narrow),
        xh=b16(chunks, length, wide),
        xl=b16(chunks, length, wide),
        fx=f32(chunks, rows_count, strip, wide),
        xr=f32(chunks, length, wide),
        ss=f32(chunks, length, wide),
        e=f32(ITERS, chunks, length, LANES),
        er=f32(ITERS, chunks, half, LANES),
        fin=f32(ITERS, chunks, half, LANES),
        sin=f32(ITERS, chunks, half, LANES),
        fout=f32(ITERS, chunks, half, LANES),
        sout=f32(ITERS, chunks, half, LANES),
        cs=f32(ITERS, chunks, half, LANES),
        zz=f32(chunks, half, LANES),
        carry=f32(ITERS, chunks, length, LANES),
        gw=f32(chunks, length, LANES),
        keep=f32(chunks, length, LANES),
        rho=f32(chunks, length, LANES),
        sd=f32(chunks, length, LANES),
        k1=f32(chunks, half, LANES),
        k2=f32(chunks, half, LANES),
        pa=f32(chunks, half, LANES),
        pb=f32(chunks, half, LANES),
        pf=f32(chunks, half, LANES),
        iy=f32(ITERS, chunks, length + 2 * EDGE, wide),
        yr=f32(ITERS, chunks, rows_count, padded, wide),
        uh=b16(length, wide),
        ul=b16(length, wide),
        lh=b16(steps * padded, rows_count * LANES),
        ll=b16(steps * padded, rows_count * LANES),
        u1p=f32(steps * padded, length),
        outv=f32(steps, strip, length),
        osem=dma((length // (2 * LANES),)),
        tsem=dma((4,)),
        hs=dma((2,)),
        hr=dma((2,)),
        ds=dma((rows_count,)),
        dr=dma((rows_count,)),
        xs=dma((chunks * rows_count,)),
        xrs=dma((chunks * rows_count,)),
        ys=dma((ITERS * chunks * rows_count,)),
        yrs=dma((ITERS * chunks * rows_count,)),
        es=dma((ITERS * chunks,)),
        ers=dma((chunks * units,)),
        fs=dma((ITERS * chunks,)),
        frs=dma((chunks * units,)),
        gs=dma((ITERS * chunks,)),
        grs=dma((chunks * units,)),
        cts=dma((ITERS * chunks,)),
        crs=dma((chunks * units,)),
    )


INPUTS = [
    "w0",
    "choice",
    "tables",
    "label",
    "icpt",
    "sens",
    "mup",
    "muq",
    "chh",
    "clh",
    "cthh",
    "ctlh",
]


def fused_kernel(steps, strip, length, tm_count, rows_count, names, *refs):
    s = SimpleNamespace(**dict(zip(names, refs)))
    narrow = length // rows_count
    chunks = narrow // LANES
    half = length // 2
    units = half // UNIT
    padded = strip + 2 * EDGE
    blocks = strip // TILE
    tiles = length // TILE
    big = 2 * LANES
    zs, ys_count = tm_count // 2, rows_count // 2

    t, r = lax.axis_index("tm"), lax.axis_index("rows")
    z, x = lax.div(t, 2), lax.rem(t, 2)
    y, c = lax.div(r, 2), lax.rem(r, 2)
    pair = t + 1 - 2 * x
    peers = [(dy, dc) for dy in range(1, ys_count) for dc in range(2)] + [(0, 1)]

    def to(dy, dc):
        return lax.rem(y + dy, ys_count) * 2 + lax.rem(c + dc, 2)

    def frm(dy, dc):
        return lax.rem(y + ys_count - dy, ys_count) * 2 + lax.rem(c + 2 - dc, 2)

    def rows_at(start, size):
        return pl.ds(pl.multiple_of(start, size), size)

    tables_in = [
        pltpu.make_async_copy(a, b, s.tsem.at[i])
        for i, (a, b) in enumerate(
            [(s.cthh, s.cth), (s.ctlh, s.ctl), (s.chh, s.ch), (s.clh, s.cl)]
        )
    ]
    for copy in tables_in:
        copy.start()

    barrier = pltpu.get_barrier_semaphore()
    for dy, dc in peers:
        pl.semaphore_signal(barrier, inc=1, device_id=(t, to(dy, dc)), device_id_type=MESH)
    pl.semaphore_signal(barrier, inc=1, device_id=(pair, r), device_id_type=MESH)

    @pl.when(z > 0)
    def _():
        pl.semaphore_signal(barrier, inc=1, device_id=(t - 2, r), device_id_type=MESH)

    @pl.when(z < zs - 1)
    def _():
        pl.semaphore_signal(barrier, inc=1, device_id=(t + 2, r), device_id_type=MESH)

    def halo_down(to_row):
        return remote(
            s.w0.at[pl.ds(strip - EDGE, EDGE)], s.halo.at[0], s.hs.at[0], s.hr.at[0], (t, to_row)
        )

    def halo_up(to_row):
        return remote(s.w0.at[pl.ds(0, EDGE)], s.halo.at[1], s.hs.at[1], s.hr.at[1], (t, to_row))

    count = s.icpt.shape[0]
    total = s.icpt[0]
    for i in range(1, count):
        total = total + s.icpt[i]
    conduct = total / count
    for i in range(blocks + 2):
        ty = lax.min(lax.max(r * blocks - 1 + i, 0), tiles - 1)
        for tx in range(tiles):
            label = s.label[ty, tx]
            s.base[i : i + 1, tx * TILE : (tx + 1) * TILE] = jnp.full((1, TILE), s.icpt[label], F32)
            s.slope[i : i + 1, tx * TILE : (tx + 1) * TILE] = jnp.full((1, TILE), s.sens[label], F32)

    def factors_of(j):

        def factors(i, _):
            rows = rows_at(i * LANES, LANES)
            rate = conduct * (s.mup[rows] + CROSS_WEIGHT * s.muq[j * rows_count + r, 0:1, :])
            gain = 1.0 / (1.0 / TIMESTEP_SIZE + rate)
            keep = gain * (1.0 / TIMESTEP_SIZE)
            p = i * LANES + lax.broadcasted_iota(jnp.int32, (LANES, LANES), 0)
            q = (j * rows_count + r) * LANES + lax.broadcasted_iota(jnp.int32, (LANES, LANES), 1)
            weight = (jnp.where(p == 0, 1.0, 2.0) / length) * (jnp.where(q == 0, 1.0, 2.0) / length)
            s.gw[j, rows] = gain * weight
            s.keep[j, rows] = keep
            one = 1.0 + keep
            k = keep * keep
            around, power = one, k
            for _ in range(tm_count - 1):
                around = one + k * around
                power = power * k
            first = ALPHA * around / (1.0 - ALPHA * power)
            s.rho[j, rows] = lax.fori_loop(0, t, lambda _, a: one + k * a, first)
            return 0

        lax.fori_loop(0, length // LANES, factors, 0)

        def chain(i, _):
            rows = rows_at(i * UNIT, UNIT)
            keep = s.keep[j, rows_at(x * half + i * UNIT, UNIT)]
            k = keep * keep
            k2 = k * k
            ones = jnp.ones_like(k)
            whole = k2
            for _ in range(zs - 1):
                whole = whole * k2
            upper = lax.fori_loop(0, zs - 1 - z, lambda _, a: a * k2, ones)
            lower = lax.fori_loop(0, z, lambda _, a: a * k2, ones)
            close = lower * (ALPHA / (1.0 - ALPHA * whole))
            s.k1[j, rows] = k
            s.k2[j, rows] = k2
            s.pa[j, rows] = upper
            s.pb[j, rows] = close
            s.pf[j, rows] = 1.0 + close * (upper * k2)
            return 0

        lax.fori_loop(0, units, chain, 0)

    factors_of(0)

    @pl.when(z == 0)
    def _():
        s.fin[...] = jnp.zeros_like(s.fin)

    @pl.when(z == zs - 1)
    def _():
        s.sin[...] = jnp.zeros_like(s.sin)

    for j in range(chunks):
        s.iy[0, j, 0:EDGE] = jnp.zeros((EDGE, steps * LANES), F32)
        s.iy[0, j, length + EDGE :] = jnp.zeros((EDGE, steps * LANES), F32)
    for k in range(s.tables.shape[0]):
        s.th[k], s.tl[k] = split(s.tables[k])

    def kappa(offset):
        def part(start, size, i):
            rows = pl.ds(start, size)
            warmth = s.w0p[rows]
            if offset is not None:
                warmth = warmth + s.u1p[pl.ds(pl.multiple_of(offset + start, EDGE), size)]
            bent = s.slope[i : i + 1] * jnp.tanh(warmth)
            s.kp[rows] = s.base[i : i + 1] * (1.0 + bent)

        part(0, EDGE, 0)
        part(EDGE + strip, EDGE, blocks + 1)
        for b in range(blocks):

            def inner(i, _, b=b):
                part(pl.multiple_of(EDGE + b * TILE + i * ROWS, EDGE), ROWS, b + 1)
                return 0

            lax.fori_loop(0, TILE // ROWS, inner, 0)

    lane = lax.broadcasted_iota(jnp.int32, (ROWS, length), 1)
    ext = ROWS + 2 * EDGE

    def forcing(offset, out_row):
        def inner(i, _):
            rows = pl.ds(pl.multiple_of(i * ROWS, ROWS), ext)
            warmth, k = s.w0p[rows], s.kp[rows]
            mid = slice(EDGE, EDGE + ROWS)
            if offset is not None:
                warmth = warmth + s.u1p[pl.ds(pl.multiple_of(offset + i * ROWS, EDGE), ext)]

            def flux(shift, w, k):
                return 0.5 * (k + shift(k)) * (shift(w) - w)

            down = flux(lambda v: pltpu.roll(v, ext - 1, 0), warmth, k)
            total = (down - pltpu.roll(down, 1, 0))[mid]
            right = flux(lambda v: pltpu.roll(v, length - 1, 1), warmth[mid], k[mid])
            right = jnp.where(lane < length - 1, right, 0.0)
            total = total + CROSS_WEIGHT * (right - pltpu.roll(right, 1, 1))
            rows = pl.ds(pl.multiple_of(out_row + i * ROWS, ROWS), ROWS)
            s.ph[rows], s.pl[rows] = split(total)
            return 0

        lax.fori_loop(0, strip // ROWS, inner, 0)

    def send_d(dy, dc):
        n, target = dy * 2 + dc, to(dy, dc)
        rows = rows_at(r * strip, strip)
        return remote(s.dst.at[target], s.xd.at[rows], s.ds.at[n], s.dr.at[n], (t, target))

    beside = lax.min(z, 1) + lax.min(zs - 1 - z, 1)
    pl.semaphore_wait(barrier, len(peers) + 1 + beside)

    @pl.when(r < rows_count - 1)
    def _():
        halo_down(r + 1).start()

    @pl.when(r > 0)
    def _():
        halo_up(r - 1).start()

    tables_in[0].wait()
    tables_in[1].wait()

    for j in range(chunks):
        columns = rows_at((j * rows_count + r) * LANES, LANES)
        s.oh[:, j * LANES : (j + 1) * LANES] = s.cth[:, columns]
        s.ol[:, j * LANES : (j + 1) * LANES] = s.ctl[:, columns]

    def power(n, _):
        def place(ty, _):
            rows = rows_at(ty * TILE, TILE)
            for tx in range(tiles):
                picked = s.choice[n, ty, tx]
                s.ph[rows, tx * TILE : (tx + 1) * TILE] = s.th[picked]
                s.pl[rows, tx * TILE : (tx + 1) * TILE] = s.tl[picked]
            return 0

        lax.fori_loop(0, tiles, place, 0)

        def across(i, _):
            rows = rows_at(i * half, half)
            out = dot3(s.ph[rows], s.pl[rows], s.oh[...], s.ol[...])
            high, low = split(out)
            lanes = rows_at(n * LANES, LANES)
            for j in range(chunks):
                s.xh[j, rows, lanes] = high[:, j * LANES : (j + 1) * LANES]
                s.xl[j, rows, lanes] = low[:, j * LANES : (j + 1) * LANES]
            return 0

        lax.fori_loop(0, 2, across, 0)
        return 0

    lax.fori_loop(0, steps, power, 0)
    tables_in[2].wait()
    tables_in[3].wait()

    def unit(sweep, j, i):
        return j * units + i

    def send_e(sweep, j, i, size=UNIT):
        n = unit(sweep, j, i)
        return remote(
            s.e.at[sweep, j, rows_at((1 - x) * half + i * size, size)],
            s.er.at[sweep, j, rows_at(i * size, size)],
            s.es.at[sweep * chunks + j],
            s.ers.at[n],
            (pair, r),
        )

    def send_f(sweep, j, i, device, size=UNIT):
        n = unit(sweep, j, i)
        rows = rows_at(i * size, size)
        return remote(
            s.fout.at[sweep, j, rows], s.fin.at[sweep, j, rows], s.fs.at[sweep * chunks + j], s.frs.at[n], device
        )

    def send_s(sweep, j, i, device, size=UNIT):
        n = unit(sweep, j, i)
        rows = rows_at(i * size, size)
        return remote(
            s.sout.at[sweep, j, rows], s.sin.at[sweep, j, rows], s.gs.at[sweep * chunks + j], s.grs.at[n], device
        )

    def send_c(sweep, j, i, size=UNIT):
        n = unit(sweep, j, i)
        return remote(
            s.cs.at[sweep, j, rows_at(i * size, size)],
            s.carry.at[sweep, j, rows_at(x * half + i * size, size)],
            s.cts.at[sweep * chunks + j],
            s.crs.at[n],
            (pair, r),
        )

    is_first = jnp.where(t == 0, 1.0, 0.0)

    def rows_out(sweep, j, action=None, beside_j=0, at_once=False):
        parts = length // big
        per = big // UNIT

        def part(i, _):
            rows = rows_at(lax.rem(i + (1 - x) * (parts // 2), parts) * big, big)
            out = dot3(s.ch[rows], s.cl[rows], s.xh[j], s.xl[j])
            gw, keep = s.gw[j, rows], s.keep[j, rows]
            first, second = out[:, :LANES] * gw, out[:, LANES:] * gw
            if sweep > 0:
                first = first + s.ss[j, rows, :LANES]
                second = second + s.ss[j, rows, LANES:]
            s.ss[j, rows, :LANES] = first
            s.ss[j, rows, LANES:] = second
            s.e[sweep, j, rows] = second + keep * first

            @pl.when(i < parts // 2)
            def _():
                for n in range(per):
                    send_e(sweep, j, i * per + n).start()

            if at_once:

                @pl.when(i == 0)
                def _():
                    some(action, sweep, beside_j, 0, units)
            else:
                share(action, sweep, beside_j, i, parts)
            return 0

        lax.fori_loop(0, parts, part, 0)

    def halves(sweep, j, i):
        mine = s.e[sweep, j, rows_at(x * half + i * UNIT, UNIT)]
        other = s.er[sweep, j, rows_at(i * UNIT, UNIT)]
        return jnp.where(x == 0, mine, other), jnp.where(x == 0, other, mine)

    def repeat(sweep, j, *actions):
        def body(i, _):
            for action in actions:
                action(sweep, j, i)
            return 0

        lax.fori_loop(0, units, body, 0)

    def pair_up(sweep, j, i):
        rows = rows_at(i * UNIT, UNIT)
        send_e(sweep, j, i).wait_recv()
        even, odd = halves(sweep, j, i)
        block = odd + s.k1[j, rows] * even
        s.zz[j, rows] = block

        @pl.when(z == 0)
        def _():
            s.fout[sweep, j, rows] = block
            send_f(sweep, j, i, (t + 2, r)).start()

        @pl.when(z == zs - 1)
        def _():
            s.sout[sweep, j, rows] = block
            send_s(sweep, j, i, (t - 2, r)).start()

    def relay_f(sweep, j, i):
        rows = rows_at(i * UNIT, UNIT)

        @pl.when(z > 0)
        def _():
            send_f(sweep, j, i, (t, r)).wait_recv()

            @pl.when(z < zs - 1)
            def _():
                s.fout[sweep, j, rows] = s.zz[j, rows] + s.k2[j, rows] * s.fin[sweep, j, rows]
                send_f(sweep, j, i, (t + 2, r)).start()

    def relay_s(sweep, j, i):
        rows = rows_at(i * UNIT, UNIT)

        @pl.when(z < zs - 1)
        def _():
            send_s(sweep, j, i, (t, r)).wait_recv()
            s.sout[sweep, j, rows] = s.sin[sweep, j, rows] + s.pa[j, rows] * s.zz[j, rows]

            @pl.when(z > 0)
            def _():
                send_s(sweep, j, i, (t - 2, r)).start()

    def finish(sweep, j, i):
        rows = rows_at(i * UNIT, UNIT)
        even, _ = halves(sweep, j, i)
        lower = s.fin[sweep, j, rows] * s.pf[j, rows] + s.pb[j, rows] * s.sout[sweep, j, rows]
        upper = even + s.k1[j, rows] * lower
        s.carry[sweep, j, rows_at(x * half + i * UNIT, UNIT)] = jnp.where(x == 0, lower, upper)
        s.cs[sweep, j, rows] = jnp.where(x == 0, upper, lower)
        send_c(sweep, j, i).start()

    def relay_near(sweep, j, i):
        @pl.when(z < zs // 2)
        def _():
            relay_f(sweep, j, i)

        @pl.when(z >= zs // 2)
        def _():
            relay_s(sweep, j, i)

    def relay_away(sweep, j, i):
        @pl.when(z < zs // 2)
        def _():
            relay_s(sweep, j, i)

        @pl.when(z >= zs // 2)
        def _():
            relay_f(sweep, j, i)

        finish(sweep, j, i)

    def some(action, sweep, j, first, last):
        def body(i, _):
            action(sweep, j, i)
            return 0

        lax.fori_loop(first, last, body, 0)

    def share(action, sweep, j, i, parts):
        if action is not None:
            some(action, sweep, j, i * (units // parts), (i + 1) * (units // parts))

    inner = (z > 0) & (z < zs - 1)

    def by_place(relaying, ending):
        @pl.when(inner)
        def _():
            relaying()

        @pl.when(jnp.logical_not(inner))
        def _():
            ending()

    def send_y(sweep, j, dy, dc):
        n, target = (sweep * chunks + j) * rows_count + dy * 2 + dc, to(dy, dc)
        size = padded if sweep == 0 else strip
        start = target * strip if sweep == 0 else target * strip + EDGE
        return remote(
            s.iy.at[sweep, j, pl.ds(pl.multiple_of(start, EDGE), size)],
            s.yr.at[sweep, j, r, pl.ds(0, size)],
            s.ys.at[n],
            s.yrs.at[n],
            (t, target),
        )

    def rows_in(sweep, j, action=None):
        some(lambda *which: send_c(*which).wait_recv(), sweep, j, 0, units)

        def solve(i, _):
            rows = rows_at(i * LANES, LANES)
            keep, carry = s.keep[j, rows], s.carry[sweep, j, rows]
            first, second = s.ss[j, rows, :LANES], s.ss[j, rows, LANES:]
            if sweep == 0:
                steady = s.sd[j, rows]
                first, second = first + steady, second + steady
                carry = carry + s.rho[j, rows] * steady
            first = first + keep * carry
            second = second + keep * first
            if sweep == 0:
                left = (1.0 - keep) * first - steady
                s.ss[j, rows, :LANES] = left - is_first * keep * carry
                s.ss[j, rows, LANES:] = (1.0 - keep) * second - steady
            s.uh[rows, :LANES], s.ul[rows, :LANES] = split(first)
            s.uh[rows, LANES:], s.ul[rows, LANES:] = split(second)
            return 0

        lax.fori_loop(0, length // LANES, solve, 0)

        def part(i, _):
            dy, q = lax.rem(lax.div(i, 2) + 1, ys_count), lax.rem(i, 2)
            target = lax.rem(y + dy, ys_count) * 2 + q
            rows = rows_at(target * strip, strip)
            out = dot3(s.cth[rows], s.ctl[rows], s.uh[...], s.ul[...])
            s.iy[sweep, j, pl.ds(pl.multiple_of(target * strip + EDGE, EDGE), strip)] = out
            if sweep > 0:

                @pl.when(target != r)
                def _():
                    send_y(sweep, j, dy, lax.rem(q + c, 2)).start()

            share(action, sweep, j + 1, i, rows_count)
            return 0

        lax.fori_loop(0, rows_count, part, 0)
        if sweep == 0:
            for dy, dc in peers:
                send_y(sweep, j, dy, dc).start()
            s.yr[sweep, j, r] = s.iy[sweep, j, pl.ds(pl.multiple_of(r * strip, EDGE), padded)]
        else:
            mid = pl.ds(pl.multiple_of(r * strip + EDGE, EDGE), strip)
            s.yr[sweep, j, r, 0:strip] = s.iy[sweep, j, mid]

    def store(i):
        columns = rows_at(i * big, big)
        return pltpu.make_async_copy(
            s.outv.at[:, :, columns], s.out.at[:, :, columns], s.osem.at[i]
        )

    def columns_in(sweep):
        size = padded if sweep == 0 else strip

        def chunk(j, _):
            for dy, dc in peers:
                send_y(sweep, j, dy, dc).wait_recv()
            for source in range(rows_count):
                high, low = split(s.yr[sweep, j, source, 0:size])
                lanes = slice(source * LANES, (source + 1) * LANES)
                for n in range(steps):
                    part = slice(n * LANES, (n + 1) * LANES)
                    s.lh[n * size : (n + 1) * size, lanes] = high[:, part]
                    s.ll[n * size : (n + 1) * size, lanes] = low[:, part]

            def tile(i, _):
                columns = rows_at(i * big, big)
                depth = rows_at(j * rows_count * LANES, rows_count * LANES)
                rows = slice(0, steps * size)
                out = dot3(s.lh[rows], s.ll[rows], s.ch[depth, columns], s.cl[depth, columns])
                if sweep == 0:
                    s.u1p[:, columns] = s.u1p[:, columns] + out
                else:
                    for n in range(steps):
                        value = s.outv[n, :, columns] + out[n * size : (n + 1) * size]
                        s.outv[n, :, columns] = value

                    @pl.when(j == chunks - 1)
                    def _():
                        store(i).start()

                return 0

            lax.fori_loop(0, length // big, tile, 0)
            return 0

        lax.fori_loop(0, chunks, chunk, 0)

    def send_x(j, dy, dc):
        n, target = j * rows_count + dy * 2 + dc, to(dy, dc)
        rows = rows_at(r * strip, strip)
        return remote(
            s.fx.at[j, target], s.xr.at[j, rows], s.xs.at[n], s.xrs.at[n], (t, target)
        )

    def send_chip(send, dy):
        for q in range(2):
            dc = lax.rem(q + c, 2)

            @pl.when(dy * 2 + dc > 0)
            def _():
                send(dy, dc).start()

    def columns_out():
        def part(i, _):
            n, g = lax.rem(i, steps), lax.div(i, steps)
            dy, j = lax.rem(g + 1, ys_count), lax.div(g, ys_count)
            chip = lax.rem(y + dy, ys_count) * 2
            rows = rows_at(n * strip, strip)
            columns = rows_at((j * rows_count + chip) * LANES, big)
            out = dot3(s.ph[rows], s.pl[rows], s.cth[:, columns], s.ctl[:, columns])
            for q in range(2):
                s.fx[j, chip + q, :, rows_at(n * LANES, LANES)] = out[
                    :, q * LANES : (q + 1) * LANES
                ]

            @pl.when(n == steps - 1)
            def _():
                send_chip(lambda *to_: send_x(j, *to_), dy)

            return 0

        lax.fori_loop(0, chunks * ys_count * steps, part, 0)

    def gather_x(j):
        own = rows_at(r * strip, strip)
        s.xr[j, own] = s.fx[j, r]
        for dy, dc in peers:
            send_x(j, dy, dc).wait_recv()

        def body(i, _):
            rows = rows_at(i * LANES, LANES)
            s.xh[j, rows], s.xl[j, rows] = split(s.xr[j, rows])
            return 0

        lax.fori_loop(0, length // LANES, body, 0)

    def steady_out(action, sweep, beside_j):
        s.w0p[EDGE : EDGE + strip] = s.w0[...]

        @pl.when(r > 0)
        def _():
            halo_down(r).wait_recv()
            s.w0p[0:EDGE] = s.halo[0]

        @pl.when(r == 0)
        def _():
            s.w0p[0:EDGE] = jnp.broadcast_to(s.w0[0:1], (EDGE, length))

        @pl.when(r < rows_count - 1)
        def _():
            halo_up(r).wait_recv()
            s.w0p[EDGE + strip :] = s.halo[1]

        @pl.when(r == rows_count - 1)
        def _():
            s.w0p[EDGE + strip :] = jnp.broadcast_to(s.w0[strip - 1 :], (EDGE, length))

        kappa(None)
        forcing(None, 0)

        def part(i, _):
            j, dy = lax.rem(i, chunks), lax.rem(lax.div(i, chunks) + 1, ys_count)
            chip = lax.rem(y + dy, ys_count) * 2
            columns = rows_at((j * rows_count + chip) * LANES, big)
            out = dot3(s.ph[0:strip], s.pl[0:strip], s.cth[:, columns], s.ctl[:, columns])
            for q in range(2):
                s.dst[chip + q, :, rows_at(j * LANES, LANES)] = out[:, q * LANES : (q + 1) * LANES]

            @pl.when(j == chunks - 1)
            def _():
                send_chip(send_d, dy)

            share(action, sweep, beside_j, i, chunks * ys_count)
            return 0

        lax.fori_loop(0, chunks * ys_count, part, 0)
        s.xd[rows_at(r * strip, strip)] = s.dst[r]

    def steady_in():
        for dy, dc in peers:
            send_d(dy, dc).wait_recv()

        def spread(i, _):
            rows = rows_at(i * LANES, LANES)
            s.xh[0, rows], s.xl[0, rows] = split(s.xd[rows])
            return 0

        lax.fori_loop(0, length // LANES, spread, 0)

        def block(i, _):
            rows = rows_at(i * big, big)
            out = dot3(s.ch[rows], s.cl[rows], s.xh[0], s.xl[0])
            for j in range(chunks):
                s.sd[j, rows] = out[:, j * LANES : (j + 1) * LANES] * s.gw[j, rows]
            return 0

        lax.fori_loop(0, length // big, block, 0)

    rows_out(0, 0)
    for j in range(1, chunks):
        factors_of(j)
    steady_out(pair_up, 0, 0)
    rows_out(0, 1, relay_near, 0)
    some(relay_away, 0, 0, 0, units)
    some(pair_up, 0, 1, 0, units)
    steady_in()
    rows_in(0, 0, relay_near)
    some(relay_away, 0, 1, 0, units)
    rows_in(0, 1)
    s.u1p[...] = jnp.zeros_like(s.u1p)
    columns_in(0)

    def force(n, _):
        offset = n * padded

        @pl.when(r == 0)
        def _():
            edge = s.u1p[pl.ds(pl.multiple_of(offset + EDGE, EDGE), EDGE)][0:1]
            home = pl.ds(pl.multiple_of(offset, EDGE), EDGE)
            s.u1p[home] = jnp.broadcast_to(edge, (EDGE, length))

        @pl.when(r == rows_count - 1)
        def _():
            edge = s.u1p[pl.ds(pl.multiple_of(offset + strip, EDGE), EDGE)][EDGE - 1 :]
            home = pl.ds(pl.multiple_of(offset + strip + EDGE, EDGE), EDGE)
            s.u1p[home] = jnp.broadcast_to(edge, (EDGE, length))

        kappa(offset)
        forcing(offset, n * strip)
        return 0

    lax.fori_loop(0, steps, force, 0)
    columns_out()
    for n in range(steps):
        first = n * padded + EDGE
        s.outv[n] = s.w0[...] + s.u1p[first : first + strip]
    gather_x(0)
    rows_out(1, 0)
    some(pair_up, 1, 0, 0, units)
    some(relay_near, 1, 0, 0, units)

    def relay_then_rows():
        some(relay_away, 1, 0, 0, units)
        gather_x(1)
        rows_out(1, 1)

    def rows_then_end():
        gather_x(1)
        rows_out(1, 1, relay_away, 0, at_once=True)

    by_place(relay_then_rows, rows_then_end)
    some(pair_up, 1, 1, 0, units)
    rows_in(1, 0, relay_near)
    some(relay_away, 1, 1, 0, units)
    rows_in(1, 1)
    @pl.when(r < rows_count - 1)
    def _():
        halo_down(r + 1).wait_send()

    @pl.when(r > 0)
    def _():
        halo_up(r - 1).wait_send()

    for dy, dc in peers:
        send_d(dy, dc).wait_send()
        for j in range(chunks):
            send_x(j, dy, dc).wait_send()
            send_y(0, j, dy, dc).wait_send()
    for sweep in range(ITERS):
        for j in range(chunks):
            send_e(sweep, j, 0, half).wait_send()
            send_c(sweep, j, 0, half).wait_send()

            @pl.when(z < zs - 1)
            def _():
                send_f(sweep, j, 0, (t + 2, r), half).wait_send()

            @pl.when(z > 0)
            def _():
                send_s(sweep, j, 0, (t - 2, r), half).wait_send()
    columns_in(1)
    for i in range(length // big):
        store(i).wait()
    for dy, dc in peers:
        for j in range(chunks):
            send_y(1, j, dy, dc).wait_send()


def pass_on_kernel(in_ref, out_ref, held, in_sem, out_sem):
    count = in_sem.shape[0]
    rows = in_ref.shape[0] // count

    def part(i):
        return pl.ds(i * rows, rows)

    loads = [
        pltpu.make_async_copy(in_ref.at[part(i)], held.at[part(i)], in_sem.at[i])
        for i in range(count)
    ]
    stores = [
        pltpu.make_async_copy(held.at[part(i)], out_ref.at[part(i)], out_sem.at[i])
        for i in range(count)
    ]
    for load in loads:
        load.start()
    for load, store in zip(loads, stores):
        load.wait()
        store.start()
    for store in stores:
        store.wait()


def pass_on(values, parts=8):
    flat = values.reshape(-1, values.shape[-1])
    hbm = pl.BlockSpec(memory_space=pl.ANY)
    dma = pltpu.SemaphoreType.DMA
    return pl.pallas_call(
        pass_on_kernel,
        out_shape=jax.ShapeDtypeStruct(flat.shape, flat.dtype),
        in_specs=[hbm],
        out_specs=hbm,
        scratch_shapes=[pltpu.VMEM(flat.shape, flat.dtype), dma((parts,)), dma((parts,))],
    )(flat).reshape(values.shape)


def fused(
    initial_warmth,
    pattern_choice,
    dissipation_tables,
    material_label,
    intercept_kappa,
    sensitivity_coef,
):
    steps = pattern_choice.shape[0]
    strip, length = initial_warmth.shape
    tm_count, rows_count = lax.axis_size("tm"), lax.axis_size("rows")
    chunks = length // rows_count // LANES
    column_cos = cosine_table(length)
    forward, inverse = two_parts(column_cos.T), two_parts(column_cos)
    mu = 2.0 - 2.0 * np.cos(np.arange(length) * (math.pi / length))
    mup = np.broadcast_to(mu[:, None], (length, LANES)).astype(np.float32)
    muq = np.broadcast_to(mu.reshape(rows_count * chunks, 1, LANES), (rows_count * chunks, 8, LANES))
    scratch = scratch_of(steps, strip, length, tm_count, rows_count)
    names = INPUTS + ["out"] + list(scratch)
    smem, vmem, hbm = (
        pl.BlockSpec(memory_space=space) for space in (pltpu.SMEM, pltpu.VMEM, pl.ANY)
    )
    result = pl.pallas_call(
        lambda *refs: fused_kernel(steps, strip, length, tm_count, rows_count, names, *refs),
        out_shape=jax.ShapeDtypeStruct((steps, strip, length), F32),
        in_specs=[vmem, smem, vmem, smem, smem, smem, vmem, vmem] + [hbm] * 4,
        out_specs=hbm,
        scratch_shapes=list(scratch.values()),
        compiler_params=pltpu.CompilerParams(
            collective_id=0, has_side_effects=True, vmem_limit_bytes=67043328
        ),
    )(
        initial_warmth,
        pattern_choice,
        dissipation_tables,
        material_label,
        intercept_kappa,
        sensitivity_coef,
        jnp.asarray(mup),
        jnp.asarray(muq.astype(np.float32)),
        *inverse,
        *forward,
    )
    return pass_on(result)


def pick(initial_warmth, pattern_choice, *rest):
    strip, width = initial_warmth.shape
    tm_count, rows_count = lax.axis_size("tm"), lax.axis_size("rows")
    aligned = (
        pattern_choice.shape[0] == 2
        and strip * rows_count == width
        and strip % TILE == 0
        and width == rows_count * 2 * LANES
        and width % (4 * LANES) == 0
        and tm_count % 2 == 0
        and rows_count % 2 == 0
    )
    return (fused if aligned else shards)(initial_warmth, pattern_choice, *rest)


def solution(mesh):
    in_specs = (P("rows", None), P("tm", None, None), P(), P(), P(), P())
    out_specs = P("tm", "rows", None)
    return jax.shard_map(pick, mesh=mesh, in_specs=in_specs, out_specs=out_specs, check_vma=False)
```
